32 devices in a mesh: dev: 32 (over z, y, x, core).
Axes of the slice: x: 2, y: 2, z: 4, core: 2. Of those that a mesh axis runs over, the one named last changes fastest.
Arguments:
- gauss_params: float32 [59, 262144], P(None, 'dev'), may hold values from -8 to 8, as said below
- adam_first: float32 [59, 262144], P(None, 'dev'), may hold values from -6 to 6
- adam_second: float32 [59, 262144], P(None, 'dev'), may hold values from 0.0001 to 100
- camera: float32 [2, 6], replicated, may hold values from -0.004 to 0.004
- send_first: int32 [32, 4096], P('dev'), may hold values from -1 to 8191, as said below
- send_second: int32 [32, 4096], P('dev'), may hold values from -1 to 8191, as said below
- lists_first: int32 [1024, 128], P('dev'), may hold values from -1 to 4095, as said below
- lists_second: int32 [1024, 128], P('dev'), may hold values from -1 to 4095, as said below
- tiles_first: int32 [1024], P('dev'), may hold values from 0 to 1023, as said below
- tiles_second: int32 [1024], P('dev'), may hold values from 0 to 1023, as said below
- targets: float32 [1024, 3, 256], P('dev'), may hold values from 0 to 1
Outputs:
- new_params: float32 [59, 262144], P(None, 'dev')
- new_first: float32 [59, 262144], P(None, 'dev')
- new_second: float32 [59, 262144], P(None, 'dev')
- rendered_next: float32 [1024, 3, 256], P('dev')
The draws below stay inside these ranges and needn't reach their ends.
Inputs may be any that keep to these rules, and one draw needn't show every extreme that they name: `gauss_params`: rows 0 to 2 hold a position, 3 to 5 log scales, 6 to 9 a quaternion (w, x, y, z) with w at least 1, 10 an opacity logit, 11 + 16 c + k the spherical-harmonic coefficient k of colour c. Every Gaussian lies at depth 1.4 or more in front of both cameras. `send_first`: row s holds, for each destination d in turn, 128 slots: local column indices of Gaussians of device s, the used ones first, then -1. Entries other than -1 in a row are distinct. Some destination gets 128 used slots from every device. `send_second`: same form as send_first, but unused slots (-1) may stand anywhere in a destination's run. Some destination gets 128 used slots from every device. `lists_first`: row r, rendered by device r // 32, lists in compositing order (front first) received slots s * 128 + k of that device (slot k from device s), only used slots, then -1 to the end. Every used slot of a device appears exactly once among its rows. Some rows have no -1. `lists_second`: same form as lists_first, for the next view and its send array. `tiles_first`: A permutation of the image's tiles. `tiles_second`: A permutation of the image's tiles.
All inputs are finite; a program needn't handle non-finite values.
Results may differ from the reference program's by a relative error of at most 0.0003.
Values sent between devices are 32-bit elements; how exact they have to be, the bound alone decides.
No kernel may reach another device: no remote copies, remote signals or barrier semaphores. Data moves between devices by JAX's collectives and lax.ppermute only.
A program may use at most 128 MiB of HBM per device.

```python
import math
import jax
import jax.numpy as jnp
import numpy as np
from jax import lax

PARAMS = 59
LIST_LEN = 128
TILE_PIXELS = 256
TILES_X = 128
TILE_DEV = 32
G_DEV = 8192
CAP = 128
TILES = 1024
GAUSS = 262144
N_DEV = 32


def routing_tables(key):
    base = jax.random.fold_in(key, 911)
    key_list = jax.random.split(base, 7)
    half_cap = CAP // 2
    received = N_DEV * CAP
    device_ids = jnp.arange(N_DEV, dtype=jnp.int32)
    level_table = jnp.array([1, 1, 1, 1, 1, 2, 2, 4], jnp.int32)
    load_level = level_table[jax.random.randint(key_list[0], (N_DEV,), 0, 8)]
    ranking = jax.random.permutation(key_list[1], N_DEV).astype(jnp.int32)
    hot_first = ranking[0]
    hot_second = ranking[1]
    is_hot = (device_ids == hot_first) | (device_ids == hot_second)
    ceiling = CAP * load_level // 4
    drops = jax.random.randint(key_list[2], (N_DEV, N_DEV), 0, CAP + 1) % (ceiling // 8 + 1)[None, :]
    counts = jnp.where(is_hot[None, :], CAP, ceiling[None, :] - drops).astype(jnp.int32)
    source_keys = jax.random.split(key_list[3], N_DEV)
    local_ids = jax.vmap(lambda one_key: jax.random.permutation(one_key, G_DEV)[:received])(source_keys).astype(jnp.int32)
    run_slot = jnp.arange(received, dtype=jnp.int32) % CAP
    run_dest = jnp.arange(received, dtype=jnp.int32) // CAP
    used = run_slot[None, :] < counts[:, run_dest]
    send_first = jnp.where(used, local_ids, -1).astype(jnp.int32)
    tiles_first = jax.random.permutation(key_list[4], TILES).astype(jnp.int32)

    def device_lists(device_key, count_column):
        slot_ids = jnp.arange(received, dtype=jnp.int32)
        source_of = slot_ids // CAP
        slot_of = slot_ids % CAP
        half_of = slot_of // half_cap
        within = source_of * half_cap + slot_of - half_of * half_cap
        half_size = N_DEV * half_cap
        order_low = jax.random.permutation(jax.random.fold_in(device_key, 1), half_size).astype(jnp.int32)
        order_high = jax.random.permutation(jax.random.fold_in(device_key, 2), half_size).astype(jnp.int32)
        place = jnp.where(half_of == 0, order_low[within], half_size + order_high[within]).astype(jnp.int32)
        live = (slot_of < count_column[source_of]).astype(jnp.int32)
        entries = jnp.zeros((received,), jnp.int32).at[place].set(slot_ids).reshape(TILE_DEV, LIST_LEN)
        live_at = jnp.zeros((received,), jnp.int32).at[place].set(live).reshape(TILE_DEV, LIST_LEN)
        sort_key = (1 - live_at) * LIST_LEN + jnp.arange(LIST_LEN, dtype=jnp.int32)[None, :]
        order = jnp.argsort(sort_key, axis=1)
        entries = jnp.take_along_axis(entries, order, axis=1)
        live_at = jnp.take_along_axis(live_at, order, axis=1)
        return (jnp.where(live_at == 1, entries, -1).astype(jnp.int32), place)
    lists_all, places = jax.vmap(device_lists)(jax.random.split(key_list[5], N_DEV), counts.T)
    lists_first = lists_all.reshape(TILES, LIST_LEN)
    tile_rows = device_ids[:, None] * TILE_DEV + places // LIST_LEN
    tile_of_slot = tiles_first[tile_rows]
    by_source = jnp.transpose(tile_of_slot.reshape(N_DEV, N_DEV, CAP), (1, 0, 2)).reshape(N_DEV, received)
    home = jax.random.randint(key_list[6], (N_DEV, G_DEV), 0, TILES).astype(jnp.int32)
    home = home.at[device_ids[:, None], local_ids].set(by_source)
    loads = jnp.sum(counts, axis=0)
    score = loads + is_hot.astype(jnp.int32) * (N_DEV * CAP) + (device_ids == hot_first).astype(jnp.int32) * (N_DEV * CAP)
    descending = jnp.argsort(-(score * N_DEV + device_ids)).astype(jnp.int32)
    ascending = descending[::-1]
    previous = ascending[0]
    pair_high = ascending.at[0].set(descending[1]).at[N_DEV - 2].set(previous)
    pair_low = descending
    source_dest = jnp.where(run_slot < half_cap, pair_low[run_dest], pair_high[run_dest])
    send_second = send_first[:, source_dest * CAP + run_slot].astype(jnp.int32)
    row_ids = jnp.arange(TILES, dtype=jnp.int32)
    row_owner = row_ids // TILE_DEV
    row_within = row_ids % TILE_DEV
    from_device = jnp.where(row_within < TILE_DEV // 2, pair_low[row_owner], pair_high[row_owner])
    source_rows = from_device * TILE_DEV + row_within
    tiles_second = tiles_first[source_rows].astype(jnp.int32)
    lists_second = lists_first[source_rows].astype(jnp.int32)
    return (send_first, send_second, lists_first, lists_second, tiles_first, tiles_second, home.reshape(-1))


def draw_send_first(key, part):
    return routing_tables(key)[0]


def draw_send_second(key, part):
    return routing_tables(key)[1]


def draw_lists_first(key, part):
    return routing_tables(key)[2]


def draw_lists_second(key, part):
    return routing_tables(key)[3]


def draw_tiles_first(key, part):
    return routing_tables(key)[4]


def draw_tiles_second(key, part):
    return routing_tables(key)[5]


def draw_gauss_params(key, part):
    home = routing_tables(key)[6]
    float_keys = jax.random.split(jax.random.fold_in(key, 4242), 9)
    number = N_DEV * G_DEV
    image_width = TILES_X * 16.0
    image_height = TILES // TILES_X * 16.0
    across = (home % TILES_X).astype(jnp.float32) * 16.0 + jax.random.uniform(float_keys[0], (number,), jnp.float32, 0.0, 16.0)
    downward = (home // TILES_X).astype(jnp.float32) * 16.0 + jax.random.uniform(float_keys[1], (number,), jnp.float32, 0.0, 16.0)
    distance = jax.random.uniform(float_keys[2], (number,), jnp.float32, 2.0, 4.0)
    log_scales = jax.random.uniform(float_keys[3], (3, number), jnp.float32, -5.3, -4.3)
    logits = jax.random.uniform(float_keys[5], (1, number), jnp.float32, -4.0, 0.0)
    base_terms = jnp.clip(1.2 * jax.random.normal(float_keys[6], (3, 1, number), jnp.float32), -3.0, 3.0)
    high_terms = jnp.clip(0.25 * jax.random.normal(float_keys[7], (3, 15, number), jnp.float32), -1.0, 1.0)
    position_x = (across - 0.5 * image_width) * distance / 1000.0
    position_y = (downward - 0.5 * image_height) * distance / 1000.0
    versor = jnp.concatenate([jax.random.uniform(float_keys[4], (1, number), jnp.float32, 1.0, 2.0), jax.random.uniform(float_keys[8], (3, number), jnp.float32, -1.0, 1.0)])
    harmonics = jnp.concatenate([base_terms, high_terms], axis=1).reshape(48, number)
    return jnp.concatenate([jnp.stack([position_x, position_y, distance]), log_scales, versor, logits, harmonics]).astype(jnp.float32)


def levels(own_key, extent, cuts, smallest, largest):
    loudness = 1.0
    for axis_at, blocks in cuts:
        heights = jax.random.uniform(jax.random.fold_in(jax.random.fold_in(own_key, 6), axis_at), (blocks,), jnp.float32, smallest / len(cuts), largest / len(cuts))
        loudness = loudness * jnp.repeat(jnp.exp(heights), extent[axis_at] // blocks).reshape((-1,) + (1,) * (len(extent) - 1 - axis_at))
    return loudness


def bell_draw(stream_key, extent, scale, most, pieces=(), kind=jnp.bfloat16):
    gain = levels(stream_key, extent, pieces, -0.22, 0.18) if pieces else 1.0
    values = jax.random.normal(stream_key, extent, jnp.float32) * scale * gain
    return jnp.minimum(jnp.maximum(values, -most), most).astype(kind)


def setup_inputs(seed: int = 0) -> dict:
    streams_of = jax.random.split(jax.random.key(seed), 12)
    gauss_params = draw_gauss_params(jax.random.fold_in(streams_of[11], 71), 0)
    adam_first = bell_draw(streams_of[1], (PARAMS, GAUSS), 1.0, 6.0, ((1, 32),), jnp.float32)
    adam_second = jnp.clip(jnp.exp(math.log(100.0) - 13.815511 * jax.random.uniform(streams_of[2], (PARAMS, GAUSS), jnp.float32) ** levels(streams_of[2], (PARAMS, GAUSS), ((1, 32),), -0.2, 0.2)), 0.0001, 100.0)
    camera = jnp.clip(jax.random.uniform(streams_of[3], (2, 6), jnp.float32, -0.004, 0.004), -0.004, 0.004)
    send_first = draw_send_first(jax.random.fold_in(streams_of[11], 71), 0)
    send_second = draw_send_second(jax.random.fold_in(streams_of[11], 71), 0)
    lists_first = draw_lists_first(jax.random.fold_in(streams_of[11], 71), 0)
    lists_second = draw_lists_second(jax.random.fold_in(streams_of[11], 71), 0)
    tiles_first = draw_tiles_first(jax.random.fold_in(streams_of[11], 71), 0)
    tiles_second = draw_tiles_second(jax.random.fold_in(streams_of[11], 71), 0)
    targets = jnp.clip(1.0 * jax.random.uniform(streams_of[10], (TILES, 3, TILE_PIXELS), jnp.float32) ** levels(streams_of[10], (TILES, 3, TILE_PIXELS), ((0, 32),), -0.2, 0.2), 0.0, 1.0)
    return {"gauss_params": gauss_params, "adam_first": adam_first, "adam_second": adam_second, "camera": camera, "send_first": send_first, "send_second": send_second, "lists_first": lists_first, "lists_second": lists_second, "tiles_first": tiles_first, "tiles_second": tiles_second, "targets": targets}


tile_edge = 16
focal_length = 1000.0
blur_floor = 0.3
adam_epsilon = 1e-08
bias_first = 1.0 - 0.9 ** 20
bias_second = 1.0 - 0.999 ** 20
sh_first = 0.28209479177387814
sh_second = 0.4886025119029199
sh_third = (1.0925484305920792, -1.0925484305920792, 0.31539156525252005, -1.0925484305920792, 0.5462742152960396)
sh_fourth = (-0.5900435899266435, 2.890611442640554, -0.4570457994644658, 0.3731763325901154, -0.4570457994644658, 1.445305721320277, -0.5900435899266435)

def rate_values():
    values = np.full((59,), 0.000125)
    values[0:3] = 0.00016
    values[3:6] = 0.005
    values[6:10] = 0.001
    values[10] = 0.05
    values[11] = 0.0025
    values[27] = 0.0025
    values[43] = 0.0025
    return values

def camera_frame(camera_row):
    cosine_a, sine_a = (jnp.cos(camera_row[0]), jnp.sin(camera_row[0]))
    cosine_b, sine_b = (jnp.cos(camera_row[1]), jnp.sin(camera_row[1]))
    cosine_c, sine_c = (jnp.cos(camera_row[2]), jnp.sin(camera_row[2]))
    filler_zero = jnp.zeros_like(cosine_a)
    filler_one = jnp.ones_like(cosine_a)
    turn_x = jnp.stack([jnp.stack([filler_one, filler_zero, filler_zero]), jnp.stack([filler_zero, cosine_a, -sine_a]), jnp.stack([filler_zero, sine_a, cosine_a])])
    turn_y = jnp.stack([jnp.stack([cosine_b, filler_zero, sine_b]), jnp.stack([filler_zero, filler_one, filler_zero]), jnp.stack([-sine_b, filler_zero, cosine_b])])
    turn_z = jnp.stack([jnp.stack([cosine_c, -sine_c, filler_zero]), jnp.stack([sine_c, cosine_c, filler_zero]), jnp.stack([filler_zero, filler_zero, filler_one])])
    highest = lax.Precision.HIGHEST
    rotation = jnp.dot(turn_z, jnp.dot(turn_y, turn_x, precision=highest), precision=highest)
    return (rotation, camera_row[3:6])

def sh_terms(along_x, along_y, along_z):
    square_x, square_y, square_z = (along_x * along_x, along_y * along_y, along_z * along_z)
    return [-sh_second * along_y, sh_second * along_z, -sh_second * along_x, sh_third[0] * along_x * along_y, sh_third[1] * along_y * along_z, sh_third[2] * (2.0 * square_z - square_x - square_y), sh_third[3] * along_x * along_z, sh_third[4] * (square_x - square_y), sh_fourth[0] * along_y * (3.0 * square_x - square_y), sh_fourth[1] * along_x * along_y * along_z, sh_fourth[2] * along_y * (4.0 * square_z - square_x - square_y), sh_fourth[3] * along_z * (2.0 * square_z - 3.0 * square_x - 3.0 * square_y), sh_fourth[4] * along_x * (4.0 * square_z - square_x - square_y), sh_fourth[5] * along_z * (square_x - square_y), sh_fourth[6] * along_x * (square_x - 3.0 * square_y)]

def project(params, camera_row, image_width, image_height):
    rotation, offset = camera_frame(camera_row)
    centres = params[0:3]
    viewed = [rotation[row_index, 0] * centres[0] + rotation[row_index, 1] * centres[1] + rotation[row_index, 2] * centres[2] + offset[row_index] for row_index in range(3)]
    inverse_depth = 1.0 / viewed[2]
    screen_u = focal_length * viewed[0] * inverse_depth + 0.5 * image_width
    screen_v = focal_length * viewed[1] * inverse_depth + 0.5 * image_height
    scales = jnp.exp(params[3:6])
    versor = params[6:10] / jnp.sqrt(lax.optimization_barrier(jnp.sum(params[6:10] * params[6:10], axis=0)))
    part_w, part_x, part_y, part_z = (versor[0], versor[1], versor[2], versor[3])
    turn_rows = [[1.0 - 2.0 * (part_y * part_y + part_z * part_z), 2.0 * (part_x * part_y - part_w * part_z), 2.0 * (part_x * part_z + part_w * part_y)], [2.0 * (part_x * part_y + part_w * part_z), 1.0 - 2.0 * (part_x * part_x + part_z * part_z), 2.0 * (part_y * part_z - part_w * part_x)], [2.0 * (part_x * part_z - part_w * part_y), 2.0 * (part_y * part_z + part_w * part_x), 1.0 - 2.0 * (part_x * part_x + part_y * part_y)]]
    factor = [[turn_rows[row_index][col_index] * scales[col_index] for col_index in range(3)] for row_index in range(3)]
    spread = [[factor[row_index][0] * factor[col_index][0] + factor[row_index][1] * factor[col_index][1] + factor[row_index][2] * factor[col_index][2] for col_index in range(3)] for row_index in range(3)]
    jacobian = [[focal_length * inverse_depth, 0.0, -focal_length * viewed[0] * inverse_depth * inverse_depth], [0.0, focal_length * inverse_depth, -focal_length * viewed[1] * inverse_depth * inverse_depth]]
    mapping = [[jacobian[row_index][0] * rotation[0, col_index] + jacobian[row_index][1] * rotation[1, col_index] + jacobian[row_index][2] * rotation[2, col_index] for col_index in range(3)] for row_index in range(2)]

    def mapped(first_index, second_index):
        running = 0.0
        for inner_a in range(3):
            for inner_b in range(3):
                running = running + mapping[first_index][inner_a] * spread[inner_a][inner_b] * mapping[second_index][inner_b]
        return running
    cover_a = mapped(0, 0) + blur_floor
    cover_b = mapped(0, 1)
    cover_c = mapped(1, 1) + blur_floor
    determinant = cover_a * cover_c - cover_b * cover_b
    opacity = jax.nn.sigmoid(params[10])
    centre_cam = [-(rotation[0, col_index] * offset[0] + rotation[1, col_index] * offset[1] + rotation[2, col_index] * offset[2]) for col_index in range(3)]
    towards = [centres[col_index] - centre_cam[col_index] for col_index in range(3)]
    length = jnp.sqrt(towards[0] * towards[0] + towards[1] * towards[1] + towards[2] * towards[2])
    harmonics = sh_terms(towards[0] / length, towards[1] / length, towards[2] / length)
    colours = []
    for channel in range(3):
        running = 0.5 + sh_first * params[11 + 16 * channel]
        for term_index in range(1, 16):
            running = running + harmonics[term_index - 1] * params[11 + 16 * channel + term_index]
        colours.append(jnp.maximum(running, 0.0))
    return jnp.stack([screen_u, screen_v, cover_c / determinant, -cover_b / determinant, cover_a / determinant, opacity] + colours)

def composite(gathered, live_mask, tile_numbers):
    pixel_ids = jnp.arange(TILE_PIXELS, dtype=jnp.int32)
    pixel_col = (tile_numbers % TILES_X)[:, None] * tile_edge + pixel_ids[None, :] % tile_edge
    pixel_row = (tile_numbers // TILES_X)[:, None] * tile_edge + pixel_ids[None, :] // tile_edge
    offset_x = gathered[0][:, None, :] - (pixel_col.astype(gathered.dtype) + 0.5)[:, :, None]
    offset_y = gathered[1][:, None, :] - (pixel_row.astype(gathered.dtype) + 0.5)[:, :, None]
    exponent = -0.5 * (gathered[2][:, None, :] * offset_x * offset_x + gathered[4][:, None, :] * offset_y * offset_y) - gathered[3][:, None, :] * offset_x * offset_y
    coverage = gathered[5][:, None, :] * jnp.exp(exponent) * live_mask[:, None, :]
    log_clear = jnp.log1p(-coverage)
    before = jnp.cumsum(log_clear, axis=2) - log_clear
    weight = coverage * jnp.exp(before)
    return jnp.einsum('bpi,cbi->bcp', weight, gathered[6:9], precision=lax.Precision.HIGHEST)

def gathered_splats(splats, send, tile_lists):
    slot_table = jnp.maximum(send, 0).reshape(N_DEV, N_DEV, CAP) + (jnp.arange(N_DEV, dtype=jnp.int32) * G_DEV)[:, None, None]
    slot_table = jnp.transpose(slot_table, (1, 0, 2)).reshape(N_DEV, N_DEV * CAP)
    safe_ids = jnp.maximum(tile_lists, 0).reshape(N_DEV, TILE_DEV * LIST_LEN)
    global_ids = jnp.take_along_axis(slot_table, safe_ids, axis=1).reshape(TILES * LIST_LEN)
    return jnp.take(splats, global_ids, axis=1).reshape(9, TILES, LIST_LEN)

def render_all(gathered, live_mask, tile_numbers):
    group_size = 32
    block_count = TILES // group_size
    stacked = jnp.transpose(gathered.reshape(9, block_count, group_size, LIST_LEN), (1, 0, 2, 3))
    masks = live_mask.reshape(block_count, group_size, LIST_LEN)
    numbers = tile_numbers.reshape(block_count, group_size)
    rendered = lax.map(jax.checkpoint(lambda items: composite(items[0], items[1], items[2])), (stacked, masks, numbers))
    return rendered.reshape(TILES, 3, TILE_PIXELS)

def reference(gauss_params, adam_first, adam_second, camera, send_first, send_second, lists_first, lists_second, tiles_first, tiles_second, targets):
    image_width = TILES_X * tile_edge * 1.0
    image_height = TILES // TILES_X * tile_edge * 1.0
    live_first = (lists_first >= 0).astype(gauss_params.dtype)
    live_second = (lists_second >= 0).astype(gauss_params.dtype)

    def loss_of(params):
        splats = project(params, camera[0], image_width, image_height)
        rendered = render_all(gathered_splats(splats, send_first, lists_first), live_first, tiles_first)
        return 0.5 * jnp.sum((rendered - targets) ** 2)
    gradient = jax.grad(loss_of)(gauss_params)
    new_first = 0.9 * adam_first + 0.1 * gradient
    new_second = 0.999 * adam_second + 0.001 * gradient * gradient
    step_sizes = jnp.asarray(rate_values(), gauss_params.dtype)[:, None]
    new_params = gauss_params - step_sizes * (new_first / bias_first) / (jnp.sqrt(new_second / bias_second) + adam_epsilon)
    splats_next = project(new_params, camera[1], image_width, image_height)
    rendered_next = render_all(gathered_splats(splats_next, send_second, lists_second), live_second, tiles_second)
    return (new_params, new_first, new_second, rendered_next)
```

```python
import functools

import jax
import jax.numpy as jnp
import numpy as np
from jax import lax
from jax.experimental import pallas as pl
from jax.experimental.pallas import tpu as pltpu
from jax.sharding import PartitionSpec as P

PARAMS = 59
LIST_LEN = 128
TILE_PIXELS = 256
TILES_X = 128
LANES = 128
ROWS = 9
STRIDE = 72

tile_edge = 16
focal_length = 1000.0
blur_floor = 0.3
adam_epsilon = 1e-08
bias_first = 1.0 - 0.9**20
bias_second = 1.0 - 0.999**20
sh_first = 0.28209479177387814
sh_second = 0.4886025119029199
sh_third = (
    1.0925484305920792,
    -1.0925484305920792,
    0.31539156525252005,
    -1.0925484305920792,
    0.5462742152960396,
)
sh_fourth = (
    -0.5900435899266435,
    2.890611442640554,
    -0.4570457994644658,
    0.3731763325901154,
    -0.4570457994644658,
    1.445305721320277,
    -0.5900435899266435,
)

f32 = jnp.float32
bf16 = jnp.bfloat16
VMEM = pl.BlockSpec(memory_space=pltpu.VMEM)
SMEM = pl.BlockSpec(memory_space=pltpu.SMEM)
ANY = pl.BlockSpec(memory_space=pl.ANY)


def rate_values():
    values = np.full((64,), 0.000125)
    values[0:3] = 0.00016
    values[3:6] = 0.005
    values[6:10] = 0.001
    values[10] = 0.05
    values[11] = 0.0025
    values[27] = 0.0025
    values[43] = 0.0025
    return values


def camera_frame(camera_ref, view):
    shape = (8, LANES)
    angle = [jnp.full(shape, camera_ref[view, k], f32) for k in range(3)]
    shift = [jnp.full(shape, camera_ref[view, 3 + k], f32) for k in range(3)]
    (ca, cb, cc) = [jnp.cos(x) for x in angle]
    (sa, sb, sc) = [jnp.sin(x) for x in angle]
    rot = [
        [cc * cb, cc * sb * sa - sc * ca, cc * sb * ca + sc * sa],
        [sc * cb, sc * sb * sa + cc * ca, sc * sb * ca - cc * sa],
        [-sb, cb * sa, cb * ca],
    ]
    back = [
        rot[0][k] * shift[0] + rot[1][k] * shift[1] + rot[2][k] * shift[2]
        for k in range(3)
    ]
    return rot, shift, back


def sh_terms(x, y, z):
    xx, yy, zz = (x * x, y * y, z * z)
    return [
        -sh_second * y,
        sh_second * z,
        -sh_second * x,
        sh_third[0] * x * y,
        sh_third[1] * y * z,
        sh_third[2] * (2.0 * zz - xx - yy),
        sh_third[3] * x * z,
        sh_third[4] * (xx - yy),
        sh_fourth[0] * y * (3.0 * xx - yy),
        sh_fourth[1] * x * y * z,
        sh_fourth[2] * y * (4.0 * zz - xx - yy),
        sh_fourth[3] * z * (2.0 * zz - 3.0 * xx - 3.0 * yy),
        sh_fourth[4] * x * (4.0 * zz - xx - yy),
        sh_fourth[5] * z * (xx - yy),
        sh_fourth[6] * x * (xx - 3.0 * yy),
    ]


def project(params, frame, half_width, half_height):
    rot, shift, back = frame
    centres = params[0:3]
    viewed = [
        rot[k][0] * centres[0] + rot[k][1] * centres[1] + rot[k][2] * centres[2] + shift[k]
        for k in range(3)
    ]
    inverse = 1.0 / viewed[2]
    scale_z = focal_length * inverse
    u_off = scale_z * viewed[0]
    w_off = scale_z * viewed[1]
    slope_u = u_off * inverse
    slope_w = w_off * inverse
    scales = [jnp.exp(params[3 + k]) for k in range(3)]
    q = params[6:10]
    norm = lax.rsqrt(q[0] * q[0] + q[1] * q[1] + q[2] * q[2] + q[3] * q[3])
    qw, qx, qy, qz = [v * norm for v in q]
    turn = [
        [
            1.0 - 2.0 * (qy * qy + qz * qz),
            2.0 * (qx * qy - qw * qz),
            2.0 * (qx * qz + qw * qy),
        ],
        [
            2.0 * (qx * qy + qw * qz),
            1.0 - 2.0 * (qx * qx + qz * qz),
            2.0 * (qy * qz - qw * qx),
        ],
        [
            2.0 * (qx * qz - qw * qy),
            2.0 * (qy * qz + qw * qx),
            1.0 - 2.0 * (qx * qx + qy * qy),
        ],
    ]
    mapping = [
        [scale_z * rot[0][k] - slope_u * rot[2][k] for k in range(3)],
        [scale_z * rot[1][k] - slope_w * rot[2][k] for k in range(3)],
    ]
    factor = [
        [
            (row[0] * turn[0][k] + row[1] * turn[1][k] + row[2] * turn[2][k]) * scales[k]
            for k in range(3)
        ]
        for row in mapping
    ]
    first, second = factor
    cover_a = first[0] * first[0] + first[1] * first[1] + first[2] * first[2] + blur_floor
    cover_b = first[0] * second[0] + first[1] * second[1] + first[2] * second[2]
    cover_c = second[0] * second[0] + second[1] * second[1] + second[2] * second[2] + blur_floor
    scale_det = 1.0 / (cover_a * cover_c - cover_b * cover_b)
    opacity = 1.0 / (1.0 + jnp.exp(-params[10]))
    towards = [centres[k] + back[k] for k in range(3)]
    length = lax.rsqrt(
        towards[0] * towards[0] + towards[1] * towards[1] + towards[2] * towards[2]
    )
    harmonics = sh_terms(*[v * length for v in towards])
    colours = []
    for channel in range(3):
        running = 0.5 + sh_first * params[11 + 16 * channel]
        for term in range(15):
            running = running + harmonics[term] * params[12 + 16 * channel + term]
        colours.append(jnp.maximum(running, 0.0))
    return [
        u_off + half_width,
        w_off + half_height,
        cover_c * scale_det,
        -cover_b * scale_det,
        cover_a * scale_det,
        opacity,
    ] + colours


def permute(idx_ref, main_ref, last_ref, chunks, rows, write):
    def group_step(group, unused):
        base = pl.multiple_of(group * 8, 8)
        index = idx_ref[pl.ds(base, 8), :]
        high = index >> 7
        low = index & 127
        highs = [jnp.broadcast_to(high[k : k + 1], (8, LANES)) for k in range(8)]
        lows = [jnp.broadcast_to(low[k : k + 1], (8, LANES)) for k in range(8)]
        totals = [jnp.zeros((8, LANES), f32) for k in range(9)]
        for chunk in range(chunks):
            source = main_ref[chunk]
            for k in range(8):
                found = jnp.take_along_axis(
                    source, lows[k], axis=1, mode="promise_in_bounds"
                )
                totals[k] = jnp.where(highs[k] == chunk, found, totals[k])
            source = jnp.broadcast_to(last_ref[chunk : chunk + 1, :], (8, LANES))
            found = jnp.take_along_axis(source, low, axis=1, mode="promise_in_bounds")
            totals[8] = jnp.where(high == chunk, found, totals[8])
        write(group, totals[:8], totals[8])
        return unused

    lax.fori_loop(0, rows // 8, group_step, 0)


def invert(idx_ref, rows, high_count, inverse_ref):
    index = idx_ref[...]
    high = index >> 7
    low = index & 127
    high_ids = lax.broadcasted_iota(jnp.int32, (high_count, LANES), 0)
    low_ids = lax.broadcasted_iota(jnp.int32, (LANES, LANES), 0)
    lane_ids = lax.broadcasted_iota(jnp.int32, (high_count, LANES), 1).astype(f32)
    total = jnp.zeros((2 * high_count, LANES), f32)
    for start in range(0, rows, 8):
        left = []
        right = []
        for row in range(start, start + 8):
            here = high[row : row + 1] == high_ids
            left.append(
                jnp.concatenate(
                    [jnp.where(here, row + 1.0, 0.0), jnp.where(here, lane_ids, 0.0)], axis=0
                ).astype(bf16)
            )
            right.append(jnp.where(low[row : row + 1] == low_ids, 1.0, 0.0).astype(bf16))
        total = total + lax.dot_general(
            jnp.concatenate(left, axis=1),
            jnp.concatenate(right, axis=1),
            (((1,), (1,)), ((), ())),
            preferred_element_type=f32,
        )
    rows_found = total[:high_count].astype(jnp.int32)
    lanes_found = total[high_count:].astype(jnp.int32)
    inverse_ref[...] = (rows_found - 1) * LANES + lanes_found


def unpack(packed_ref, main_ref, last_ref, chunks):
    for chunk in range(chunks):
        for k in range(8):
            main_ref[chunk, k : k + 1, :] = packed_ref[chunk, :, k * LANES : (k + 1) * LANES]
        last_ref[chunk : chunk + 1, :] = packed_ref[chunk, :, 8 * LANES : 9 * LANES]


def pack_group(packed_ref):
    def write(group, vectors, last):
        for k in range(8):
            row = group * 8 + k
            for item in range(8):
                packed_ref[row, :, item * LANES : (item + 1) * LANES] = vectors[k][
                    item : item + 1
                ]
            packed_ref[row, :, 8 * LANES : 9 * LANES] = last[k : k + 1]

    return write


def slots_as_rows(slots_ref, idx_ref, rows):
    for row in range(rows):
        idx_ref[row : row + 1, :] = slots_ref[:, row * LANES : (row + 1) * LANES]


def to_dense(native, dense_ref, row_block, chunk):
    if native.shape[0] == 8:
        dense_ref[pl.ds(8 * row_block * STRIDE + chunk, 8, stride=STRIDE), :] = native
    else:
        for k in range(native.shape[0]):
            dense_ref[pl.ds((8 * row_block + k) * STRIDE + chunk, 1), :] = native[k : k + 1]


def dense_load(dense_ref, row, group):
    return dense_ref[pl.ds(pl.multiple_of(row * STRIDE + group * 8, 8), 8), :]


def dense_store(dense_ref, row, group, value):
    dense_ref[pl.ds(pl.multiple_of(row * STRIDE + group * 8, 8), 8), :] = value


def row_blocks():
    return [(block, min(8, PARAMS - 8 * block)) for block in range((PARAMS + 7) // 8)]


def project_groups(dense_ref, splat_ref, frame, half_width, half_height, chunks):
    def step(group, unused):
        params = [dense_load(dense_ref, row, group) for row in range(PARAMS)]
        for row, value in enumerate(project(params, frame, half_width, half_height)):
            dense_store(splat_ref, row, group, value)
        return unused

    lax.fori_loop(0, chunks // 8, step, 0)


def send_splats(splat_ref, main_ref, idx_ref, packed_ref, chunks, rows):
    for chunk in range(chunks):
        main_ref[chunk] = splat_ref[pl.ds(chunk, 8, stride=STRIDE), :]
    last_ref = splat_ref.at[pl.ds(8 * STRIDE, chunks), :]
    permute(idx_ref, main_ref, last_ref, chunks, rows, pack_group(packed_ref))


def first_owner_body(
    half_width,
    half_height,
    camera_ref,
    params_ref,
    slots_ref,
    packed_ref,
    dense_ref,
    splat_ref,
    main_ref,
    idx_ref,
):
    chunks = params_ref.shape[1] // LANES
    rows = slots_ref.shape[1] // LANES
    slots_as_rows(slots_ref, idx_ref, rows)

    def relayout(chunk, unused):
        lanes = pl.ds(pl.multiple_of(chunk * LANES, LANES), LANES)
        for block, size in row_blocks():
            to_dense(params_ref[8 * block : 8 * block + size, lanes], dense_ref, block, chunk)
        return unused

    lax.fori_loop(0, chunks, relayout, 0, unroll=4)
    frame = camera_frame(camera_ref, 0)
    project_groups(dense_ref, splat_ref, frame, half_width, half_height, chunks)
    send_splats(splat_ref, main_ref, idx_ref, packed_ref, chunks, rows)


def first_owner(camera, params, slots, half_width, half_height):
    chunks = params.shape[1] // LANES
    rows = slots.shape[1] // LANES
    return pl.pallas_call(
        functools.partial(first_owner_body, half_width, half_height),
        out_shape=jax.ShapeDtypeStruct((rows, 1, ROWS * LANES), f32),
        in_specs=[SMEM, VMEM, VMEM],
        out_specs=VMEM,
        scratch_shapes=[
            pltpu.VMEM((64 * STRIDE, LANES), f32),
            pltpu.VMEM((ROWS * STRIDE, LANES), f32),
            pltpu.VMEM((chunks, 8, LANES), f32),
            pltpu.VMEM((rows, LANES), jnp.int32),
        ],
        name="first_owner",
    )(camera, params, slots)


def second_owner_body(
    half_width,
    half_height,
    camera_ref,
    params_ref,
    first_hbm,
    second_hbm,
    slots_ref,
    next_slots_ref,
    packed_ref,
    out_params_hbm,
    out_first_hbm,
    out_second_hbm,
    out_packed_ref,
    dense_ref,
    grad_ref,
    splat_ref,
    main_ref,
    last_ref,
    idx_ref,
    inverse_ref,
    params_out_ref,
    first_ref,
    second_ref,
    load_sems,
    store_sems,
):
    chunks = params_ref.shape[1] // LANES
    rows = slots_ref.shape[1] // LANES
    loads = [
        pltpu.make_async_copy(first_hbm, first_ref, load_sems.at[0]),
        pltpu.make_async_copy(second_hbm, second_ref, load_sems.at[1]),
    ]
    for copy in loads:
        copy.start()
    slots_as_rows(slots_ref, idx_ref, rows)
    invert(idx_ref, rows, chunks, inverse_ref)
    unpack(packed_ref, main_ref, last_ref, rows)

    def relayout(chunk, unused):
        lanes = pl.ds(pl.multiple_of(chunk * LANES, LANES), LANES)
        for block, size in row_blocks():
            to_dense(params_ref[8 * block : 8 * block + size, lanes], dense_ref, block, chunk)
        return unused

    lax.fori_loop(0, chunks, relayout, 0, unroll=4)

    def write_columns(group, vectors, last):
        for k in range(8):
            splat_ref[pl.ds(group * 8 + k, 8, stride=STRIDE), :] = vectors[k]
        dense_store(splat_ref, 8, group, last)

    permute(inverse_ref, main_ref, last_ref, rows, chunks, write_columns)

    frame = camera_frame(camera_ref, 0)

    def pull_step(group, unused):
        params = [dense_load(dense_ref, row, group) for row in range(PARAMS)]
        splats, pullback = jax.vjp(
            lambda *p: project(list(p), frame, half_width, half_height), *params
        )
        cotangents = [dense_load(splat_ref, row, group) for row in range(ROWS)]
        through_opacity = cotangents[5] * (1.0 - splats[5])
        cotangents[5] = jnp.zeros_like(cotangents[5])
        grads = list(pullback(cotangents))
        grads[10] = through_opacity
        for row, value in enumerate(grads):
            dense_store(grad_ref, row, group, value)
        return unused

    lax.fori_loop(0, chunks // 8, pull_step, 0)

    for copy in loads:
        copy.wait()
    rates = rate_values() / bias_first
    stores = []
    row_ids = lax.broadcasted_iota(jnp.int32, (8, LANES), 0)
    for block, size in row_blocks():
        span = slice(8 * block, 8 * block + size)
        block_rates = rates[8 * block : 8 * block + 8]
        step_size = jnp.full((8, LANES), block_rates[0], f32)
        for k in range(1, 8):
            if block_rates[k] != block_rates[0]:
                step_size = jnp.where(row_ids == k, f32(block_rates[k]), step_size)
        step_size = step_size[:size]

        def adam_step(chunk, unused, block=block, size=size, span=span, step_size=step_size):
            lanes = pl.ds(pl.multiple_of(chunk * LANES, LANES), LANES)
            gradient = grad_ref[pl.ds(8 * block * STRIDE + chunk, 8, stride=STRIDE), :][:size]
            moment = 0.9 * first_ref[span, lanes] + 0.1 * gradient
            square = 0.999 * second_ref[span, lanes] + 0.001 * gradient * gradient
            scaled = square * (1.0 / bias_second)
            root = scaled * lax.rsqrt(scaled)
            fresh = params_ref[span, lanes] - step_size * moment / (root + adam_epsilon)
            first_ref[span, lanes] = moment
            second_ref[span, lanes] = square
            params_out_ref[span, lanes] = fresh
            to_dense(fresh, dense_ref, block, chunk)
            return unused

        lax.fori_loop(0, chunks, adam_step, 0, unroll=8)
        for number, (source, target) in enumerate(
            [
                (params_out_ref, out_params_hbm),
                (first_ref, out_first_hbm),
                (second_ref, out_second_hbm),
            ]
        ):
            copy = pltpu.make_async_copy(
                source.at[span, :], target.at[span, :], store_sems.at[number, block]
            )
            copy.start()
            stores.append(copy)

    slots_as_rows(next_slots_ref, idx_ref, rows)
    frame = camera_frame(camera_ref, 1)
    project_groups(dense_ref, splat_ref, frame, half_width, half_height, chunks)
    send_splats(splat_ref, main_ref, idx_ref, out_packed_ref, chunks, rows)
    for copy in stores:
        copy.wait()


def second_owner(camera, params, first, second, slots, next_slots, packed, half_width, half_height):
    chunks = params.shape[1] // LANES
    rows = slots.shape[1] // LANES
    shape = jax.ShapeDtypeStruct(params.shape, f32)
    return pl.pallas_call(
        functools.partial(second_owner_body, half_width, half_height),
        out_shape=(shape, shape, shape, jax.ShapeDtypeStruct((rows, 1, ROWS * LANES), f32)),
        in_specs=[SMEM, VMEM, ANY, ANY, VMEM, VMEM, VMEM],
        out_specs=(ANY, ANY, ANY, VMEM),
        scratch_shapes=[
            pltpu.VMEM((64 * STRIDE, LANES), f32),
            pltpu.VMEM((64 * STRIDE, LANES), f32),
            pltpu.VMEM((ROWS * STRIDE, LANES), f32),
            pltpu.VMEM((max(chunks, rows), 8, LANES), f32),
            pltpu.VMEM((rows, LANES), f32),
            pltpu.VMEM((rows, LANES), jnp.int32),
            pltpu.VMEM((chunks, LANES), jnp.int32),
            pltpu.VMEM(params.shape, f32),
            pltpu.VMEM(params.shape, f32),
            pltpu.VMEM(params.shape, f32),
            pltpu.SemaphoreType.DMA((2,)),
            pltpu.SemaphoreType.DMA((3, 8)),
        ],
        name="second_owner",
    )(camera, params, first, second, slots, next_slots, packed)


def halves(value):
    high = value.astype(bf16)
    return high, (value - high.astype(f32)).astype(bf16)


def triangle_pair(forward):
    rows = lax.broadcasted_iota(jnp.int32, (LIST_LEN, LIST_LEN), 0)
    cols = lax.broadcasted_iota(jnp.int32, (LIST_LEN, LIST_LEN), 1)
    chosen = rows < cols if forward else rows > cols
    one = jnp.where(chosen, 1.0, 0.0).astype(bf16)
    return jnp.concatenate([one, one], axis=0)


def batch_tiles(tile_count):
    return 8 if tile_count % 8 == 0 else 1


def tile_offsets(splat_ref, tile, number):
    left = (number % TILES_X) * tile_edge
    top = (number // TILES_X) * tile_edge
    ids = lax.broadcasted_iota(jnp.int32, (8, LANES), 0)
    u = jnp.broadcast_to(splat_ref[tile, 0:1, :], (8, LANES))
    w = jnp.broadcast_to(splat_ref[tile, 1:2, :], (8, LANES))
    across = [u - ((ids + (left + 8 * h)).astype(f32) + 0.5) for h in range(2)]
    down = [w - ((ids + (top + 8 * h)).astype(f32) + 0.5) for h in range(2)]
    return across, down


def spread_row(ref, row):
    return jnp.broadcast_to(ref[row : row + 1, :], (8, LANES))


def alpha_phase(splat_ref, tile, number, base, row_ref, alpha_ref, odds_ref, pair_ref):
    a, b, c, o = [jnp.broadcast_to(splat_ref[tile, k : k + 1, :], (8, LANES)) for k in (2, 3, 4, 5)]
    across, down = tile_offsets(splat_ref, tile, number)
    along = [(-0.5 * a) * x * x for x in across]
    for h in range(2):
        row_ref[8 * h : 8 * h + 8, :] = (-0.5 * c) * down[h] * down[h]
        row_ref[16 + 8 * h : 24 + 8 * h, :] = -(b * down[h])
    for row in range(tile_edge):
        fixed = spread_row(row_ref, row)
        slope = spread_row(row_ref, 16 + row)
        logs = []
        for h in range(2):
            exponent = along[h] + (fixed + slope * across[h])
            alpha = o * jnp.exp(exponent)
            log_clear = jnp.log(1.0 - alpha)
            where = pl.ds(base + row * tile_edge + 8 * h, 8)
            alpha_ref[where, :] = alpha
            if odds_ref is not None:
                odds_ref[where, :] = alpha * jnp.exp(-log_clear)
            logs.append(log_clear)
        high, low = halves(jnp.concatenate(logs, axis=0))
        where = pl.ds(base + row * tile_edge, tile_edge)
        pair_ref[where, :LIST_LEN] = high
        pair_ref[where, LIST_LEN:] = low


def weight_phase(base, before_ref, alpha_ref, weight_ref, pair_ref):
    for row in range(tile_edge):
        where = pl.ds(base + row * tile_edge, tile_edge)
        weight = alpha_ref[where, :] * jnp.exp(before_ref[where, :])
        if weight_ref is not None:
            weight_ref[where, :] = weight
        high, low = halves(weight)
        pair_ref[where, :LIST_LEN] = high
        pair_ref[where, LIST_LEN:] = low


def split_colours(splat_ref, tile):
    colours = splat_ref[tile, 6:14, :]
    high = colours.astype(bf16).astype(f32)
    return high, colours - high


def colour_sum(high, low, pair):
    upper = jnp.concatenate([high, high], axis=1)
    lower = jnp.concatenate([low, jnp.zeros_like(low)], axis=1)
    result = lax.dot_general(
        jnp.concatenate([upper, lower], axis=0).astype(bf16),
        pair,
        (((1,), (1,)), ((), ())),
        preferred_element_type=f32,
    )
    return result[0:8] + result[8:16]


def gather_tiles(lists_ref, packed_ref, main_ref, last_ref, splat_ref):
    chunks = packed_ref.shape[0]
    tile_count = lists_ref.shape[0]
    unpack(packed_ref, main_ref, last_ref, chunks)

    def write(group, vectors, last):
        for k in range(8):
            tile = group * 8 + k
            splat_ref[tile, 0:8, :] = vectors[k]
            splat_ref[tile, 8:9, :] = last[k : k + 1]
            splat_ref[tile, 9:16, :] = jnp.zeros((7, LANES), f32)

    permute(lists_ref, main_ref, last_ref, chunks, tile_count, write)


def train_body(
    numbers_ref,
    lists_ref,
    targets_ref,
    packed_ref,
    out_packed_ref,
    main_ref,
    last_ref,
    splat_ref,
    row_ref,
    alpha_ref,
    odds_ref,
    plain_ref,
    weight_ref,
    pair_ref,
    grad_pair_ref,
    grad_ref,
    grad_last_ref,
    inverse_ref,
):
    tile_count = lists_ref.shape[0]
    batch = batch_tiles(tile_count)
    gather_tiles(lists_ref, packed_ref, main_ref, last_ref, splat_ref)
    invert(lists_ref, tile_count, packed_ref.shape[0], inverse_ref)
    forward = triangle_pair(True)
    backward = triangle_pair(False)

    def batch_step(step, unused):
        first = step * batch

        def alphas(k, unused):
            tile = first + k
            base = pl.multiple_of(k * TILE_PIXELS, TILE_PIXELS)
            alpha_phase(
                splat_ref, tile, numbers_ref[tile], base, row_ref, alpha_ref, odds_ref, pair_ref
            )
            return unused

        lax.fori_loop(0, batch, alphas, 0)
        plain_ref[...] = jnp.dot(pair_ref[...], forward, preferred_element_type=f32)

        def weights(k, unused):
            base = pl.multiple_of(k * TILE_PIXELS, TILE_PIXELS)
            weight_phase(base, plain_ref, alpha_ref, weight_ref, pair_ref)
            return unused

        lax.fori_loop(0, batch, weights, 0)

        for k in range(batch):
            tile = first + k
            span = slice(k * TILE_PIXELS, (k + 1) * TILE_PIXELS)
            pair = pair_ref[span, :]
            high, low = split_colours(splat_ref, tile)
            rendered = colour_sum(high, low, pair)
            wanted = targets_ref[tile]
            wanted = jnp.concatenate([wanted, jnp.zeros((5, TILE_PIXELS), f32)], axis=0)
            delta = rendered - wanted
            delta_high = delta.astype(bf16).astype(f32)
            delta_low = delta - delta_high
            left = jnp.concatenate(
                [delta_high, delta_high, delta_low, jnp.zeros_like(delta)], axis=0
            ).astype(bf16)
            right = jnp.concatenate([high, low, high, jnp.zeros_like(high)], axis=0).astype(bf16)
            plain_ref[span, :] = lax.dot_general(
                left, right, (((0,), (0,)), ((), ())), preferred_element_type=f32
            )
            colour = jnp.dot(
                jnp.concatenate([delta_high, delta_low], axis=0).astype(bf16),
                pair,
                preferred_element_type=f32,
            )
            colour = colour[0:8, :LIST_LEN] + (colour[0:8, LIST_LEN:] + colour[8:16, :LIST_LEN])
            grad_ref[tile, 6:8, :] = colour[0:2]
            grad_last_ref[pl.ds(tile, 1), :] = colour[2:3]

        def pulls(k, unused):
            for row in range(tile_edge):
                where = pl.ds(pl.multiple_of(k * TILE_PIXELS, TILE_PIXELS) + row * tile_edge, tile_edge)
                product = plain_ref[where, :] * weight_ref[where, :]
                weight_ref[where, :] = product
                high, low = halves(product)
                grad_pair_ref[where, :LIST_LEN] = high
                grad_pair_ref[where, LIST_LEN:] = low
            return unused

        lax.fori_loop(0, batch, pulls, 0)
        plain_ref[...] = jnp.dot(grad_pair_ref[...], backward, preferred_element_type=f32)

        def moments(k, unused):
            tile = first + k
            base = pl.multiple_of(k * TILE_PIXELS, TILE_PIXELS)
            across, down = tile_offsets(splat_ref, tile, numbers_ref[tile])
            for h in range(2):
                row_ref[8 * h : 8 * h + 8, :] = down[h]
            sums = [[jnp.zeros((8, LANES), f32) for j in range(3)] for h in range(2)]
            for row in range(tile_edge):
                offset = spread_row(row_ref, row)
                for h in range(2):
                    where = pl.ds(base + row * tile_edge + 8 * h, 8)
                    slope = weight_ref[where, :] - plain_ref[where, :] * odds_ref[where, :]
                    once = slope * offset
                    sums[h][0] = sums[h][0] + slope
                    sums[h][1] = sums[h][1] + once
                    sums[h][2] = sums[h][2] + once * offset

            def total(parts):
                return jnp.sum(parts[0] + parts[1], axis=0, keepdims=True)

            whole = total([sums[h][0] for h in range(2)])
            along = [sums[h][0] * across[h] for h in range(2)]
            moment_x = total(along)
            moment_xx = total([along[h] * across[h] for h in range(2)])
            moment_y = total([sums[h][1] for h in range(2)])
            moment_xy = total([sums[h][1] * across[h] for h in range(2)])
            moment_yy = total([sums[h][2] for h in range(2)])
            a = splat_ref[tile, 2:3, :]
            b = splat_ref[tile, 3:4, :]
            c = splat_ref[tile, 4:5, :]
            grad_ref[tile, 0:1, :] = -(a * moment_x + b * moment_y)
            grad_ref[tile, 1:2, :] = -(c * moment_y + b * moment_x)
            grad_ref[tile, 2:3, :] = -0.5 * moment_xx
            grad_ref[tile, 3:4, :] = -moment_xy
            grad_ref[tile, 4:5, :] = -0.5 * moment_yy
            grad_ref[tile, 5:6, :] = whole
            return unused

        lax.fori_loop(0, batch, moments, 0)
        return unused

    lax.fori_loop(0, tile_count // batch, batch_step, 0)
    permute(
        inverse_ref,
        grad_ref,
        grad_last_ref,
        tile_count,
        out_packed_ref.shape[0],
        pack_group(out_packed_ref),
    )


def train(numbers, lists, targets, packed):
    tile_count = lists.shape[0]
    chunks = packed.shape[0]
    pixels = batch_tiles(tile_count) * TILE_PIXELS
    return pl.pallas_call(
        train_body,
        out_shape=jax.ShapeDtypeStruct(packed.shape, f32),
        in_specs=[SMEM, VMEM, VMEM, VMEM],
        out_specs=VMEM,
        scratch_shapes=[
            pltpu.VMEM((chunks, 8, LANES), f32),
            pltpu.VMEM((chunks, LANES), f32),
            pltpu.VMEM((tile_count, 16, LANES), f32),
            pltpu.VMEM((32, LANES), f32),
            pltpu.VMEM((pixels, LIST_LEN), f32),
            pltpu.VMEM((pixels, LIST_LEN), f32),
            pltpu.VMEM((pixels, LIST_LEN), f32),
            pltpu.VMEM((pixels, LIST_LEN), f32),
            pltpu.VMEM((pixels, 2 * LIST_LEN), bf16),
            pltpu.VMEM((pixels, 2 * LIST_LEN), bf16),
            pltpu.VMEM((tile_count, 8, LANES), f32),
            pltpu.VMEM((tile_count, LANES), f32),
            pltpu.VMEM((chunks, LANES), jnp.int32),
        ],
        name="train_tiles",
    )(numbers, lists, targets, packed)


def render_body(
    numbers_ref,
    lists_ref,
    packed_ref,
    out_ref,
    main_ref,
    last_ref,
    splat_ref,
    row_ref,
    alpha_ref,
    plain_ref,
    pair_ref,
):
    tile_count = lists_ref.shape[0]
    batch = batch_tiles(tile_count)
    gather_tiles(lists_ref, packed_ref, main_ref, last_ref, splat_ref)
    forward = triangle_pair(True)

    def batch_step(step, unused):
        first = step * batch

        def alphas(k, unused):
            tile = first + k
            base = pl.multiple_of(k * TILE_PIXELS, TILE_PIXELS)
            alpha_phase(splat_ref, tile, numbers_ref[tile], base, row_ref, alpha_ref, None, pair_ref)
            return unused

        lax.fori_loop(0, batch, alphas, 0)
        plain_ref[...] = jnp.dot(pair_ref[...], forward, preferred_element_type=f32)

        def weights(k, unused):
            base = pl.multiple_of(k * TILE_PIXELS, TILE_PIXELS)
            weight_phase(base, plain_ref, alpha_ref, None, pair_ref)
            return unused

        lax.fori_loop(0, batch, weights, 0)
        for k in range(batch):
            tile = first + k
            high, low = split_colours(splat_ref, tile)
            pair = pair_ref[k * TILE_PIXELS : (k + 1) * TILE_PIXELS, :]
            out_ref[tile] = colour_sum(high, low, pair)[0:3]
        return unused

    lax.fori_loop(0, tile_count // batch, batch_step, 0)


def render(numbers, lists, packed):
    tile_count = lists.shape[0]
    chunks = packed.shape[0]
    pixels = batch_tiles(tile_count) * TILE_PIXELS
    return pl.pallas_call(
        render_body,
        out_shape=jax.ShapeDtypeStruct((tile_count, 3, TILE_PIXELS), f32),
        in_specs=[SMEM, VMEM, VMEM],
        out_specs=VMEM,
        scratch_shapes=[
            pltpu.VMEM((chunks, 8, LANES), f32),
            pltpu.VMEM((chunks, LANES), f32),
            pltpu.VMEM((tile_count, 16, LANES), f32),
            pltpu.VMEM((32, LANES), f32),
            pltpu.VMEM((pixels, LIST_LEN), f32),
            pltpu.VMEM((pixels, LIST_LEN), f32),
            pltpu.VMEM((pixels, 2 * LIST_LEN), bf16),
        ],
        name="render_tiles",
    )(numbers, lists, packed)


def exchange(packed, devices):
    rows = packed.shape[0]
    if rows == devices:
        return lax.all_to_all(packed, "dev", split_axis=0, concat_axis=0, tiled=True)
    cap = rows * LANES // devices
    slots = packed.reshape(rows, ROWS, LANES).transpose(1, 0, 2).reshape(ROWS, devices, cap)
    slots = lax.all_to_all(slots, "dev", split_axis=1, concat_axis=1, tiled=True)
    slots = slots.reshape(ROWS, rows, LANES).transpose(1, 0, 2)
    return slots.reshape(rows, 1, ROWS * LANES)


def shards(
    gauss_params,
    adam_first,
    adam_second,
    camera,
    send_first,
    send_second,
    lists_first,
    lists_second,
    tiles_first,
    tiles_second,
    targets,
):
    devices = lax.axis_size("dev")
    half_width = 0.5 * TILES_X * tile_edge
    half_height = 0.5 * (lists_first.shape[0] * devices // TILES_X * tile_edge)
    packed = first_owner(camera, gauss_params, send_first, half_width, half_height)
    packed = exchange(packed, devices)
    packed = train(tiles_first, lists_first, targets, packed)
    packed = exchange(packed, devices)
    new_params, new_first, new_second, packed = second_owner(
        camera,
        gauss_params,
        adam_first,
        adam_second,
        send_first,
        send_second,
        packed,
        half_width,
        half_height,
    )
    packed = exchange(packed, devices)
    rendered = render(tiles_second, lists_second, packed)
    return (new_params, new_first, new_second, rendered)


def solution(mesh):
    placed = (
        P(None, "dev"),
        P(None, "dev"),
        P(None, "dev"),
        P(),
        P("dev", None),
        P("dev", None),
        P("dev", None),
        P("dev", None),
        P("dev"),
        P("dev"),
        P("dev", None, None),
    )
    return jax.shard_map(
        shards,
        mesh=mesh,
        in_specs=placed,
        out_specs=(P(None, "dev"), P(None, "dev"), P(None, "dev"), P("dev", None, None)),
        check_vma=False,
    )
```

```python
import functools

import jax
import jax.numpy as jnp
import numpy as np
from jax import lax
from jax.experimental import pallas as pl
from jax.experimental.pallas import tpu as pltpu
from jax.sharding import PartitionSpec as P

PARAMS = 59
LIST_LEN = 128
TILE_PIXELS = 256
TILES_X = 128
LANES = 128
ROWS = 9
STRIDE = 72

tile_edge = 16
focal_length = 1000.0
blur_floor = 0.3
adam_epsilon = 1e-08
bias_first = 1.0 - 0.9**20
bias_second = 1.0 - 0.999**20
sh_first = 0.28209479177387814
sh_second = 0.4886025119029199
sh_third = (
    1.0925484305920792,
    -1.0925484305920792,
    0.31539156525252005,
    -1.0925484305920792,
    0.5462742152960396,
)
sh_fourth = (
    -0.5900435899266435,
    2.890611442640554,
    -0.4570457994644658,
    0.3731763325901154,
    -0.4570457994644658,
    1.445305721320277,
    -0.5900435899266435,
)

f32 = jnp.float32
bf16 = jnp.bfloat16
VMEM = pl.BlockSpec(memory_space=pltpu.VMEM)
SMEM = pl.BlockSpec(memory_space=pltpu.SMEM)
ANY = pl.BlockSpec(memory_space=pl.ANY)


def rate_values():
    values = np.full((64,), 0.000125)
    values[0:3] = 0.00016
    values[3:6] = 0.005
    values[6:10] = 0.001
    values[10] = 0.05
    values[11] = 0.0025
    values[27] = 0.0025
    values[43] = 0.0025
    return values


def camera_frame(camera_ref, view):
    shape = (8, LANES)
    angle = [jnp.full(shape, camera_ref[view, k], f32) for k in range(3)]
    shift = [jnp.full(shape, camera_ref[view, 3 + k], f32) for k in range(3)]
    (ca, cb, cc) = [jnp.cos(x) for x in angle]
    (sa, sb, sc) = [jnp.sin(x) for x in angle]
    rot = [
        [cc * cb, cc * sb * sa - sc * ca, cc * sb * ca + sc * sa],
        [sc * cb, sc * sb * sa + cc * ca, sc * sb * ca - cc * sa],
        [-sb, cb * sa, cb * ca],
    ]
    back = [
        rot[0][k] * shift[0] + rot[1][k] * shift[1] + rot[2][k] * shift[2]
        for k in range(3)
    ]
    return rot, shift, back


def sh_terms(x, y, z):
    xx, yy, zz = (x * x, y * y, z * z)
    return [
        -sh_second * y,
        sh_second * z,
        -sh_second * x,
        sh_third[0] * x * y,
        sh_third[1] * y * z,
        sh_third[2] * (2.0 * zz - xx - yy),
        sh_third[3] * x * z,
        sh_third[4] * (xx - yy),
        sh_fourth[0] * y * (3.0 * xx - yy),
        sh_fourth[1] * x * y * z,
        sh_fourth[2] * y * (4.0 * zz - xx - yy),
        sh_fourth[3] * z * (2.0 * zz - 3.0 * xx - 3.0 * yy),
        sh_fourth[4] * x * (4.0 * zz - xx - yy),
        sh_fourth[5] * z * (xx - yy),
        sh_fourth[6] * x * (xx - 3.0 * yy),
    ]


def project(params, frame, half_width, half_height):
    rot, shift, back = frame
    centres = params[0:3]
    viewed = [
        rot[k][0] * centres[0] + rot[k][1] * centres[1] + rot[k][2] * centres[2] + shift[k]
        for k in range(3)
    ]
    inverse = 1.0 / viewed[2]
    scale_z = focal_length * inverse
    u_off = scale_z * viewed[0]
    w_off = scale_z * viewed[1]
    slope_u = u_off * inverse
    slope_w = w_off * inverse
    scales = [jnp.exp(params[3 + k]) for k in range(3)]
    q = params[6:10]
    norm = lax.rsqrt(q[0] * q[0] + q[1] * q[1] + q[2] * q[2] + q[3] * q[3])
    qw, qx, qy, qz = [v * norm for v in q]
    turn = [
        [
            1.0 - 2.0 * (qy * qy + qz * qz),
            2.0 * (qx * qy - qw * qz),
            2.0 * (qx * qz + qw * qy),
        ],
        [
            2.0 * (qx * qy + qw * qz),
            1.0 - 2.0 * (qx * qx + qz * qz),
            2.0 * (qy * qz - qw * qx),
        ],
        [
            2.0 * (qx * qz - qw * qy),
            2.0 * (qy * qz + qw * qx),
            1.0 - 2.0 * (qx * qx + qy * qy),
        ],
    ]
    mapping = [
        [scale_z * rot[0][k] - slope_u * rot[2][k] for k in range(3)],
        [scale_z * rot[1][k] - slope_w * rot[2][k] for k in range(3)],
    ]
    factor = [
        [
            (row[0] * turn[0][k] + row[1] * turn[1][k] + row[2] * turn[2][k]) * scales[k]
            for k in range(3)
        ]
        for row in mapping
    ]
    first, second = factor
    cover_a = first[0] * first[0] + first[1] * first[1] + first[2] * first[2] + blur_floor
    cover_b = first[0] * second[0] + first[1] * second[1] + first[2] * second[2]
    cover_c = second[0] * second[0] + second[1] * second[1] + second[2] * second[2] + blur_floor
    scale_det = 1.0 / (cover_a * cover_c - cover_b * cover_b)
    opacity = 1.0 / (1.0 + jnp.exp(-params[10]))
    towards = [centres[k] + back[k] for k in range(3)]
    length = lax.rsqrt(
        towards[0] * towards[0] + towards[1] * towards[1] + towards[2] * towards[2]
    )
    harmonics = sh_terms(*[v * length for v in towards])
    colours = []
    for channel in range(3):
        running = 0.5 + sh_first * params[11 + 16 * channel]
        for term in range(15):
            running = running + harmonics[term] * params[12 + 16 * channel + term]
        colours.append(jnp.maximum(running, 0.0))
    return [
        u_off + half_width,
        w_off + half_height,
        cover_c * scale_det,
        -cover_b * scale_det,
        cover_a * scale_det,
        opacity,
    ] + colours


def permute(idx_ref, main_ref, last_ref, chunks, rows, write):
    def group_step(group, unused):
        base = pl.multiple_of(group * 8, 8)
        index = idx_ref[pl.ds(base, 8), :]
        high = index >> 7
        low = index & 127
        totals = []
        for k in range(8):
            row_high = jnp.broadcast_to(high[k : k + 1], (8, LANES))
            row_low = jnp.broadcast_to(low[k : k + 1], (8, LANES))
            total = jnp.zeros((8, LANES), f32)
            for chunk in range(chunks):
                found = jnp.take_along_axis(
                    main_ref[chunk], row_low, axis=1, mode="promise_in_bounds"
                )
                total = jnp.where(row_high == chunk, found, total)
            totals.append(total)
        total = jnp.zeros((8, LANES), f32)
        for chunk in range(chunks):
            source = jnp.broadcast_to(last_ref[chunk : chunk + 1, :], (8, LANES))
            found = jnp.take_along_axis(source, low, axis=1, mode="promise_in_bounds")
            total = jnp.where(high == chunk, found, total)
        totals.append(total)
        write(group, totals[:8], totals[8])
        return unused

    lax.fori_loop(0, rows // 8, group_step, 0)


def invert(idx_ref, rows, high_count, inverse_ref):
    index = idx_ref[...]
    high = index >> 7
    low = index & 127
    high_ids = lax.broadcasted_iota(jnp.int32, (high_count, LANES), 0)
    low_ids = lax.broadcasted_iota(jnp.int32, (LANES, LANES), 0)
    lane_ids = lax.broadcasted_iota(jnp.int32, (high_count, LANES), 1).astype(f32)
    total = jnp.zeros((2 * high_count, LANES), f32)
    for start in range(0, rows, 8):
        left = []
        right = []
        for row in range(start, start + 8):
            here = high[row : row + 1] == high_ids
            left.append(
                jnp.concatenate(
                    [jnp.where(here, row + 1.0, 0.0), jnp.where(here, lane_ids, 0.0)], axis=0
                ).astype(bf16)
            )
            right.append(jnp.where(low[row : row + 1] == low_ids, 1.0, 0.0).astype(bf16))
        total = total + lax.dot_general(
            jnp.concatenate(left, axis=1),
            jnp.concatenate(right, axis=1),
            (((1,), (1,)), ((), ())),
            preferred_element_type=f32,
        )
    rows_found = total[:high_count].astype(jnp.int32)
    lanes_found = total[high_count:].astype(jnp.int32)
    inverse_ref[...] = (rows_found - 1) * LANES + lanes_found


def unpack(packed_ref, main_ref, last_ref, chunks):
    for chunk in range(chunks):
        for k in range(8):
            main_ref[chunk, k : k + 1, :] = packed_ref[chunk, :, k * LANES : (k + 1) * LANES]
        last_ref[chunk : chunk + 1, :] = packed_ref[chunk, :, 8 * LANES : 9 * LANES]


def pack_group(packed_ref):
    def write(group, vectors, last):
        for k in range(8):
            row = group * 8 + k
            for item in range(8):
                packed_ref[row, :, item * LANES : (item + 1) * LANES] = vectors[k][
                    item : item + 1
                ]
            packed_ref[row, :, 8 * LANES : 9 * LANES] = last[k : k + 1]

    return write


def slots_as_rows(slots_ref, idx_ref, rows):
    for row in range(rows):
        idx_ref[row : row + 1, :] = slots_ref[:, row * LANES : (row + 1) * LANES]


def to_dense(native, dense_ref, row_block, chunk):
    if native.shape[0] == 8:
        dense_ref[pl.ds(8 * row_block * STRIDE + chunk, 8, stride=STRIDE), :] = native
    else:
        for k in range(native.shape[0]):
            dense_ref[pl.ds((8 * row_block + k) * STRIDE + chunk, 1), :] = native[k : k + 1]


def dense_load(dense_ref, row, group):
    return dense_ref[pl.ds(pl.multiple_of(row * STRIDE + group * 8, 8), 8), :]


def dense_store(dense_ref, row, group, value):
    dense_ref[pl.ds(pl.multiple_of(row * STRIDE + group * 8, 8), 8), :] = value


def row_blocks():
    return [(block, min(8, PARAMS - 8 * block)) for block in range((PARAMS + 7) // 8)]


def project_groups(dense_ref, splat_ref, frame, half_width, half_height, chunks):
    def step(group, unused):
        params = [dense_load(dense_ref, row, group) for row in range(PARAMS)]
        for row, value in enumerate(project(params, frame, half_width, half_height)):
            dense_store(splat_ref, row, group, value)
        return unused

    lax.fori_loop(0, chunks // 8, step, 0)


def send_splats(splat_ref, main_ref, idx_ref, packed_ref, chunks, rows):
    for chunk in range(chunks):
        main_ref[chunk] = splat_ref[pl.ds(chunk, 8, stride=STRIDE), :]
    last_ref = splat_ref.at[pl.ds(8 * STRIDE, chunks), :]
    permute(idx_ref, main_ref, last_ref, chunks, rows, pack_group(packed_ref))


def first_owner_body(
    half_width,
    half_height,
    camera_ref,
    params_ref,
    slots_ref,
    packed_ref,
    dense_ref,
    splat_ref,
    main_ref,
    idx_ref,
):
    chunks = params_ref.shape[1] // LANES
    rows = slots_ref.shape[1] // LANES
    slots_as_rows(slots_ref, idx_ref, rows)

    def relayout(chunk, unused):
        lanes = pl.ds(pl.multiple_of(chunk * LANES, LANES), LANES)
        for block, size in row_blocks():
            to_dense(params_ref[8 * block : 8 * block + size, lanes], dense_ref, block, chunk)
        return unused

    lax.fori_loop(0, chunks, relayout, 0, unroll=4)
    frame = camera_frame(camera_ref, 0)
    project_groups(dense_ref, splat_ref, frame, half_width, half_height, chunks)
    send_splats(splat_ref, main_ref, idx_ref, packed_ref, chunks, rows)


def first_owner(camera, params, slots, half_width, half_height):
    chunks = params.shape[1] // LANES
    rows = slots.shape[1] // LANES
    return pl.pallas_call(
        functools.partial(first_owner_body, half_width, half_height),
        out_shape=jax.ShapeDtypeStruct((rows, 1, ROWS * LANES), f32),
        in_specs=[SMEM, VMEM, VMEM],
        out_specs=VMEM,
        scratch_shapes=[
            pltpu.VMEM((64 * STRIDE, LANES), f32),
            pltpu.VMEM((ROWS * STRIDE, LANES), f32),
            pltpu.VMEM((chunks, 8, LANES), f32),
            pltpu.VMEM((rows, LANES), jnp.int32),
        ],
        name="first_owner",
    )(camera, params, slots)


def second_owner_body(
    half_width,
    half_height,
    camera_ref,
    params_ref,
    first_hbm,
    second_hbm,
    slots_ref,
    next_slots_ref,
    packed_ref,
    out_params_hbm,
    out_first_hbm,
    out_second_hbm,
    out_packed_ref,
    dense_ref,
    grad_ref,
    splat_ref,
    main_ref,
    last_ref,
    idx_ref,
    inverse_ref,
    params_out_ref,
    first_ref,
    second_ref,
    load_sems,
    store_sems,
):
    chunks = params_ref.shape[1] // LANES
    rows = slots_ref.shape[1] // LANES
    loads = [
        pltpu.make_async_copy(first_hbm, first_ref, load_sems.at[0]),
        pltpu.make_async_copy(second_hbm, second_ref, load_sems.at[1]),
    ]
    for copy in loads:
        copy.start()
    slots_as_rows(slots_ref, idx_ref, rows)
    invert(idx_ref, rows, chunks, inverse_ref)
    unpack(packed_ref, main_ref, last_ref, rows)

    def relayout(chunk, unused):
        lanes = pl.ds(pl.multiple_of(chunk * LANES, LANES), LANES)
        for block, size in row_blocks():
            to_dense(params_ref[8 * block : 8 * block + size, lanes], dense_ref, block, chunk)
        return unused

    lax.fori_loop(0, chunks, relayout, 0, unroll=4)

    def write_columns(group, vectors, last):
        for k in range(8):
            splat_ref[pl.ds(group * 8 + k, 8, stride=STRIDE), :] = vectors[k]
        dense_store(splat_ref, 8, group, last)

    permute(inverse_ref, main_ref, last_ref, rows, chunks, write_columns)

    frame = camera_frame(camera_ref, 0)

    def pull_step(group, unused):
        params = [dense_load(dense_ref, row, group) for row in range(PARAMS)]
        splats, pullback = jax.vjp(
            lambda *p: project(list(p), frame, half_width, half_height), *params
        )
        cotangents = [dense_load(splat_ref, row, group) for row in range(ROWS)]
        through_opacity = cotangents[5] * (1.0 - splats[5])
        cotangents[5] = jnp.zeros_like(cotangents[5])
        grads = list(pullback(cotangents))
        grads[10] = through_opacity
        for row, value in enumerate(grads):
            dense_store(grad_ref, row, group, value)
        return unused

    lax.fori_loop(0, chunks // 8, pull_step, 0)

    for copy in loads:
        copy.wait()
    rates = rate_values() / bias_first
    stores = []
    row_ids = lax.broadcasted_iota(jnp.int32, (8, LANES), 0)
    for block, size in row_blocks():
        span = slice(8 * block, 8 * block + size)
        block_rates = rates[8 * block : 8 * block + 8]
        step_size = jnp.full((8, LANES), block_rates[0], f32)
        for k in range(1, 8):
            if block_rates[k] != block_rates[0]:
                step_size = jnp.where(row_ids == k, f32(block_rates[k]), step_size)
        step_size = step_size[:size]

        def adam_step(chunk, unused, block=block, size=size, span=span, step_size=step_size):
            lanes = pl.ds(pl.multiple_of(chunk * LANES, LANES), LANES)
            gradient = grad_ref[pl.ds(8 * block * STRIDE + chunk, 8, stride=STRIDE), :][:size]
            moment = 0.9 * first_ref[span, lanes] + 0.1 * gradient
            square = 0.999 * second_ref[span, lanes] + 0.001 * gradient * gradient
            scaled = square * (1.0 / bias_second)
            root = scaled * lax.rsqrt(scaled)
            fresh = params_ref[span, lanes] - step_size * moment / (root + adam_epsilon)
            first_ref[span, lanes] = moment
            second_ref[span, lanes] = square
            params_out_ref[span, lanes] = fresh
            to_dense(fresh, dense_ref, block, chunk)
            return unused

        lax.fori_loop(0, chunks, adam_step, 0, unroll=8)
        for number, (source, target) in enumerate(
            [
                (params_out_ref, out_params_hbm),
                (first_ref, out_first_hbm),
                (second_ref, out_second_hbm),
            ]
        ):
            copy = pltpu.make_async_copy(
                source.at[span, :], target.at[span, :], store_sems.at[number, block]
            )
            copy.start()
            stores.append(copy)

    slots_as_rows(next_slots_ref, idx_ref, rows)
    frame = camera_frame(camera_ref, 1)
    project_groups(dense_ref, splat_ref, frame, half_width, half_height, chunks)
    send_splats(splat_ref, main_ref, idx_ref, out_packed_ref, chunks, rows)
    for copy in stores:
        copy.wait()


def second_owner(camera, params, first, second, slots, next_slots, packed, half_width, half_height):
    chunks = params.shape[1] // LANES
    rows = slots.shape[1] // LANES
    shape = jax.ShapeDtypeStruct(params.shape, f32)
    return pl.pallas_call(
        functools.partial(second_owner_body, half_width, half_height),
        out_shape=(shape, shape, shape, jax.ShapeDtypeStruct((rows, 1, ROWS * LANES), f32)),
        in_specs=[SMEM, VMEM, ANY, ANY, VMEM, VMEM, VMEM],
        out_specs=(ANY, ANY, ANY, VMEM),
        scratch_shapes=[
            pltpu.VMEM((64 * STRIDE, LANES), f32),
            pltpu.VMEM((64 * STRIDE, LANES), f32),
            pltpu.VMEM((ROWS * STRIDE, LANES), f32),
            pltpu.VMEM((max(chunks, rows), 8, LANES), f32),
            pltpu.VMEM((rows, LANES), f32),
            pltpu.VMEM((rows, LANES), jnp.int32),
            pltpu.VMEM((chunks, LANES), jnp.int32),
            pltpu.VMEM(params.shape, f32),
            pltpu.VMEM(params.shape, f32),
            pltpu.VMEM(params.shape, f32),
            pltpu.SemaphoreType.DMA((2,)),
            pltpu.SemaphoreType.DMA((3, 8)),
        ],
        name="second_owner",
    )(camera, params, first, second, slots, next_slots, packed)


def halves(value):
    high = value.astype(bf16)
    return high, (value - high.astype(f32)).astype(bf16)


def triangle_pair(forward):
    rows = lax.broadcasted_iota(jnp.int32, (LIST_LEN, LIST_LEN), 0)
    cols = lax.broadcasted_iota(jnp.int32, (LIST_LEN, LIST_LEN), 1)
    chosen = rows < cols if forward else rows > cols
    one = jnp.where(chosen, 1.0, 0.0).astype(bf16)
    return jnp.concatenate([one, one], axis=0)


def batch_tiles(tile_count):
    return 8 if tile_count % 8 == 0 else 1


def tile_offsets(splat_ref, tile, number):
    left = (number % TILES_X) * tile_edge
    top = (number // TILES_X) * tile_edge
    ids = lax.broadcasted_iota(jnp.int32, (8, LANES), 0)
    u = jnp.broadcast_to(splat_ref[tile, 0:1, :], (8, LANES))
    w = jnp.broadcast_to(splat_ref[tile, 1:2, :], (8, LANES))
    across = [u - ((ids + (left + 8 * h)).astype(f32) + 0.5) for h in range(2)]
    down = [w - ((ids + (top + 8 * h)).astype(f32) + 0.5) for h in range(2)]
    return across, down


def spread_row(ref, row):
    return jnp.broadcast_to(ref[row : row + 1, :], (8, LANES))


def alpha_phase(splat_ref, tile, number, base, row_ref, alpha_ref, odds_ref, pair_ref):
    a, b, c, o = [jnp.broadcast_to(splat_ref[tile, k : k + 1, :], (8, LANES)) for k in (2, 3, 4, 5)]
    across, down = tile_offsets(splat_ref, tile, number)
    along = [(-0.5 * a) * x * x for x in across]
    for h in range(2):
        row_ref[8 * h : 8 * h + 8, :] = (-0.5 * c) * down[h] * down[h]
        row_ref[16 + 8 * h : 24 + 8 * h, :] = -(b * down[h])
    for row in range(tile_edge):
        fixed = spread_row(row_ref, row)
        slope = spread_row(row_ref, 16 + row)
        logs = []
        for h in range(2):
            exponent = along[h] + (fixed + slope * across[h])
            alpha = o * jnp.exp(exponent)
            log_clear = jnp.log(1.0 - alpha)
            where = pl.ds(base + row * tile_edge + 8 * h, 8)
            alpha_ref[where, :] = alpha
            if odds_ref is not None:
                odds_ref[where, :] = alpha * jnp.exp(-log_clear)
            logs.append(log_clear)
        high, low = halves(jnp.concatenate(logs, axis=0))
        where = pl.ds(base + row * tile_edge, tile_edge)
        pair_ref[where, :LIST_LEN] = high
        pair_ref[where, LIST_LEN:] = low


def weight_phase(base, before_ref, alpha_ref, weight_ref, pair_ref):
    for row in range(tile_edge):
        where = pl.ds(base + row * tile_edge, tile_edge)
        weight = alpha_ref[where, :] * jnp.exp(before_ref[where, :])
        if weight_ref is not None:
            weight_ref[where, :] = weight
        high, low = halves(weight)
        pair_ref[where, :LIST_LEN] = high
        pair_ref[where, LIST_LEN:] = low


def split_colours(splat_ref, tile):
    colours = splat_ref[tile, 6:14, :]
    high = colours.astype(bf16).astype(f32)
    return high, colours - high


def colour_sum(high, low, pair):
    upper = jnp.concatenate([high, high], axis=1)
    lower = jnp.concatenate([low, jnp.zeros_like(low)], axis=1)
    result = lax.dot_general(
        jnp.concatenate([upper, lower], axis=0).astype(bf16),
        pair,
        (((1,), (1,)), ((), ())),
        preferred_element_type=f32,
    )
    return result[0:8] + result[8:16]


def gather_tiles(lists_ref, packed_ref, main_ref, last_ref, splat_ref):
    chunks = packed_ref.shape[0]
    tile_count = lists_ref.shape[0]
    unpack(packed_ref, main_ref, last_ref, chunks)

    def write(group, vectors, last):
        for k in range(8):
            tile = group * 8 + k
            splat_ref[tile, 0:8, :] = vectors[k]
            splat_ref[tile, 8:9, :] = last[k : k + 1]
            splat_ref[tile, 9:16, :] = jnp.zeros((7, LANES), f32)

    permute(lists_ref, main_ref, last_ref, chunks, tile_count, write)


def train_body(
    numbers_ref,
    lists_ref,
    targets_ref,
    packed_ref,
    out_packed_ref,
    main_ref,
    last_ref,
    splat_ref,
    row_ref,
    alpha_ref,
    odds_ref,
    plain_ref,
    weight_ref,
    pair_ref,
    grad_pair_ref,
    grad_ref,
    grad_last_ref,
    inverse_ref,
):
    tile_count = lists_ref.shape[0]
    batch = batch_tiles(tile_count)
    gather_tiles(lists_ref, packed_ref, main_ref, last_ref, splat_ref)
    invert(lists_ref, tile_count, packed_ref.shape[0], inverse_ref)
    forward = triangle_pair(True)
    backward = triangle_pair(False)

    def batch_step(step, unused):
        first = step * batch

        def alphas(k, unused):
            tile = first + k
            base = pl.multiple_of(k * TILE_PIXELS, TILE_PIXELS)
            alpha_phase(
                splat_ref, tile, numbers_ref[tile], base, row_ref, alpha_ref, odds_ref, pair_ref
            )
            return unused

        lax.fori_loop(0, batch, alphas, 0)
        plain_ref[...] = jnp.dot(pair_ref[...], forward, preferred_element_type=f32)

        def weights(k, unused):
            base = pl.multiple_of(k * TILE_PIXELS, TILE_PIXELS)
            weight_phase(base, plain_ref, alpha_ref, weight_ref, pair_ref)
            return unused

        lax.fori_loop(0, batch, weights, 0)

        for k in range(batch):
            tile = first + k
            span = slice(k * TILE_PIXELS, (k + 1) * TILE_PIXELS)
            pair = pair_ref[span, :]
            high, low = split_colours(splat_ref, tile)
            rendered = colour_sum(high, low, pair)
            wanted = [targets_ref[channel, pl.ds(tile, 1), :] for channel in range(3)]
            wanted = jnp.concatenate(wanted + [jnp.zeros((5, TILE_PIXELS), f32)], axis=0)
            delta = rendered - wanted
            delta_high = delta.astype(bf16).astype(f32)
            delta_low = delta - delta_high
            left = jnp.concatenate(
                [delta_high, delta_high, delta_low, jnp.zeros_like(delta)], axis=0
            ).astype(bf16)
            right = jnp.concatenate([high, low, high, jnp.zeros_like(high)], axis=0).astype(bf16)
            plain_ref[span, :] = lax.dot_general(
                left, right, (((0,), (0,)), ((), ())), preferred_element_type=f32
            )
            colour = jnp.dot(
                jnp.concatenate([delta_high, delta_low], axis=0).astype(bf16),
                pair,
                preferred_element_type=f32,
            )
            colour = colour[0:8, :LIST_LEN] + (colour[0:8, LIST_LEN:] + colour[8:16, :LIST_LEN])
            grad_ref[tile, 6:8, :] = colour[0:2]
            grad_last_ref[pl.ds(tile, 1), :] = colour[2:3]

        def pulls(k, unused):
            for row in range(tile_edge):
                where = pl.ds(pl.multiple_of(k * TILE_PIXELS, TILE_PIXELS) + row * tile_edge, tile_edge)
                product = plain_ref[where, :] * weight_ref[where, :]
                weight_ref[where, :] = product
                high, low = halves(product)
                grad_pair_ref[where, :LIST_LEN] = high
                grad_pair_ref[where, LIST_LEN:] = low
            return unused

        lax.fori_loop(0, batch, pulls, 0)
        plain_ref[...] = jnp.dot(grad_pair_ref[...], backward, preferred_element_type=f32)

        def moments(k, unused):
            tile = first + k
            base = pl.multiple_of(k * TILE_PIXELS, TILE_PIXELS)
            across, down = tile_offsets(splat_ref, tile, numbers_ref[tile])
            for h in range(2):
                row_ref[8 * h : 8 * h + 8, :] = down[h]
            sums = [[jnp.zeros((8, LANES), f32) for j in range(3)] for h in range(2)]
            for row in range(tile_edge):
                offset = spread_row(row_ref, row)
                for h in range(2):
                    where = pl.ds(base + row * tile_edge + 8 * h, 8)
                    slope = weight_ref[where, :] - plain_ref[where, :] * odds_ref[where, :]
                    once = slope * offset
                    sums[h][0] = sums[h][0] + slope
                    sums[h][1] = sums[h][1] + once
                    sums[h][2] = sums[h][2] + once * offset

            def total(parts):
                return jnp.sum(parts[0] + parts[1], axis=0, keepdims=True)

            whole = total([sums[h][0] for h in range(2)])
            along = [sums[h][0] * across[h] for h in range(2)]
            moment_x = total(along)
            moment_xx = total([along[h] * across[h] for h in range(2)])
            moment_y = total([sums[h][1] for h in range(2)])
            moment_xy = total([sums[h][1] * across[h] for h in range(2)])
            moment_yy = total([sums[h][2] for h in range(2)])
            a = splat_ref[tile, 2:3, :]
            b = splat_ref[tile, 3:4, :]
            c = splat_ref[tile, 4:5, :]
            grad_ref[tile, 0:1, :] = -(a * moment_x + b * moment_y)
            grad_ref[tile, 1:2, :] = -(c * moment_y + b * moment_x)
            grad_ref[tile, 2:3, :] = -0.5 * moment_xx
            grad_ref[tile, 3:4, :] = -moment_xy
            grad_ref[tile, 4:5, :] = -0.5 * moment_yy
            grad_ref[tile, 5:6, :] = whole
            return unused

        lax.fori_loop(0, batch, moments, 0)
        return unused

    lax.fori_loop(0, tile_count // batch, batch_step, 0)
    permute(
        inverse_ref,
        grad_ref,
        grad_last_ref,
        tile_count,
        out_packed_ref.shape[0],
        pack_group(out_packed_ref),
    )


def train(numbers, lists, targets, packed):
    tile_count = lists.shape[0]
    chunks = packed.shape[0]
    pixels = batch_tiles(tile_count) * TILE_PIXELS
    return pl.pallas_call(
        train_body,
        out_shape=jax.ShapeDtypeStruct(packed.shape, f32),
        in_specs=[SMEM, VMEM, VMEM, VMEM],
        out_specs=VMEM,
        scratch_shapes=[
            pltpu.VMEM((chunks, 8, LANES), f32),
            pltpu.VMEM((chunks, LANES), f32),
            pltpu.VMEM((tile_count, 16, LANES), f32),
            pltpu.VMEM((32, LANES), f32),
            pltpu.VMEM((pixels, LIST_LEN), f32),
            pltpu.VMEM((pixels, LIST_LEN), f32),
            pltpu.VMEM((pixels, LIST_LEN), f32),
            pltpu.VMEM((pixels, LIST_LEN), f32),
            pltpu.VMEM((pixels, 2 * LIST_LEN), bf16),
            pltpu.VMEM((pixels, 2 * LIST_LEN), bf16),
            pltpu.VMEM((tile_count, 8, LANES), f32),
            pltpu.VMEM((tile_count, LANES), f32),
            pltpu.VMEM((chunks, LANES), jnp.int32),
        ],
        name="train_tiles",
    )(numbers, lists, targets, packed)


def render_body(
    numbers_ref,
    lists_ref,
    packed_ref,
    out_ref,
    main_ref,
    last_ref,
    splat_ref,
    row_ref,
    alpha_ref,
    plain_ref,
    pair_ref,
):
    tile_count = lists_ref.shape[0]
    batch = batch_tiles(tile_count)
    gather_tiles(lists_ref, packed_ref, main_ref, last_ref, splat_ref)
    forward = triangle_pair(True)

    def batch_step(step, unused):
        first = step * batch

        def alphas(k, unused):
            tile = first + k
            base = pl.multiple_of(k * TILE_PIXELS, TILE_PIXELS)
            alpha_phase(splat_ref, tile, numbers_ref[tile], base, row_ref, alpha_ref, None, pair_ref)
            return unused

        lax.fori_loop(0, batch, alphas, 0)
        plain_ref[...] = jnp.dot(pair_ref[...], forward, preferred_element_type=f32)

        def weights(k, unused):
            base = pl.multiple_of(k * TILE_PIXELS, TILE_PIXELS)
            weight_phase(base, plain_ref, alpha_ref, None, pair_ref)
            return unused

        lax.fori_loop(0, batch, weights, 0)
        for k in range(batch):
            tile = first + k
            high, low = split_colours(splat_ref, tile)
            pair = pair_ref[k * TILE_PIXELS : (k + 1) * TILE_PIXELS, :]
            rendered = colour_sum(high, low, pair)
            for channel in range(3):
                out_ref[channel, pl.ds(tile, 1), :] = rendered[channel : channel + 1]
        return unused

    lax.fori_loop(0, tile_count // batch, batch_step, 0)


def render(numbers, lists, packed):
    tile_count = lists.shape[0]
    chunks = packed.shape[0]
    pixels = batch_tiles(tile_count) * TILE_PIXELS
    return pl.pallas_call(
        render_body,
        out_shape=jax.ShapeDtypeStruct((3, tile_count, TILE_PIXELS), f32),
        in_specs=[SMEM, VMEM, VMEM],
        out_specs=VMEM,
        scratch_shapes=[
            pltpu.VMEM((chunks, 8, LANES), f32),
            pltpu.VMEM((chunks, LANES), f32),
            pltpu.VMEM((tile_count, 16, LANES), f32),
            pltpu.VMEM((32, LANES), f32),
            pltpu.VMEM((pixels, LIST_LEN), f32),
            pltpu.VMEM((pixels, LIST_LEN), f32),
            pltpu.VMEM((pixels, 2 * LIST_LEN), bf16),
        ],
        name="render_tiles",
    )(numbers, lists, packed)


def exchange(packed, devices):
    rows = packed.shape[0]
    if rows == devices:
        return lax.all_to_all(packed, "dev", split_axis=0, concat_axis=0, tiled=True)
    cap = rows * LANES // devices
    slots = packed.reshape(rows, ROWS, LANES).transpose(1, 0, 2).reshape(ROWS, devices, cap)
    slots = lax.all_to_all(slots, "dev", split_axis=1, concat_axis=1, tiled=True)
    slots = slots.reshape(ROWS, rows, LANES).transpose(1, 0, 2)
    return slots.reshape(rows, 1, ROWS * LANES)


def shards(
    gauss_params,
    adam_first,
    adam_second,
    camera,
    send_first,
    send_second,
    lists_first,
    lists_second,
    tiles_first,
    tiles_second,
    targets,
):
    devices = lax.axis_size("dev")
    half_width = 0.5 * TILES_X * tile_edge
    half_height = 0.5 * (lists_first.shape[0] * devices // TILES_X * tile_edge)
    packed = first_owner(camera, gauss_params, send_first, half_width, half_height)
    packed = exchange(packed, devices)
    packed = train(tiles_first, lists_first, jnp.transpose(targets, (1, 0, 2)), packed)
    packed = exchange(packed, devices)
    new_params, new_first, new_second, packed = second_owner(
        camera,
        gauss_params,
        adam_first,
        adam_second,
        send_first,
        send_second,
        packed,
        half_width,
        half_height,
    )
    packed = exchange(packed, devices)
    rendered = render(tiles_second, lists_second, packed)
    return (new_params, new_first, new_second, jnp.transpose(rendered, (1, 0, 2)))


def solution(mesh):
    placed = (
        P(None, "dev"),
        P(None, "dev"),
        P(None, "dev"),
        P(),
        P("dev", None),
        P("dev", None),
        P("dev", None),
        P("dev", None),
        P("dev"),
        P("dev"),
        P("dev", None, None),
    )
    return jax.shard_map(
        shards,
        mesh=mesh,
        in_specs=placed,
        out_specs=(P(None, "dev"), P(None, "dev"), P(None, "dev"), P("dev", None, None)),
        check_vma=False,
    )
```

```python
import functools

import jax
import jax.numpy as jnp
import numpy as np
from jax import lax
from jax.experimental import pallas as pl
from jax.experimental.pallas import tpu as pltpu
from jax.sharding import PartitionSpec as P

PARAMS = 59
LIST_LEN = 128
TILE_PIXELS = 256
TILES_X = 128
LANES = 128
ROWS = 9
STRIDE = 72
PARTS = 4

tile_edge = 16
focal_length = 1000.0
blur_floor = 0.3
adam_epsilon = 1e-08
bias_first = 1.0 - 0.9**20
bias_second = 1.0 - 0.999**20
sh_first = 0.28209479177387814
sh_second = 0.4886025119029199
sh_third = (
    1.0925484305920792,
    -1.0925484305920792,
    0.31539156525252005,
    -1.0925484305920792,
    0.5462742152960396,
)
sh_fourth = (
    -0.5900435899266435,
    2.890611442640554,
    -0.4570457994644658,
    0.3731763325901154,
    -0.4570457994644658,
    1.445305721320277,
    -0.5900435899266435,
)

f32 = jnp.float32
bf16 = jnp.bfloat16
VMEM = pl.BlockSpec(memory_space=pltpu.VMEM)
SMEM = pl.BlockSpec(memory_space=pltpu.SMEM)
ANY = pl.BlockSpec(memory_space=pl.ANY)


def rate_values():
    values = np.full((64,), 0.000125)
    values[0:3] = 0.00016
    values[3:6] = 0.005
    values[6:10] = 0.001
    values[10] = 0.05
    values[11] = 0.0025
    values[27] = 0.0025
    values[43] = 0.0025
    return values


def camera_frame(camera_ref, view):
    shape = (8, LANES)
    angle = [jnp.full(shape, camera_ref[view, k], f32) for k in range(3)]
    shift = [jnp.full(shape, camera_ref[view, 3 + k], f32) for k in range(3)]
    (ca, cb, cc) = [jnp.cos(x) for x in angle]
    (sa, sb, sc) = [jnp.sin(x) for x in angle]
    rot = [
        [cc * cb, cc * sb * sa - sc * ca, cc * sb * ca + sc * sa],
        [sc * cb, sc * sb * sa + cc * ca, sc * sb * ca - cc * sa],
        [-sb, cb * sa, cb * ca],
    ]
    back = [
        rot[0][k] * shift[0] + rot[1][k] * shift[1] + rot[2][k] * shift[2]
        for k in range(3)
    ]
    return rot, shift, back


def sh_terms(x, y, z):
    xx, yy, zz = (x * x, y * y, z * z)
    return [
        -sh_second * y,
        sh_second * z,
        -sh_second * x,
        sh_third[0] * x * y,
        sh_third[1] * y * z,
        sh_third[2] * (2.0 * zz - xx - yy),
        sh_third[3] * x * z,
        sh_third[4] * (xx - yy),
        sh_fourth[0] * y * (3.0 * xx - yy),
        sh_fourth[1] * x * y * z,
        sh_fourth[2] * y * (4.0 * zz - xx - yy),
        sh_fourth[3] * z * (2.0 * zz - 3.0 * xx - 3.0 * yy),
        sh_fourth[4] * x * (4.0 * zz - xx - yy),
        sh_fourth[5] * z * (xx - yy),
        sh_fourth[6] * x * (xx - 3.0 * yy),
    ]


def project(params, frame, half_width, half_height):
    rot, shift, back = frame
    centres = params[0:3]
    viewed = [
        rot[k][0] * centres[0] + rot[k][1] * centres[1] + rot[k][2] * centres[2] + shift[k]
        for k in range(3)
    ]
    inverse = 1.0 / viewed[2]
    scale_z = focal_length * inverse
    u_off = scale_z * viewed[0]
    w_off = scale_z * viewed[1]
    slope_u = u_off * inverse
    slope_w = w_off * inverse
    scales = [jnp.exp(params[3 + k]) for k in range(3)]
    q = params[6:10]
    norm = lax.rsqrt(q[0] * q[0] + q[1] * q[1] + q[2] * q[2] + q[3] * q[3])
    qw, qx, qy, qz = [v * norm for v in q]
    turn = [
        [
            1.0 - 2.0 * (qy * qy + qz * qz),
            2.0 * (qx * qy - qw * qz),
            2.0 * (qx * qz + qw * qy),
        ],
        [
            2.0 * (qx * qy + qw * qz),
            1.0 - 2.0 * (qx * qx + qz * qz),
            2.0 * (qy * qz - qw * qx),
        ],
        [
            2.0 * (qx * qz - qw * qy),
            2.0 * (qy * qz + qw * qx),
            1.0 - 2.0 * (qx * qx + qy * qy),
        ],
    ]
    mapping = [
        [scale_z * rot[0][k] - slope_u * rot[2][k] for k in range(3)],
        [scale_z * rot[1][k] - slope_w * rot[2][k] for k in range(3)],
    ]
    factor = [
        [
            (row[0] * turn[0][k] + row[1] * turn[1][k] + row[2] * turn[2][k]) * scales[k]
            for k in range(3)
        ]
        for row in mapping
    ]
    first, second = factor
    cover_a = first[0] * first[0] + first[1] * first[1] + first[2] * first[2] + blur_floor
    cover_b = first[0] * second[0] + first[1] * second[1] + first[2] * second[2]
    cover_c = second[0] * second[0] + second[1] * second[1] + second[2] * second[2] + blur_floor
    scale_det = 1.0 / (cover_a * cover_c - cover_b * cover_b)
    opacity = 1.0 / (1.0 + jnp.exp(-params[10]))
    towards = [centres[k] + back[k] for k in range(3)]
    length = lax.rsqrt(
        towards[0] * towards[0] + towards[1] * towards[1] + towards[2] * towards[2]
    )
    harmonics = sh_terms(*[v * length for v in towards])
    colours = []
    for channel in range(3):
        running = 0.5 + sh_first * params[11 + 16 * channel]
        for term in range(15):
            running = running + harmonics[term] * params[12 + 16 * channel + term]
        colours.append(jnp.maximum(running, 0.0))
    return [
        u_off + half_width,
        w_off + half_height,
        cover_c * scale_det,
        -cover_b * scale_det,
        cover_a * scale_det,
        opacity,
    ] + colours


def permute(idx_ref, main_ref, last_ref, chunks, rows, write):
    def group_step(group, unused):
        base = pl.multiple_of(group * 8, 8)
        index = idx_ref[pl.ds(base, 8), :]
        high = index >> 7
        low = index & 127
        totals = []
        for k in range(8):
            row_high = jnp.broadcast_to(high[k : k + 1], (8, LANES))
            row_low = jnp.broadcast_to(low[k : k + 1], (8, LANES))
            total = jnp.zeros((8, LANES), f32)
            for chunk in range(chunks):
                found = jnp.take_along_axis(
                    main_ref[chunk], row_low, axis=1, mode="promise_in_bounds"
                )
                total = jnp.where(row_high == chunk, found, total)
            totals.append(total)
        total = jnp.zeros((8, LANES), f32)
        for chunk in range(chunks):
            source = jnp.broadcast_to(last_ref[chunk : chunk + 1, :], (8, LANES))
            found = jnp.take_along_axis(source, low, axis=1, mode="promise_in_bounds")
            total = jnp.where(high == chunk, found, total)
        totals.append(total)
        write(group, totals[:8], totals[8])
        return unused

    lax.fori_loop(0, rows // 8, group_step, 0)


def invert(idx_ref, rows, high_count, inverse_ref):
    index = idx_ref[...]
    high = index >> 7
    low = index & 127
    high_ids = lax.broadcasted_iota(jnp.int32, (high_count, LANES), 0)
    low_ids = lax.broadcasted_iota(jnp.int32, (LANES, LANES), 0)
    lane_ids = lax.broadcasted_iota(jnp.int32, (high_count, LANES), 1).astype(f32)
    total = jnp.zeros((2 * high_count, LANES), f32)
    for start in range(0, rows, 8):
        left = []
        right = []
        for row in range(start, start + 8):
            here = high[row : row + 1] == high_ids
            left.append(
                jnp.concatenate(
                    [jnp.where(here, row + 1.0, 0.0), jnp.where(here, lane_ids, 0.0)], axis=0
                ).astype(bf16)
            )
            right.append(jnp.where(low[row : row + 1] == low_ids, 1.0, 0.0).astype(bf16))
        total = total + lax.dot_general(
            jnp.concatenate(left, axis=1),
            jnp.concatenate(right, axis=1),
            (((1,), (1,)), ((), ())),
            preferred_element_type=f32,
        )
    rows_found = total[:high_count].astype(jnp.int32)
    lanes_found = total[high_count:].astype(jnp.int32)
    inverse_ref[...] = (rows_found - 1) * LANES + lanes_found


def unpack(packed_ref, main_ref, last_ref, chunks):
    for chunk in range(chunks):
        for k in range(8):
            main_ref[chunk, k : k + 1, :] = packed_ref[chunk, :, k * LANES : (k + 1) * LANES]
        last_ref[chunk : chunk + 1, :] = packed_ref[chunk, :, 8 * LANES : 9 * LANES]


def pack_group(packed_ref):
    def write(group, vectors, last):
        for k in range(8):
            row = group * 8 + k
            for item in range(8):
                packed_ref[row, :, item * LANES : (item + 1) * LANES] = vectors[k][
                    item : item + 1
                ]
            packed_ref[row, :, 8 * LANES : 9 * LANES] = last[k : k + 1]

    return write


def slots_as_rows(slots_ref, idx_ref, rows):
    for row in range(rows):
        idx_ref[row : row + 1, :] = slots_ref[:, row * LANES : (row + 1) * LANES]


def to_dense(native, dense_ref, row_block, chunk):
    if native.shape[0] == 8:
        dense_ref[pl.ds(8 * row_block * STRIDE + chunk, 8, stride=STRIDE), :] = native
    else:
        for k in range(native.shape[0]):
            dense_ref[pl.ds((8 * row_block + k) * STRIDE + chunk, 1), :] = native[k : k + 1]


def dense_load(dense_ref, row, group):
    return dense_ref[pl.ds(pl.multiple_of(row * STRIDE + group * 8, 8), 8), :]


def dense_store(dense_ref, row, group, value):
    dense_ref[pl.ds(pl.multiple_of(row * STRIDE + group * 8, 8), 8), :] = value


def row_blocks():
    return [(block, min(8, PARAMS - 8 * block)) for block in range((PARAMS + 7) // 8)]


def project_groups(dense_ref, splat_ref, frame, half_width, half_height, chunks):
    def step(group, unused):
        params = [dense_load(dense_ref, row, group) for row in range(PARAMS)]
        for row, value in enumerate(project(params, frame, half_width, half_height)):
            dense_store(splat_ref, row, group, value)
        return unused

    lax.fori_loop(0, chunks // 8, step, 0)


def send_splats(splat_ref, main_ref, idx_ref, packed_ref, chunks, rows):
    for chunk in range(chunks):
        main_ref[chunk] = splat_ref[pl.ds(chunk, 8, stride=STRIDE), :]
    last_ref = splat_ref.at[pl.ds(8 * STRIDE, chunks), :]
    permute(idx_ref, main_ref, last_ref, chunks, rows, pack_group(packed_ref))


def first_owner_body(
    half_width,
    half_height,
    camera_ref,
    params_ref,
    slots_ref,
    packed_ref,
    dense_ref,
    splat_ref,
    main_ref,
    idx_ref,
):
    chunks = params_ref.shape[1] // LANES
    rows = slots_ref.shape[1] // LANES
    slots_as_rows(slots_ref, idx_ref, rows)

    def relayout(chunk, unused):
        lanes = pl.ds(pl.multiple_of(chunk * LANES, LANES), LANES)
        for block, size in row_blocks():
            to_dense(params_ref[8 * block : 8 * block + size, lanes], dense_ref, block, chunk)
        return unused

    lax.fori_loop(0, chunks, relayout, 0, unroll=4)
    frame = camera_frame(camera_ref, 0)
    project_groups(dense_ref, splat_ref, frame, half_width, half_height, chunks)
    send_splats(splat_ref, main_ref, idx_ref, packed_ref, chunks, rows)


def first_owner(camera, params, slots, half_width, half_height):
    chunks = params.shape[1] // LANES
    rows = slots.shape[1] // LANES
    return pl.pallas_call(
        functools.partial(first_owner_body, half_width, half_height),
        out_shape=pltpu.VMEM((rows, 1, ROWS * LANES), f32),
        in_specs=[SMEM, VMEM, VMEM],
        out_specs=VMEM,
        scratch_shapes=[
            pltpu.VMEM((64 * STRIDE, LANES), f32),
            pltpu.VMEM((ROWS * STRIDE, LANES), f32),
            pltpu.VMEM((chunks, 8, LANES), f32),
            pltpu.VMEM((rows, LANES), jnp.int32),
        ],
        name="first_owner",
    )(camera, params, slots)


def second_owner_body(
    half_width,
    half_height,
    camera_ref,
    params_ref,
    first_hbm,
    second_hbm,
    slots_ref,
    next_slots_ref,
    packed_ref,
    out_params_hbm,
    out_first_hbm,
    out_second_hbm,
    out_packed_ref,
    dense_ref,
    grad_ref,
    splat_ref,
    main_ref,
    last_ref,
    idx_ref,
    inverse_ref,
    params_out_ref,
    first_ref,
    second_ref,
    load_sems,
    store_sems,
):
    chunks = params_ref.shape[1] // LANES
    rows = slots_ref.shape[1] // LANES
    loads = [
        pltpu.make_async_copy(first_hbm, first_ref, load_sems.at[0]),
        pltpu.make_async_copy(second_hbm, second_ref, load_sems.at[1]),
    ]
    for copy in loads:
        copy.start()
    slots_as_rows(slots_ref, idx_ref, rows)
    invert(idx_ref, rows, chunks, inverse_ref)
    unpack(packed_ref, main_ref, last_ref, rows)

    def relayout(chunk, unused):
        lanes = pl.ds(pl.multiple_of(chunk * LANES, LANES), LANES)
        for block, size in row_blocks():
            to_dense(params_ref[8 * block : 8 * block + size, lanes], dense_ref, block, chunk)
        return unused

    lax.fori_loop(0, chunks, relayout, 0, unroll=4)

    def write_columns(group, vectors, last):
        for k in range(8):
            splat_ref[pl.ds(group * 8 + k, 8, stride=STRIDE), :] = vectors[k]
        dense_store(splat_ref, 8, group, last)

    permute(inverse_ref, main_ref, last_ref, rows, chunks, write_columns)

    frame = camera_frame(camera_ref, 0)

    def pull_step(group, unused):
        params = [dense_load(dense_ref, row, group) for row in range(PARAMS)]
        splats, pullback = jax.vjp(
            lambda *p: project(list(p), frame, half_width, half_height), *params
        )
        cotangents = [dense_load(splat_ref, row, group) for row in range(ROWS)]
        through_opacity = cotangents[5] * (1.0 - splats[5])
        cotangents[5] = jnp.zeros_like(cotangents[5])
        grads = list(pullback(cotangents))
        grads[10] = through_opacity
        for row, value in enumerate(grads):
            dense_store(grad_ref, row, group, value)
        return unused

    lax.fori_loop(0, chunks // 8, pull_step, 0)

    for copy in loads:
        copy.wait()
    rates = rate_values() / bias_first
    stores = []
    row_ids = lax.broadcasted_iota(jnp.int32, (8, LANES), 0)
    for block, size in row_blocks():
        span = slice(8 * block, 8 * block + size)
        block_rates = rates[8 * block : 8 * block + 8]
        step_size = jnp.full((8, LANES), block_rates[0], f32)
        for k in range(1, 8):
            if block_rates[k] != block_rates[0]:
                step_size = jnp.where(row_ids == k, f32(block_rates[k]), step_size)
        step_size = step_size[:size]

        def adam_step(chunk, unused, block=block, size=size, span=span, step_size=step_size):
            lanes = pl.ds(pl.multiple_of(chunk * LANES, LANES), LANES)
            gradient = grad_ref[pl.ds(8 * block * STRIDE + chunk, 8, stride=STRIDE), :][:size]
            moment = 0.9 * first_ref[span, lanes] + 0.1 * gradient
            square = 0.999 * second_ref[span, lanes] + 0.001 * gradient * gradient
            scaled = square * (1.0 / bias_second)
            root = scaled * lax.rsqrt(scaled)
            fresh = params_ref[span, lanes] - step_size * moment / (root + adam_epsilon)
            first_ref[span, lanes] = moment
            second_ref[span, lanes] = square
            params_out_ref[span, lanes] = fresh
            to_dense(fresh, dense_ref, block, chunk)
            return unused

        lax.fori_loop(0, chunks, adam_step, 0, unroll=8)
        for number, (source, target) in enumerate(
            [
                (params_out_ref, out_params_hbm),
                (first_ref, out_first_hbm),
                (second_ref, out_second_hbm),
            ]
        ):
            copy = pltpu.make_async_copy(
                source.at[span, :], target.at[span, :], store_sems.at[number, block]
            )
            copy.start()
            stores.append(copy)

    slots_as_rows(next_slots_ref, idx_ref, rows)
    frame = camera_frame(camera_ref, 1)
    project_groups(dense_ref, splat_ref, frame, half_width, half_height, chunks)
    send_splats(splat_ref, main_ref, idx_ref, out_packed_ref, chunks, rows)
    for copy in stores:
        copy.wait()


def second_owner(camera, params, first, second, slots, next_slots, packed, half_width, half_height):
    chunks = params.shape[1] // LANES
    rows = slots.shape[1] // LANES
    shape = jax.ShapeDtypeStruct(params.shape, f32)
    return pl.pallas_call(
        functools.partial(second_owner_body, half_width, half_height),
        out_shape=(shape, shape, shape, pltpu.VMEM((rows, 1, ROWS * LANES), f32)),
        in_specs=[SMEM, VMEM, ANY, ANY, VMEM, VMEM, VMEM],
        out_specs=(ANY, ANY, ANY, VMEM),
        scratch_shapes=[
            pltpu.VMEM((64 * STRIDE, LANES), f32),
            pltpu.VMEM((64 * STRIDE, LANES), f32),
            pltpu.VMEM((ROWS * STRIDE, LANES), f32),
            pltpu.VMEM((max(chunks, rows), 8, LANES), f32),
            pltpu.VMEM((rows, LANES), f32),
            pltpu.VMEM((rows, LANES), jnp.int32),
            pltpu.VMEM((chunks, LANES), jnp.int32),
            pltpu.VMEM(params.shape, f32),
            pltpu.VMEM(params.shape, f32),
            pltpu.VMEM(params.shape, f32),
            pltpu.SemaphoreType.DMA((2,)),
            pltpu.SemaphoreType.DMA((3, 8)),
        ],
        name="second_owner",
    )(camera, params, first, second, slots, next_slots, packed)


def halves(value):
    high = value.astype(bf16)
    return high, (value - high.astype(f32)).astype(bf16)


def triangle_pair(forward):
    rows = lax.broadcasted_iota(jnp.int32, (LIST_LEN, LIST_LEN), 0)
    cols = lax.broadcasted_iota(jnp.int32, (LIST_LEN, LIST_LEN), 1)
    chosen = rows < cols if forward else rows > cols
    one = jnp.where(chosen, 1.0, 0.0).astype(bf16)
    return jnp.concatenate([one, one], axis=0)


def batch_tiles(tile_count):
    return 8 if tile_count % 8 == 0 else 1


LOG2_E = 1.4426950408889634


def tile_offsets(splat_ref, tile, number):
    left = (number % TILES_X) * tile_edge
    top = (number // TILES_X) * tile_edge
    ids = lax.broadcasted_iota(jnp.int32, (8, LANES), 0)
    u = jnp.broadcast_to(splat_ref[tile, 0:1, :], (8, LANES))
    w = jnp.broadcast_to(splat_ref[tile, 1:2, :], (8, LANES))
    across = [u - ((ids + (left + 8 * h)).astype(f32) + 0.5) for h in range(2)]
    down = [w - ((ids + (top + 8 * h)).astype(f32) + 0.5) for h in range(2)]
    return across, down


def spread_row(ref, item, row):
    return jnp.broadcast_to(ref[item, row : row + 1, :], (8, LANES))


def alpha_phase(splat_ref, tile, number, item, row_ref, alpha_ref, odds_ref, pair_ref):
    a, b, c, o = [jnp.broadcast_to(splat_ref[tile, k : k + 1, :], (8, LANES)) for k in (2, 3, 4, 5)]
    across, down = tile_offsets(splat_ref, tile, number)
    base = item * TILE_PIXELS
    along = [((-0.5 * LOG2_E) * a) * x * x for x in across]
    for h in range(2):
        row_ref[item, 8 * h : 8 * h + 8, :] = ((-0.5 * LOG2_E) * c) * down[h] * down[h]
        row_ref[item, 16 + 8 * h : 24 + 8 * h, :] = ((-LOG2_E) * b) * down[h]
        if odds_ref is not None:
            row_ref[item, 32 + 8 * h : 40 + 8 * h, :] = down[h]
    for row in range(tile_edge):
        fixed = spread_row(row_ref, item, row)
        slope = spread_row(row_ref, item, 16 + row)
        logs = []
        for h in range(2):
            exponent = along[h] + (fixed + slope * across[h])
            alpha = o * jnp.exp2(exponent)
            log_clear = jnp.log(1.0 - alpha) * LOG2_E
            where = slice(base + row * tile_edge + 8 * h, base + row * tile_edge + 8 * h + 8)
            alpha_ref[where, :] = alpha
            if odds_ref is not None:
                odds_ref[where, :] = alpha * jnp.exp2(-log_clear)
            logs.append(log_clear)
        high, low = halves(jnp.concatenate(logs, axis=0))
        where = slice(base + row * tile_edge, base + (row + 1) * tile_edge)
        pair_ref[where, :LIST_LEN] = high
        pair_ref[where, LIST_LEN:] = low


def weight_phase(item, before_ref, alpha_ref, weight_ref, pair_ref):
    for row in range(tile_edge):
        start = item * TILE_PIXELS + row * tile_edge
        where = slice(start, start + tile_edge)
        weight = alpha_ref[where, :] * jnp.exp2(before_ref[where, :])
        if weight_ref is not None:
            weight_ref[where, :] = weight
        high, low = halves(weight)
        pair_ref[where, :LIST_LEN] = high
        pair_ref[where, LIST_LEN:] = low


def split_colours(splat_ref, tile):
    colours = splat_ref[tile, 6:14, :]
    high = colours.astype(bf16).astype(f32)
    return high, colours - high


def colour_sum(high, low, pair):
    upper = jnp.concatenate([high, high], axis=1)
    lower = jnp.concatenate([low, jnp.zeros_like(low)], axis=1)
    result = lax.dot_general(
        jnp.concatenate([upper, lower], axis=0).astype(bf16),
        pair,
        (((1,), (1,)), ((), ())),
        preferred_element_type=f32,
    )
    return result[0:8] + result[8:16]


def write_tiles(splat_ref):
    def write(group, vectors, last):
        for k in range(8):
            tile = group * 8 + k
            splat_ref[tile, 0:8, :] = vectors[k]
            splat_ref[tile, 8:9, :] = last[k : k + 1]
            splat_ref[tile, 9:16, :] = jnp.zeros((7, LANES), f32)

    return write


def staggered(stages, parts):
    for turn in range(len(stages) + parts - 1):
        for part in range(parts):
            if 0 <= turn - part < len(stages):
                stages[turn - part](part)


def train_body(
    numbers_ref,
    lists_ref,
    targets_ref,
    packed_ref,
    out_packed_ref,
    main_ref,
    last_ref,
    splat_ref,
    row_ref,
    alpha_ref,
    odds_ref,
    before_ref,
    weight_ref,
    log_pair_ref,
    pair_ref,
    pull_ref,
    grad_pair_ref,
    grad_ref,
    grad_last_ref,
    inverse_ref,
):
    tile_count = lists_ref.shape[0]
    chunks = packed_ref.shape[0]
    batch = batch_tiles(tile_count)
    parts = PARTS if batch % PARTS == 0 else 1
    size = batch // parts
    unpack(packed_ref, main_ref, last_ref, chunks)
    permute(lists_ref, main_ref, last_ref, chunks, tile_count, write_tiles(splat_ref))
    invert(lists_ref, tile_count, chunks, inverse_ref)
    forward = triangle_pair(True)
    backward = triangle_pair(False)

    def batch_step(step, unused):
        first = step * batch

        def items(part):
            return range(part * size, (part + 1) * size)

        def span(part):
            return slice(part * size * TILE_PIXELS, (part + 1) * size * TILE_PIXELS)

        def alphas(part):
            for item in items(part):
                tile = first + item
                alpha_phase(
                    splat_ref, tile, numbers_ref[tile], item, row_ref, alpha_ref, odds_ref, log_pair_ref
                )

        def befores(part):
            before_ref[span(part), :] = jnp.dot(
                log_pair_ref[span(part), :], forward, preferred_element_type=f32
            )

        def weights(part):
            for item in items(part):
                weight_phase(item, before_ref, alpha_ref, weight_ref, pair_ref)

        def deltas(part):
            for item in items(part):
                tile = first + item
                pixels = slice(item * TILE_PIXELS, (item + 1) * TILE_PIXELS)
                pair = pair_ref[pixels, :]
                high, low = split_colours(splat_ref, tile)
                rendered = colour_sum(high, low, pair)
                wanted = [targets_ref[channel, pl.ds(tile, 1), :] for channel in range(3)]
                wanted = jnp.concatenate(wanted + [jnp.zeros((5, TILE_PIXELS), f32)], axis=0)
                delta = rendered - wanted
                delta_high = delta.astype(bf16).astype(f32)
                delta_low = delta - delta_high
                left = jnp.concatenate(
                    [delta_high, delta_high, delta_low, jnp.zeros_like(delta)], axis=0
                ).astype(bf16)
                right = jnp.concatenate([high, low, high, jnp.zeros_like(high)], axis=0).astype(bf16)
                pulled = lax.dot_general(
                    left, right, (((0,), (0,)), ((), ())), preferred_element_type=f32
                )
                for row in range(tile_edge):
                    start = item * TILE_PIXELS + row * tile_edge
                    where = slice(start, start + tile_edge)
                    product = pulled[row * tile_edge : (row + 1) * tile_edge] * weight_ref[where, :]
                    pull_ref[where, :] = product
                    product_high, product_low = halves(product)
                    grad_pair_ref[where, :LIST_LEN] = product_high
                    grad_pair_ref[where, LIST_LEN:] = product_low
                colour = jnp.dot(
                    jnp.concatenate([delta_high, delta_low], axis=0).astype(bf16),
                    pair,
                    preferred_element_type=f32,
                )
                colour = colour[0:8, :LIST_LEN] + (colour[0:8, LIST_LEN:] + colour[8:16, :LIST_LEN])
                grad_ref[tile, 6:8, :] = colour[0:2]
                grad_last_ref[pl.ds(tile, 1), :] = colour[2:3]

        def afters(part):
            before_ref[span(part), :] = jnp.dot(
                grad_pair_ref[span(part), :], backward, preferred_element_type=f32
            )

        def moments(part):
            for item in items(part):
                tile = first + item
                across, down = tile_offsets(splat_ref, tile, numbers_ref[tile])
                sums = [[jnp.zeros((8, LANES), f32) for j in range(3)] for h in range(2)]
                for row in range(tile_edge):
                    offset = spread_row(row_ref, item, 32 + row)
                    for h in range(2):
                        start = item * TILE_PIXELS + row * tile_edge + 8 * h
                        where = slice(start, start + 8)
                        slope = pull_ref[where, :] - before_ref[where, :] * odds_ref[where, :]
                        once = slope * offset
                        sums[h][0] = sums[h][0] + slope
                        sums[h][1] = sums[h][1] + once
                        sums[h][2] = sums[h][2] + once * offset

                def total(pieces):
                    return jnp.sum(pieces[0] + pieces[1], axis=0, keepdims=True)

                whole = total([sums[h][0] for h in range(2)])
                along = [sums[h][0] * across[h] for h in range(2)]
                moment_x = total(along)
                moment_xx = total([along[h] * across[h] for h in range(2)])
                moment_y = total([sums[h][1] for h in range(2)])
                moment_xy = total([sums[h][1] * across[h] for h in range(2)])
                moment_yy = total([sums[h][2] for h in range(2)])
                a = splat_ref[tile, 2:3, :]
                b = splat_ref[tile, 3:4, :]
                c = splat_ref[tile, 4:5, :]
                grad_ref[tile, 0:1, :] = -(a * moment_x + b * moment_y)
                grad_ref[tile, 1:2, :] = -(c * moment_y + b * moment_x)
                grad_ref[tile, 2:3, :] = -0.5 * moment_xx
                grad_ref[tile, 3:4, :] = -moment_xy
                grad_ref[tile, 4:5, :] = -0.5 * moment_yy
                grad_ref[tile, 5:6, :] = whole

        staggered([alphas, befores, weights, deltas, afters, moments], parts)
        return unused

    lax.fori_loop(0, tile_count // batch, batch_step, 0)
    permute(
        inverse_ref,
        grad_ref,
        grad_last_ref,
        tile_count,
        out_packed_ref.shape[0],
        pack_group(out_packed_ref),
    )


def train(numbers, lists, targets, packed):
    tile_count = lists.shape[0]
    chunks = packed.shape[0]
    batch = batch_tiles(tile_count)
    pixels = batch * TILE_PIXELS
    plain = pltpu.VMEM((pixels, LIST_LEN), f32)
    pairs = pltpu.VMEM((pixels, 2 * LIST_LEN), bf16)
    return pl.pallas_call(
        train_body,
        out_shape=pltpu.VMEM(packed.shape, f32),
        in_specs=[SMEM, VMEM, VMEM, VMEM],
        out_specs=VMEM,
        scratch_shapes=[
            pltpu.VMEM((chunks, 8, LANES), f32),
            pltpu.VMEM((chunks, LANES), f32),
            pltpu.VMEM((tile_count, 16, LANES), f32),
            pltpu.VMEM((batch, 48, LANES), f32),
            plain,
            plain,
            plain,
            plain,
            pairs,
            pairs,
            plain,
            pairs,
            pltpu.VMEM((tile_count, 8, LANES), f32),
            pltpu.VMEM((tile_count, LANES), f32),
            pltpu.VMEM((chunks, LANES), jnp.int32),
        ],
        name="train_tiles",
    )(numbers, lists, targets, packed)


def render_body(
    numbers_ref,
    lists_ref,
    packed_ref,
    out_ref,
    main_ref,
    last_ref,
    splat_ref,
    row_ref,
    alpha_ref,
    before_ref,
    log_pair_ref,
    pair_ref,
):
    tile_count = lists_ref.shape[0]
    chunks = packed_ref.shape[0]
    batch = batch_tiles(tile_count)
    parts = PARTS if batch % PARTS == 0 else 1
    size = batch // parts
    unpack(packed_ref, main_ref, last_ref, chunks)
    permute(lists_ref, main_ref, last_ref, chunks, tile_count, write_tiles(splat_ref))
    forward = triangle_pair(True)

    def batch_step(step, unused):
        first = step * batch

        def items(part):
            return range(part * size, (part + 1) * size)

        def span(part):
            return slice(part * size * TILE_PIXELS, (part + 1) * size * TILE_PIXELS)

        def alphas(part):
            for item in items(part):
                tile = first + item
                alpha_phase(
                    splat_ref, tile, numbers_ref[tile], item, row_ref, alpha_ref, None, log_pair_ref
                )

        def befores(part):
            before_ref[span(part), :] = jnp.dot(
                log_pair_ref[span(part), :], forward, preferred_element_type=f32
            )

        def weights(part):
            for item in items(part):
                weight_phase(item, before_ref, alpha_ref, None, pair_ref)

        def colours(part):
            for item in items(part):
                tile = first + item
                high, low = split_colours(splat_ref, tile)
                pair = pair_ref[item * TILE_PIXELS : (item + 1) * TILE_PIXELS, :]
                rendered = colour_sum(high, low, pair)
                for channel in range(3):
                    out_ref[channel, pl.ds(tile, 1), :] = rendered[channel : channel + 1]

        staggered([alphas, befores, weights, colours], parts)
        return unused

    lax.fori_loop(0, tile_count // batch, batch_step, 0)


def render(numbers, lists, packed):
    tile_count = lists.shape[0]
    chunks = packed.shape[0]
    batch = batch_tiles(tile_count)
    pixels = batch * TILE_PIXELS
    plain = pltpu.VMEM((pixels, LIST_LEN), f32)
    pairs = pltpu.VMEM((pixels, 2 * LIST_LEN), bf16)
    return pl.pallas_call(
        render_body,
        out_shape=jax.ShapeDtypeStruct((3, tile_count, TILE_PIXELS), f32),
        in_specs=[SMEM, VMEM, VMEM],
        out_specs=VMEM,
        scratch_shapes=[
            pltpu.VMEM((chunks, 8, LANES), f32),
            pltpu.VMEM((chunks, LANES), f32),
            pltpu.VMEM((tile_count, 16, LANES), f32),
            pltpu.VMEM((batch, 48, LANES), f32),
            plain,
            plain,
            pairs,
            pairs,
        ],
        name="render_tiles",
    )(numbers, lists, packed)


def exchange(packed, devices):
    rows = packed.shape[0]
    if rows == devices:
        packed = lax.all_to_all(packed, "dev", split_axis=0, concat_axis=0, tiled=True)
        return pltpu.with_memory_space_constraint(packed, pltpu.VMEM)
    cap = rows * LANES // devices
    slots = packed.reshape(rows, ROWS, LANES).transpose(1, 0, 2).reshape(ROWS, devices, cap)
    slots = lax.all_to_all(slots, "dev", split_axis=1, concat_axis=1, tiled=True)
    slots = slots.reshape(ROWS, rows, LANES).transpose(1, 0, 2)
    return slots.reshape(rows, 1, ROWS * LANES)


def shards(
    gauss_params,
    adam_first,
    adam_second,
    camera,
    send_first,
    send_second,
    lists_first,
    lists_second,
    tiles_first,
    tiles_second,
    targets,
):
    devices = lax.axis_size("dev")
    half_width = 0.5 * TILES_X * tile_edge
    half_height = 0.5 * (lists_first.shape[0] * devices // TILES_X * tile_edge)
    packed = first_owner(camera, gauss_params, send_first, half_width, half_height)
    packed = exchange(packed, devices)
    packed = train(tiles_first, lists_first, jnp.transpose(targets, (1, 0, 2)), packed)
    packed = exchange(packed, devices)
    new_params, new_first, new_second, packed = second_owner(
        camera,
        gauss_params,
        adam_first,
        adam_second,
        send_first,
        send_second,
        packed,
        half_width,
        half_height,
    )
    packed = exchange(packed, devices)
    rendered = render(tiles_second, lists_second, packed)
    return (new_params, new_first, new_second, jnp.transpose(rendered, (1, 0, 2)))


def solution(mesh):
    placed = (
        P(None, "dev"),
        P(None, "dev"),
        P(None, "dev"),
        P(),
        P("dev", None),
        P("dev", None),
        P("dev", None),
        P("dev", None),
        P("dev"),
        P("dev"),
        P("dev", None, None),
    )
    return jax.shard_map(
        shards,
        mesh=mesh,
        in_specs=placed,
        out_specs=(P(None, "dev"), P(None, "dev"), P(None, "dev"), P("dev", None, None)),
        check_vma=False,
    )
```

```python
import functools

import jax
import jax.numpy as jnp
import numpy as np
from jax import lax
from jax.experimental import pallas as pl
from jax.experimental.pallas import tpu as pltpu
from jax.sharding import PartitionSpec as P

PARAMS = 59
LIST_LEN = 128
TILE_PIXELS = 256
TILES_X = 128
LANES = 128
ROWS = 9
STRIDE = 72
PARTS = 4
VMEM_LIMIT = 36 << 20

tile_edge = 16
focal_length = 1000.0
blur_floor = 0.3
adam_epsilon = 1e-08
bias_first = 1.0 - 0.9**20
bias_second = 1.0 - 0.999**20
sh_first = 0.28209479177387814
sh_second = 0.4886025119029199
sh_third = (
    1.0925484305920792,
    -1.0925484305920792,
    0.31539156525252005,
    -1.0925484305920792,
    0.5462742152960396,
)
sh_fourth = (
    -0.5900435899266435,
    2.890611442640554,
    -0.4570457994644658,
    0.3731763325901154,
    -0.4570457994644658,
    1.445305721320277,
    -0.5900435899266435,
)

f32 = jnp.float32
bf16 = jnp.bfloat16
VMEM = pl.BlockSpec(memory_space=pltpu.VMEM)
SMEM = pl.BlockSpec(memory_space=pltpu.SMEM)
ANY = pl.BlockSpec(memory_space=pl.ANY)
HBM = pl.BlockSpec(memory_space=pltpu.HBM)


def rate_values():
    values = np.full((64,), 0.000125)
    values[0:3] = 0.00016
    values[3:6] = 0.005
    values[6:10] = 0.001
    values[10] = 0.05
    values[11] = 0.0025
    values[27] = 0.0025
    values[43] = 0.0025
    return values


def camera_frame(camera_ref, view):
    shape = (8, LANES)
    angle = [jnp.full(shape, camera_ref[view, k], f32) for k in range(3)]
    shift = [jnp.full(shape, camera_ref[view, 3 + k], f32) for k in range(3)]
    (ca, cb, cc) = [jnp.cos(x) for x in angle]
    (sa, sb, sc) = [jnp.sin(x) for x in angle]
    rot = [
        [cc * cb, cc * sb * sa - sc * ca, cc * sb * ca + sc * sa],
        [sc * cb, sc * sb * sa + cc * ca, sc * sb * ca - cc * sa],
        [-sb, cb * sa, cb * ca],
    ]
    back = [
        rot[0][k] * shift[0] + rot[1][k] * shift[1] + rot[2][k] * shift[2]
        for k in range(3)
    ]
    return rot, shift, back


def sh_terms(x, y, z):
    xx, yy, zz = (x * x, y * y, z * z)
    return [
        -sh_second * y,
        sh_second * z,
        -sh_second * x,
        sh_third[0] * x * y,
        sh_third[1] * y * z,
        sh_third[2] * (2.0 * zz - xx - yy),
        sh_third[3] * x * z,
        sh_third[4] * (xx - yy),
        sh_fourth[0] * y * (3.0 * xx - yy),
        sh_fourth[1] * x * y * z,
        sh_fourth[2] * y * (4.0 * zz - xx - yy),
        sh_fourth[3] * z * (2.0 * zz - 3.0 * xx - 3.0 * yy),
        sh_fourth[4] * x * (4.0 * zz - xx - yy),
        sh_fourth[5] * z * (xx - yy),
        sh_fourth[6] * x * (xx - 3.0 * yy),
    ]


def project(params, frame, half_width, half_height):
    rot, shift, back = frame
    centres = params[0:3]
    viewed = [
        rot[k][0] * centres[0] + rot[k][1] * centres[1] + rot[k][2] * centres[2] + shift[k]
        for k in range(3)
    ]
    inverse = 1.0 / viewed[2]
    scale_z = focal_length * inverse
    u_off = scale_z * viewed[0]
    w_off = scale_z * viewed[1]
    slope_u = u_off * inverse
    slope_w = w_off * inverse
    scales = [jnp.exp(params[3 + k]) for k in range(3)]
    q = params[6:10]
    norm = lax.rsqrt(q[0] * q[0] + q[1] * q[1] + q[2] * q[2] + q[3] * q[3])
    qw, qx, qy, qz = [v * norm for v in q]
    turn = [
        [
            1.0 - 2.0 * (qy * qy + qz * qz),
            2.0 * (qx * qy - qw * qz),
            2.0 * (qx * qz + qw * qy),
        ],
        [
            2.0 * (qx * qy + qw * qz),
            1.0 - 2.0 * (qx * qx + qz * qz),
            2.0 * (qy * qz - qw * qx),
        ],
        [
            2.0 * (qx * qz - qw * qy),
            2.0 * (qy * qz + qw * qx),
            1.0 - 2.0 * (qx * qx + qy * qy),
        ],
    ]
    mapping = [
        [scale_z * rot[0][k] - slope_u * rot[2][k] for k in range(3)],
        [scale_z * rot[1][k] - slope_w * rot[2][k] for k in range(3)],
    ]
    factor = [
        [
            (row[0] * turn[0][k] + row[1] * turn[1][k] + row[2] * turn[2][k]) * scales[k]
            for k in range(3)
        ]
        for row in mapping
    ]
    first, second = factor
    cover_a = first[0] * first[0] + first[1] * first[1] + first[2] * first[2] + blur_floor
    cover_b = first[0] * second[0] + first[1] * second[1] + first[2] * second[2]
    cover_c = second[0] * second[0] + second[1] * second[1] + second[2] * second[2] + blur_floor
    scale_det = 1.0 / (cover_a * cover_c - cover_b * cover_b)
    opacity = 1.0 / (1.0 + jnp.exp(-params[10]))
    towards = [centres[k] + back[k] for k in range(3)]
    length = lax.rsqrt(
        towards[0] * towards[0] + towards[1] * towards[1] + towards[2] * towards[2]
    )
    harmonics = sh_terms(*[v * length for v in towards])
    colours = []
    for channel in range(3):
        running = 0.5 + sh_first * params[11 + 16 * channel]
        for term in range(15):
            running = running + harmonics[term] * params[12 + 16 * channel + term]
        colours.append(jnp.maximum(running, 0.0))
    return [
        u_off + half_width,
        w_off + half_height,
        cover_c * scale_det,
        -cover_b * scale_det,
        cover_a * scale_det,
        opacity,
    ] + colours


def permute_group(idx_ref, main_ref, last_ref, chunks, group, write):
    base = pl.multiple_of(group * 8, 8)
    index = idx_ref[pl.ds(base, 8), :]
    high = index >> 7
    low = index & 127
    totals = []
    for k in range(8):
        row_high = jnp.broadcast_to(high[k : k + 1], (8, LANES))
        row_low = jnp.broadcast_to(low[k : k + 1], (8, LANES))
        total = jnp.zeros((8, LANES), f32)
        for chunk in range(chunks):
            found = jnp.take_along_axis(
                main_ref[chunk], row_low, axis=1, mode="promise_in_bounds"
            )
            total = jnp.where(row_high == chunk, found, total)
        totals.append(total)
    total = jnp.zeros((8, LANES), f32)
    for chunk in range(chunks):
        source = jnp.broadcast_to(last_ref[chunk : chunk + 1, :], (8, LANES))
        found = jnp.take_along_axis(source, low, axis=1, mode="promise_in_bounds")
        total = jnp.where(high == chunk, found, total)
    write(group, totals, total)


def permute(idx_ref, main_ref, last_ref, chunks, rows, write):
    def group_step(group, unused):
        permute_group(idx_ref, main_ref, last_ref, chunks, group, write)
        return unused

    lax.fori_loop(0, rows // 8, group_step, 0)


def invert(idx_ref, rows, high_count, inverse_ref):
    index = idx_ref[...]
    high = index >> 7
    low = index & 127
    high_ids = lax.broadcasted_iota(jnp.int32, (high_count, LANES), 0)
    low_ids = lax.broadcasted_iota(jnp.int32, (LANES, LANES), 0)
    lane_ids = lax.broadcasted_iota(jnp.int32, (high_count, LANES), 1).astype(f32)
    total = jnp.zeros((2 * high_count, LANES), f32)
    for start in range(0, rows, 8):
        left = []
        right = []
        for row in range(start, start + 8):
            here = high[row : row + 1] == high_ids
            left.append(
                jnp.concatenate(
                    [jnp.where(here, row + 1.0, 0.0), jnp.where(here, lane_ids, 0.0)], axis=0
                ).astype(bf16)
            )
            right.append(jnp.where(low[row : row + 1] == low_ids, 1.0, 0.0).astype(bf16))
        total = total + lax.dot_general(
            jnp.concatenate(left, axis=1),
            jnp.concatenate(right, axis=1),
            (((1,), (1,)), ((), ())),
            preferred_element_type=f32,
        )
    rows_found = total[:high_count].astype(jnp.int32)
    lanes_found = total[high_count:].astype(jnp.int32)
    inverse_ref[...] = (rows_found - 1) * LANES + lanes_found


def unpack(packed_ref, main_ref, last_ref, chunks):
    for chunk in range(chunks):
        for k in range(8):
            main_ref[chunk, k : k + 1, :] = packed_ref[chunk, :, k * LANES : (k + 1) * LANES]
        last_ref[chunk : chunk + 1, :] = packed_ref[chunk, :, 8 * LANES : 9 * LANES]


def pack_group(packed_ref):
    def write(group, vectors, last):
        for k in range(8):
            row = group * 8 + k
            for item in range(8):
                packed_ref[row, :, item * LANES : (item + 1) * LANES] = vectors[k][
                    item : item + 1
                ]
            packed_ref[row, :, 8 * LANES : 9 * LANES] = last[k : k + 1]

    return write


def slots_as_rows(slots_ref, idx_ref, rows):
    for row in range(rows):
        idx_ref[row : row + 1, :] = slots_ref[:, row * LANES : (row + 1) * LANES]


def native_to_group(native, ref, block, k):
    if native.shape[0] == 8:
        ref[pl.ds(64 * block + k, 8, stride=8), :] = native
    else:
        for row in range(native.shape[0]):
            target = 64 * block + 8 * row + k
            ref[target : target + 1, :] = native[row : row + 1]


def dense_load(dense_ref, row, group):
    return dense_ref[pl.ds(pl.multiple_of(row * STRIDE + group * 8, 8), 8), :]


def dense_store(dense_ref, row, group, value):
    dense_ref[pl.ds(pl.multiple_of(row * STRIDE + group * 8, 8), 8), :] = value


def row_blocks():
    return [(block, min(8, PARAMS - 8 * block)) for block in range((PARAMS + 7) // 8)]


def send_splats(splat_ref, main_ref, idx_ref, packed_ref, chunks, rows):
    for chunk in range(chunks):
        main_ref[chunk] = splat_ref[pl.ds(chunk, 8, stride=STRIDE), :]
    last_ref = splat_ref.at[pl.ds(8 * STRIDE, chunks), :]
    permute(idx_ref, main_ref, last_ref, chunks, rows, pack_group(packed_ref))


def first_owner_body(
    half_width,
    half_height,
    camera_hbm,
    params_hbm,
    slots_hbm,
    packed_ref,
    params_ref,
    slots_ref,
    camera_ref,
    dense_ref,
    splat_ref,
    main_ref,
    idx_ref,
    sems,
):
    chunks = params_hbm.shape[1] // LANES
    rows = slots_hbm.shape[1] // LANES
    groups = chunks // 8
    small = [
        pltpu.make_async_copy(camera_hbm, camera_ref, sems.at[groups]),
        pltpu.make_async_copy(slots_hbm, slots_ref, sems.at[groups + 1]),
    ]

    def load(group):
        columns = pl.ds(pl.multiple_of(group * (8 * LANES), 8 * LANES), 8 * LANES)
        return pltpu.make_async_copy(
            params_hbm.at[:, columns], params_ref.at[:, columns], sems.at[group]
        )

    for copy in small:
        copy.start()
    for group in range(groups):
        load(group).start()
    for copy in small:
        copy.wait()
    frame = camera_frame(camera_ref, 0)

    def step(group, unused):
        load(group).wait()
        for k in range(8):
            chunk = group * 8 + k
            lanes = pl.ds(pl.multiple_of(chunk * LANES, LANES), LANES)
            for block, size in row_blocks():
                native_to_group(
                    params_ref[8 * block : 8 * block + size, lanes], dense_ref, block, k
                )
        params = [dense_ref[8 * row : 8 * row + 8, :] for row in range(PARAMS)]
        for row, value in enumerate(project(params, frame, half_width, half_height)):
            dense_store(splat_ref, row, group, value)
        return unused

    lax.fori_loop(0, groups, step, 0)
    slots_as_rows(slots_ref, idx_ref, rows)
    send_splats(splat_ref, main_ref, idx_ref, packed_ref, chunks, rows)


def first_owner(camera, params, slots, half_width, half_height):
    chunks = params.shape[1] // LANES
    rows = slots.shape[1] // LANES
    return pl.pallas_call(
        functools.partial(first_owner_body, half_width, half_height),
        out_shape=pltpu.VMEM((rows, 1, ROWS * LANES), f32),
        in_specs=[HBM, HBM, HBM],
        out_specs=VMEM,
        scratch_shapes=[
            pltpu.VMEM(params.shape, f32),
            pltpu.VMEM(slots.shape, jnp.int32),
            pltpu.SMEM(camera.shape, f32),
            pltpu.VMEM((64 * 8, LANES), f32),
            pltpu.VMEM((ROWS * STRIDE, LANES), f32),
            pltpu.VMEM((chunks, 8, LANES), f32),
            pltpu.VMEM((rows, LANES), jnp.int32),
            pltpu.SemaphoreType.DMA((chunks // 8 + 2,)),
        ],
        compiler_params=pltpu.CompilerParams(vmem_limit_bytes=VMEM_LIMIT),
        name="first_owner",
    )(camera, params, slots)


def second_owner_body(
    half_width,
    half_height,
    camera_ref,
    params_ref,
    first_hbm,
    second_hbm,
    slots_ref,
    next_slots_ref,
    packed_ref,
    out_params_hbm,
    out_first_hbm,
    out_second_hbm,
    out_packed_ref,
    dense_ref,
    grad_ref,
    fresh_ref,
    splat_ref,
    next_splat_ref,
    main_ref,
    last_ref,
    idx_ref,
    inverse_ref,
    first_ref,
    second_ref,
    params_out_ref,
    first_out_ref,
    second_out_ref,
    load_sems,
    store_sems,
):
    chunks = params_ref.shape[1] // LANES
    rows = slots_ref.shape[1] // LANES
    groups = chunks // 8

    def columns_of(group):
        return pl.ds(pl.multiple_of(group * (8 * LANES), 8 * LANES), 8 * LANES)

    def loads(group):
        columns = columns_of(group)
        return [
            pltpu.make_async_copy(
                source.at[:, columns], target.at[:, columns], load_sems.at[number, group]
            )
            for number, (source, target) in enumerate(
                [(first_hbm, first_ref), (second_hbm, second_ref)]
            )
        ]

    for group in range(groups):
        for copy in loads(group):
            copy.start()
    slots_as_rows(slots_ref, idx_ref, rows)
    invert(idx_ref, rows, chunks, inverse_ref)
    unpack(packed_ref, main_ref, last_ref, rows)
    frame = camera_frame(camera_ref, 0)
    next_frame = camera_frame(camera_ref, 1)
    rates = rate_values() / bias_first
    row_ids = lax.broadcasted_iota(jnp.int32, (8, LANES), 0)

    def write_columns(group, vectors, last):
        for k in range(8):
            splat_ref[pl.ds(group * 8 + k, 8, stride=STRIDE), :] = vectors[k]
        dense_store(splat_ref, 8, group, last)

    def lanes_of(group, k):
        start = pl.multiple_of(group * (8 * LANES), 8 * LANES) + k * LANES
        return pl.ds(pl.multiple_of(start, LANES), LANES)

    def stores(group):
        columns = columns_of(group)
        return [
            pltpu.make_async_copy(
                source.at[:, columns], target.at[:, columns], store_sems.at[number, group]
            )
            for number, (source, target) in enumerate(
                [
                    (params_out_ref, out_params_hbm),
                    (first_out_ref, out_first_hbm),
                    (second_out_ref, out_second_hbm),
                ]
            )
        ]

    def work(group):
        for copy in loads(group):
            copy.wait()
        for block, size in row_blocks():
            for k in range(8):
                native = params_ref[8 * block : 8 * block + size, lanes_of(group, k)]
                native_to_group(native, dense_ref, block, k)
        params = [dense_ref[8 * row : 8 * row + 8, :] for row in range(PARAMS)]
        splats, pullback = jax.vjp(
            lambda *p: project(list(p), frame, half_width, half_height), *params
        )
        cotangents = [dense_load(splat_ref, row, group) for row in range(ROWS)]
        through_opacity = cotangents[5] * (1.0 - splats[5])
        cotangents[5] = jnp.zeros_like(cotangents[5])
        grads = list(pullback(cotangents))
        grads[10] = through_opacity
        for row, value in enumerate(grads):
            grad_ref[8 * row : 8 * row + 8, :] = value
        for block, size in row_blocks():
            span = slice(8 * block, 8 * block + size)
            block_rates = rates[8 * block : 8 * block + 8]
            step_size = jnp.full((8, LANES), block_rates[0], f32)
            for k in range(1, 8):
                if block_rates[k] != block_rates[0]:
                    step_size = jnp.where(row_ids == k, f32(block_rates[k]), step_size)
            step_size = step_size[:size]
            for k in range(8):
                lanes = lanes_of(group, k)
                gradient = grad_ref[pl.ds(64 * block + k, 8, stride=8), :][:size]
                moment = 0.9 * first_ref[span, lanes] + 0.1 * gradient
                square = 0.999 * second_ref[span, lanes] + 0.001 * gradient * gradient
                scaled = square * (1.0 / bias_second)
                root = scaled * lax.rsqrt(scaled)
                fresh = params_ref[span, lanes] - step_size * moment / (root + adam_epsilon)
                first_out_ref[span, lanes] = moment
                second_out_ref[span, lanes] = square
                params_out_ref[span, lanes] = fresh
                native_to_group(fresh, fresh_ref, block, k)
        for copy in stores(group):
            copy.start()
        params = [fresh_ref[8 * row : 8 * row + 8, :] for row in range(PARAMS)]
        for row, value in enumerate(project(params, next_frame, half_width, half_height)):
            dense_store(next_splat_ref, row, group, value)

    permute_group(inverse_ref, main_ref, last_ref, rows, 0, write_columns)

    def step(group, unused):
        work(group - 1)
        permute_group(inverse_ref, main_ref, last_ref, rows, group, write_columns)
        return unused

    lax.fori_loop(1, groups, step, 0)
    work(groups - 1)
    slots_as_rows(next_slots_ref, idx_ref, rows)
    send_splats(next_splat_ref, main_ref, idx_ref, out_packed_ref, chunks, rows)
    for group in range(groups):
        for copy in stores(group):
            copy.wait()


def second_owner(camera, params, first, second, slots, next_slots, packed, half_width, half_height):
    chunks = params.shape[1] // LANES
    rows = slots.shape[1] // LANES
    shape = jax.ShapeDtypeStruct(params.shape, f32)
    return pl.pallas_call(
        functools.partial(second_owner_body, half_width, half_height),
        out_shape=(shape, shape, shape, pltpu.VMEM((rows, 1, ROWS * LANES), f32)),
        in_specs=[SMEM, VMEM, HBM, HBM, VMEM, VMEM, VMEM],
        out_specs=(ANY, ANY, ANY, VMEM),
        scratch_shapes=[
            pltpu.VMEM((64 * 8, LANES), f32),
            pltpu.VMEM((64 * 8, LANES), f32),
            pltpu.VMEM((64 * 8, LANES), f32),
            pltpu.VMEM((ROWS * STRIDE, LANES), f32),
            pltpu.VMEM((ROWS * STRIDE, LANES), f32),
            pltpu.VMEM((max(chunks, rows), 8, LANES), f32),
            pltpu.VMEM((rows, LANES), f32),
            pltpu.VMEM((rows, LANES), jnp.int32),
            pltpu.VMEM((chunks, LANES), jnp.int32),
            pltpu.VMEM(params.shape, f32),
            pltpu.VMEM(params.shape, f32),
            pltpu.VMEM(params.shape, f32),
            pltpu.VMEM(params.shape, f32),
            pltpu.VMEM(params.shape, f32),
            pltpu.SemaphoreType.DMA((2, chunks // 8)),
            pltpu.SemaphoreType.DMA((3, chunks // 8)),
        ],
        compiler_params=pltpu.CompilerParams(vmem_limit_bytes=VMEM_LIMIT),
        name="second_owner",
    )(camera, params, first, second, slots, next_slots, packed)


def halves(value):
    high = value.astype(bf16)
    return high, (value - high.astype(f32)).astype(bf16)


def triangle_pair(forward):
    rows = lax.broadcasted_iota(jnp.int32, (LIST_LEN, LIST_LEN), 0)
    cols = lax.broadcasted_iota(jnp.int32, (LIST_LEN, LIST_LEN), 1)
    chosen = rows < cols if forward else rows > cols
    one = jnp.where(chosen, 1.0, 0.0).astype(bf16)
    return jnp.concatenate([one, one], axis=0)


def batch_tiles(tile_count):
    return 8


LOG2_E = 1.4426950408889634


def tile_offsets(splat_ref, tile, number):
    left = (number % TILES_X) * tile_edge
    top = (number // TILES_X) * tile_edge
    ids = lax.broadcasted_iota(jnp.int32, (8, LANES), 0)
    u = jnp.broadcast_to(splat_ref[tile, 0:1, :], (8, LANES))
    w = jnp.broadcast_to(splat_ref[tile, 1:2, :], (8, LANES))
    across = [u - ((ids + (left + 8 * h)).astype(f32) + 0.5) for h in range(2)]
    down = [w - ((ids + (top + 8 * h)).astype(f32) + 0.5) for h in range(2)]
    return across, down


def spread_row(ref, item, row):
    return jnp.broadcast_to(ref[item, row : row + 1, :], (8, LANES))


def alpha_phase(splat_ref, tile, number, item, row_ref, alpha_ref, odds_ref, pair_ref):
    a, b, c, o = [jnp.broadcast_to(splat_ref[tile, k : k + 1, :], (8, LANES)) for k in (2, 3, 4, 5)]
    across, down = tile_offsets(splat_ref, tile, number)
    base = item * TILE_PIXELS
    along = [((-0.5 * LOG2_E) * a) * x * x for x in across]
    for h in range(2):
        row_ref[item, 8 * h : 8 * h + 8, :] = ((-0.5 * LOG2_E) * c) * down[h] * down[h]
        row_ref[item, 16 + 8 * h : 24 + 8 * h, :] = ((-LOG2_E) * b) * down[h]
        if odds_ref is not None:
            row_ref[item, 32 + 8 * h : 40 + 8 * h, :] = down[h]
    for row in range(tile_edge):
        fixed = spread_row(row_ref, item, row)
        slope = spread_row(row_ref, item, 16 + row)
        logs = []
        for h in range(2):
            exponent = along[h] + (fixed + slope * across[h])
            alpha = o * jnp.exp2(exponent)
            log_clear = jnp.log(1.0 - alpha) * LOG2_E
            where = slice(base + row * tile_edge + 8 * h, base + row * tile_edge + 8 * h + 8)
            alpha_ref[where, :] = alpha
            if odds_ref is not None:
                odds_ref[where, :] = alpha * jnp.exp2(-log_clear)
            logs.append(log_clear)
        high, low = halves(jnp.concatenate(logs, axis=0))
        where = slice(base + row * tile_edge, base + (row + 1) * tile_edge)
        pair_ref[where, :LIST_LEN] = high
        pair_ref[where, LIST_LEN:] = low


def weight_phase(item, before_ref, alpha_ref, weight_ref, pair_ref):
    for row in range(tile_edge):
        start = item * TILE_PIXELS + row * tile_edge
        where = slice(start, start + tile_edge)
        weight = alpha_ref[where, :] * jnp.exp2(before_ref[where, :])
        if weight_ref is not None:
            weight_ref[where, :] = weight
        high, low = halves(weight)
        pair_ref[where, :LIST_LEN] = high
        pair_ref[where, LIST_LEN:] = low


def split_colours(splat_ref, tile):
    colours = splat_ref[tile, 6:14, :]
    high = colours.astype(bf16).astype(f32)
    return high, colours - high


def colour_sum(high, low, pair):
    upper = jnp.concatenate([high, high], axis=1)
    lower = jnp.concatenate([low, jnp.zeros_like(low)], axis=1)
    result = lax.dot_general(
        jnp.concatenate([upper, lower], axis=0).astype(bf16),
        pair,
        (((1,), (1,)), ((), ())),
        preferred_element_type=f32,
    )
    return result[0:8] + result[8:16]


def write_tiles(splat_ref):
    def write(group, vectors, last):
        for k in range(8):
            tile = group * 8 + k
            splat_ref[tile, 0:8, :] = vectors[k]
            splat_ref[tile, 8:9, :] = last[k : k + 1]
            splat_ref[tile, 9:16, :] = jnp.zeros((7, LANES), f32)

    return write


def staggered(stages, parts):
    for turn in range(len(stages) + parts - 1):
        for part in range(parts):
            if 0 <= turn - part < len(stages):
                stages[turn - part](part)


def train_body(
    numbers_ref,
    lists_ref,
    targets_ref,
    packed_ref,
    out_packed_ref,
    main_ref,
    last_ref,
    splat_ref,
    row_ref,
    alpha_ref,
    odds_ref,
    before_ref,
    weight_ref,
    log_pair_ref,
    pair_ref,
    pull_ref,
    grad_pair_ref,
    grad_ref,
    grad_last_ref,
    inverse_ref,
):
    tile_count = lists_ref.shape[0]
    chunks = packed_ref.shape[0]
    batch = batch_tiles(tile_count)
    parts = PARTS if batch % PARTS == 0 else 1
    size = batch // parts
    unpack(packed_ref, main_ref, last_ref, chunks)
    write = write_tiles(splat_ref)
    invert(lists_ref, tile_count, chunks, inverse_ref)
    permute_group(lists_ref, main_ref, last_ref, chunks, 0, write)
    forward = triangle_pair(True)
    backward = triangle_pair(False)

    def work(step):
        first = step * batch

        def items(part):
            return range(part * size, (part + 1) * size)

        def span(part):
            return slice(part * size * TILE_PIXELS, (part + 1) * size * TILE_PIXELS)

        def alphas(part):
            for item in items(part):
                tile = first + item
                alpha_phase(
                    splat_ref, tile, numbers_ref[tile], item, row_ref, alpha_ref, odds_ref, log_pair_ref
                )

        def befores(part):
            before_ref[span(part), :] = jnp.dot(
                log_pair_ref[span(part), :], forward, preferred_element_type=f32
            )

        def weights(part):
            for item in items(part):
                weight_phase(item, before_ref, alpha_ref, weight_ref, pair_ref)

        def deltas(part):
            for item in items(part):
                tile = first + item
                pixels = slice(item * TILE_PIXELS, (item + 1) * TILE_PIXELS)
                pair = pair_ref[pixels, :]
                high, low = split_colours(splat_ref, tile)
                rendered = colour_sum(high, low, pair)
                wanted = [targets_ref[channel, pl.ds(tile, 1), :] for channel in range(3)]
                wanted = jnp.concatenate(wanted + [jnp.zeros((5, TILE_PIXELS), f32)], axis=0)
                delta = rendered - wanted
                delta_high = delta.astype(bf16).astype(f32)
                delta_low = delta - delta_high
                left = jnp.concatenate(
                    [delta_high, delta_high, delta_low, jnp.zeros_like(delta)], axis=0
                ).astype(bf16)
                right = jnp.concatenate([high, low, high, jnp.zeros_like(high)], axis=0).astype(bf16)
                pulled = lax.dot_general(
                    left, right, (((0,), (0,)), ((), ())), preferred_element_type=f32
                )
                for row in range(tile_edge):
                    start = item * TILE_PIXELS + row * tile_edge
                    where = slice(start, start + tile_edge)
                    product = pulled[row * tile_edge : (row + 1) * tile_edge] * weight_ref[where, :]
                    pull_ref[where, :] = product
                    product_high, product_low = halves(product)
                    grad_pair_ref[where, :LIST_LEN] = product_high
                    grad_pair_ref[where, LIST_LEN:] = product_low
                colour = jnp.dot(
                    jnp.concatenate([delta_high, delta_low], axis=0).astype(bf16),
                    pair,
                    preferred_element_type=f32,
                )
                colour = colour[0:8, :LIST_LEN] + (colour[0:8, LIST_LEN:] + colour[8:16, :LIST_LEN])
                grad_ref[tile, 6:8, :] = colour[0:2]
                grad_last_ref[pl.ds(tile, 1), :] = colour[2:3]

        def afters(part):
            before_ref[span(part), :] = jnp.dot(
                grad_pair_ref[span(part), :], backward, preferred_element_type=f32
            )

        def moments(part):
            for item in items(part):
                tile = first + item
                across, down = tile_offsets(splat_ref, tile, numbers_ref[tile])
                sums = [[jnp.zeros((8, LANES), f32) for j in range(3)] for h in range(2)]
                for row in range(tile_edge):
                    offset = spread_row(row_ref, item, 32 + row)
                    for h in range(2):
                        start = item * TILE_PIXELS + row * tile_edge + 8 * h
                        where = slice(start, start + 8)
                        slope = pull_ref[where, :] - before_ref[where, :] * odds_ref[where, :]
                        once = slope * offset
                        sums[h][0] = sums[h][0] + slope
                        sums[h][1] = sums[h][1] + once
                        sums[h][2] = sums[h][2] + once * offset

                def total(pieces):
                    return jnp.sum(pieces[0] + pieces[1], axis=0, keepdims=True)

                whole = total([sums[h][0] for h in range(2)])
                along = [sums[h][0] * across[h] for h in range(2)]
                moment_x = total(along)
                moment_xx = total([along[h] * across[h] for h in range(2)])
                moment_y = total([sums[h][1] for h in range(2)])
                moment_xy = total([sums[h][1] * across[h] for h in range(2)])
                moment_yy = total([sums[h][2] for h in range(2)])
                a = splat_ref[tile, 2:3, :]
                b = splat_ref[tile, 3:4, :]
                c = splat_ref[tile, 4:5, :]
                grad_ref[tile, 0:1, :] = -(a * moment_x + b * moment_y)
                grad_ref[tile, 1:2, :] = -(c * moment_y + b * moment_x)
                grad_ref[tile, 2:3, :] = -0.5 * moment_xx
                grad_ref[tile, 3:4, :] = -moment_xy
                grad_ref[tile, 4:5, :] = -0.5 * moment_yy
                grad_ref[tile, 5:6, :] = whole

        staggered([alphas, befores, weights, deltas, afters, moments], parts)

    def batch_step(step, unused):
        work(step - 1)
        permute_group(lists_ref, main_ref, last_ref, chunks, step, write)
        return unused

    lax.fori_loop(1, tile_count // batch, batch_step, 0)
    work(tile_count // batch - 1)
    permute(
        inverse_ref,
        grad_ref,
        grad_last_ref,
        tile_count,
        out_packed_ref.shape[0],
        pack_group(out_packed_ref),
    )


def train(numbers, lists, targets, packed):
    tile_count = lists.shape[0]
    chunks = packed.shape[0]
    batch = batch_tiles(tile_count)
    pixels = batch * TILE_PIXELS
    plain = pltpu.VMEM((pixels, LIST_LEN), f32)
    pairs = pltpu.VMEM((pixels, 2 * LIST_LEN), bf16)
    return pl.pallas_call(
        train_body,
        out_shape=pltpu.VMEM(packed.shape, f32),
        in_specs=[SMEM, VMEM, VMEM, VMEM],
        out_specs=VMEM,
        scratch_shapes=[
            pltpu.VMEM((chunks, 8, LANES), f32),
            pltpu.VMEM((chunks, LANES), f32),
            pltpu.VMEM((tile_count, 16, LANES), f32),
            pltpu.VMEM((batch, 48, LANES), f32),
            plain,
            plain,
            plain,
            plain,
            pairs,
            pairs,
            plain,
            pairs,
            pltpu.VMEM((tile_count, 8, LANES), f32),
            pltpu.VMEM((tile_count, LANES), f32),
            pltpu.VMEM((chunks, LANES), jnp.int32),
        ],
        compiler_params=pltpu.CompilerParams(vmem_limit_bytes=VMEM_LIMIT),
        name="train_tiles",
    )(numbers, lists, targets, packed)


def render_body(
    numbers_ref,
    lists_ref,
    packed_ref,
    out_ref,
    main_ref,
    last_ref,
    splat_ref,
    row_ref,
    alpha_ref,
    before_ref,
    log_pair_ref,
    pair_ref,
):
    tile_count = lists_ref.shape[0]
    chunks = packed_ref.shape[0]
    batch = batch_tiles(tile_count)
    parts = PARTS if batch % PARTS == 0 else 1
    size = batch // parts
    unpack(packed_ref, main_ref, last_ref, chunks)
    write = write_tiles(splat_ref)
    permute_group(lists_ref, main_ref, last_ref, chunks, 0, write)
    forward = triangle_pair(True)

    def work(step):
        first = step * batch

        def items(part):
            return range(part * size, (part + 1) * size)

        def span(part):
            return slice(part * size * TILE_PIXELS, (part + 1) * size * TILE_PIXELS)

        def alphas(part):
            for item in items(part):
                tile = first + item
                alpha_phase(
                    splat_ref, tile, numbers_ref[tile], item, row_ref, alpha_ref, None, log_pair_ref
                )

        def befores(part):
            before_ref[span(part), :] = jnp.dot(
                log_pair_ref[span(part), :], forward, preferred_element_type=f32
            )

        def weights(part):
            for item in items(part):
                weight_phase(item, before_ref, alpha_ref, None, pair_ref)

        def colours(part):
            for item in items(part):
                tile = first + item
                high, low = split_colours(splat_ref, tile)
                pair = pair_ref[item * TILE_PIXELS : (item + 1) * TILE_PIXELS, :]
                rendered = colour_sum(high, low, pair)
                for channel in range(3):
                    out_ref[channel, pl.ds(tile, 1), :] = rendered[channel : channel + 1]

        staggered([alphas, befores, weights, colours], parts)

    def batch_step(step, unused):
        work(step - 1)
        permute_group(lists_ref, main_ref, last_ref, chunks, step, write)
        return unused

    lax.fori_loop(1, tile_count // batch, batch_step, 0)
    work(tile_count // batch - 1)


def render(numbers, lists, packed):
    tile_count = lists.shape[0]
    chunks = packed.shape[0]
    batch = batch_tiles(tile_count)
    pixels = batch * TILE_PIXELS
    plain = pltpu.VMEM((pixels, LIST_LEN), f32)
    pairs = pltpu.VMEM((pixels, 2 * LIST_LEN), bf16)
    return pl.pallas_call(
        render_body,
        out_shape=jax.ShapeDtypeStruct((3, tile_count, TILE_PIXELS), f32),
        in_specs=[SMEM, VMEM, VMEM],
        out_specs=VMEM,
        scratch_shapes=[
            pltpu.VMEM((chunks, 8, LANES), f32),
            pltpu.VMEM((chunks, LANES), f32),
            pltpu.VMEM((tile_count, 16, LANES), f32),
            pltpu.VMEM((batch, 48, LANES), f32),
            plain,
            plain,
            pairs,
            pairs,
        ],
        compiler_params=pltpu.CompilerParams(vmem_limit_bytes=VMEM_LIMIT),
        name="render_tiles",
    )(numbers, lists, packed)


def exchange(packed, devices):
    rows = packed.shape[0]
    if rows == devices:
        packed = lax.all_to_all(packed, "dev", split_axis=0, concat_axis=0, tiled=True)
        return pltpu.with_memory_space_constraint(packed, pltpu.VMEM)
    cap = rows * LANES // devices
    slots = packed.reshape(rows, ROWS, LANES).transpose(1, 0, 2).reshape(ROWS, devices, cap)
    slots = lax.all_to_all(slots, "dev", split_axis=1, concat_axis=1, tiled=True)
    slots = slots.reshape(ROWS, rows, LANES).transpose(1, 0, 2)
    return slots.reshape(rows, 1, ROWS * LANES)


def shards(
    gauss_params,
    adam_first,
    adam_second,
    camera,
    send_first,
    send_second,
    lists_first,
    lists_second,
    tiles_first,
    tiles_second,
    targets,
):
    devices = lax.axis_size("dev")
    half_width = 0.5 * TILES_X * tile_edge
    half_height = 0.5 * (lists_first.shape[0] * devices // TILES_X * tile_edge)
    keep = functools.partial(pltpu.with_memory_space_constraint, memory_space=pltpu.VMEM)
    leave = functools.partial(pltpu.with_memory_space_constraint, memory_space=pltpu.HBM)
    packed = first_owner(
        leave(camera), leave(gauss_params), leave(send_first), half_width, half_height
    )
    packed = exchange(packed, devices)
    packed = train(tiles_first, keep(lists_first), jnp.transpose(targets, (1, 0, 2)), packed)
    packed = exchange(packed, devices)
    new_params, new_first, new_second, packed = second_owner(
        camera,
        keep(gauss_params),
        leave(adam_first),
        leave(adam_second),
        keep(send_first),
        keep(send_second),
        packed,
        half_width,
        half_height,
    )
    packed = exchange(packed, devices)
    rendered = render(tiles_second, keep(lists_second), packed)
    return (new_params, new_first, new_second, jnp.transpose(rendered, (1, 0, 2)))


def solution(mesh):
    placed = (
        P(None, "dev"),
        P(None, "dev"),
        P(None, "dev"),
        P(),
        P("dev", None),
        P("dev", None),
        P("dev", None),
        P("dev", None),
        P("dev"),
        P("dev"),
        P("dev", None, None),
    )
    return jax.shard_map(
        shards,
        mesh=mesh,
        in_specs=placed,
        out_specs=(P(None, "dev"), P(None, "dev"), P(None, "dev"), P("dev", None, None)),
        check_vma=False,
    )
```

```python
import functools

import jax
import jax.numpy as jnp
import numpy as np
from jax import lax
from jax.experimental import pallas as pl
from jax.experimental.pallas import tpu as pltpu
from jax.sharding import PartitionSpec as P

PARAMS = 59
LIST_LEN = 128
TILE_PIXELS = 256
TILES_X = 128
LANES = 128
ROWS = 9
STRIDE = 72
PARTS = 4
BUFFERS = 2
VMEM_LIMIT = 36 << 20

tile_edge = 16
focal_length = 1000.0
blur_floor = 0.3
adam_epsilon = 1e-08
bias_first = 1.0 - 0.9**20
bias_second = 1.0 - 0.999**20
sh_first = 0.28209479177387814
sh_second = 0.4886025119029199
sh_third = (
    1.0925484305920792,
    -1.0925484305920792,
    0.31539156525252005,
    -1.0925484305920792,
    0.5462742152960396,
)
sh_fourth = (
    -0.5900435899266435,
    2.890611442640554,
    -0.4570457994644658,
    0.3731763325901154,
    -0.4570457994644658,
    1.445305721320277,
    -0.5900435899266435,
)

f32 = jnp.float32
bf16 = jnp.bfloat16
VMEM = pl.BlockSpec(memory_space=pltpu.VMEM)
SMEM = pl.BlockSpec(memory_space=pltpu.SMEM)
ANY = pl.BlockSpec(memory_space=pl.ANY)
HBM = pl.BlockSpec(memory_space=pltpu.HBM)


def rate_values():
    values = np.full((64,), 0.000125)
    values[0:3] = 0.00016
    values[3:6] = 0.005
    values[6:10] = 0.001
    values[10] = 0.05
    values[11] = 0.0025
    values[27] = 0.0025
    values[43] = 0.0025
    return values


def camera_frame(camera_ref, view):
    shape = (8, LANES)
    angle = [jnp.full(shape, camera_ref[view, k], f32) for k in range(3)]
    shift = [jnp.full(shape, camera_ref[view, 3 + k], f32) for k in range(3)]
    (ca, cb, cc) = [jnp.cos(x) for x in angle]
    (sa, sb, sc) = [jnp.sin(x) for x in angle]
    rot = [
        [cc * cb, cc * sb * sa - sc * ca, cc * sb * ca + sc * sa],
        [sc * cb, sc * sb * sa + cc * ca, sc * sb * ca - cc * sa],
        [-sb, cb * sa, cb * ca],
    ]
    back = [
        rot[0][k] * shift[0] + rot[1][k] * shift[1] + rot[2][k] * shift[2]
        for k in range(3)
    ]
    return rot, shift, back


def sh_terms(x, y, z):
    xx, yy, zz = (x * x, y * y, z * z)
    return [
        -sh_second * y,
        sh_second * z,
        -sh_second * x,
        sh_third[0] * x * y,
        sh_third[1] * y * z,
        sh_third[2] * (2.0 * zz - xx - yy),
        sh_third[3] * x * z,
        sh_third[4] * (xx - yy),
        sh_fourth[0] * y * (3.0 * xx - yy),
        sh_fourth[1] * x * y * z,
        sh_fourth[2] * y * (4.0 * zz - xx - yy),
        sh_fourth[3] * z * (2.0 * zz - 3.0 * xx - 3.0 * yy),
        sh_fourth[4] * x * (4.0 * zz - xx - yy),
        sh_fourth[5] * z * (xx - yy),
        sh_fourth[6] * x * (xx - 3.0 * yy),
    ]


def project(params, frame, half_width, half_height):
    rot, shift, back = frame
    centres = params[0:3]
    viewed = [
        rot[k][0] * centres[0] + rot[k][1] * centres[1] + rot[k][2] * centres[2] + shift[k]
        for k in range(3)
    ]
    inverse = 1.0 / viewed[2]
    scale_z = focal_length * inverse
    u_off = scale_z * viewed[0]
    w_off = scale_z * viewed[1]
    slope_u = u_off * inverse
    slope_w = w_off * inverse
    scales = [jnp.exp(params[3 + k]) for k in range(3)]
    q = params[6:10]
    norm = lax.rsqrt(q[0] * q[0] + q[1] * q[1] + q[2] * q[2] + q[3] * q[3])
    qw, qx, qy, qz = [v * norm for v in q]
    turn = [
        [
            1.0 - 2.0 * (qy * qy + qz * qz),
            2.0 * (qx * qy - qw * qz),
            2.0 * (qx * qz + qw * qy),
        ],
        [
            2.0 * (qx * qy + qw * qz),
            1.0 - 2.0 * (qx * qx + qz * qz),
            2.0 * (qy * qz - qw * qx),
        ],
        [
            2.0 * (qx * qz - qw * qy),
            2.0 * (qy * qz + qw * qx),
            1.0 - 2.0 * (qx * qx + qy * qy),
        ],
    ]
    mapping = [
        [scale_z * rot[0][k] - slope_u * rot[2][k] for k in range(3)],
        [scale_z * rot[1][k] - slope_w * rot[2][k] for k in range(3)],
    ]
    factor = [
        [
            (row[0] * turn[0][k] + row[1] * turn[1][k] + row[2] * turn[2][k]) * scales[k]
            for k in range(3)
        ]
        for row in mapping
    ]
    first, second = factor
    cover_a = first[0] * first[0] + first[1] * first[1] + first[2] * first[2] + blur_floor
    cover_b = first[0] * second[0] + first[1] * second[1] + first[2] * second[2]
    cover_c = second[0] * second[0] + second[1] * second[1] + second[2] * second[2] + blur_floor
    scale_det = 1.0 / (cover_a * cover_c - cover_b * cover_b)
    opacity = 1.0 / (1.0 + jnp.exp(-params[10]))
    towards = [centres[k] + back[k] for k in range(3)]
    length = lax.rsqrt(
        towards[0] * towards[0] + towards[1] * towards[1] + towards[2] * towards[2]
    )
    harmonics = sh_terms(*[v * length for v in towards])
    colours = []
    for channel in range(3):
        running = 0.5 + sh_first * params[11 + 16 * channel]
        for term in range(15):
            running = running + harmonics[term] * params[12 + 16 * channel + term]
        colours.append(jnp.maximum(running, 0.0))
    return [
        u_off + half_width,
        w_off + half_height,
        cover_c * scale_det,
        -cover_b * scale_det,
        cover_a * scale_det,
        opacity,
    ] + colours


def permute_group(idx_ref, main_ref, last_ref, chunks, group, write):
    base = group * 8 if isinstance(group, int) else pl.multiple_of(group * 8, 8)
    index = idx_ref[pl.ds(base, 8), :]
    high = index >> 7
    low = index & 127
    totals = []
    for k in range(8):
        row_high = jnp.broadcast_to(high[k : k + 1], (8, LANES))
        row_low = jnp.broadcast_to(low[k : k + 1], (8, LANES))
        total = jnp.zeros((8, LANES), f32)
        for chunk in range(chunks):
            found = jnp.take_along_axis(
                main_ref[chunk], row_low, axis=1, mode="promise_in_bounds"
            )
            total = jnp.where(row_high == chunk, found, total)
        totals.append(total)
    total = jnp.zeros((8, LANES), f32)
    for chunk in range(chunks):
        source = jnp.broadcast_to(last_ref[chunk : chunk + 1, :], (8, LANES))
        found = jnp.take_along_axis(source, low, axis=1, mode="promise_in_bounds")
        total = jnp.where(high == chunk, found, total)
    write(group, totals, total)


def permute(idx_ref, main_ref, last_ref, chunks, rows, write):
    def group_step(group, unused):
        permute_group(idx_ref, main_ref, last_ref, chunks, group, write)
        return unused

    lax.fori_loop(0, rows // 8, group_step, 0)


def invert(idx_ref, rows, high_count, inverse_ref):
    index = idx_ref[...]
    high = index >> 7
    low = index & 127
    high_ids = lax.broadcasted_iota(jnp.int32, (high_count, LANES), 0)
    low_ids = lax.broadcasted_iota(jnp.int32, (LANES, LANES), 0)
    lane_ids = lax.broadcasted_iota(jnp.int32, (high_count, LANES), 1).astype(f32)
    total = jnp.zeros((2 * high_count, LANES), f32)
    for start in range(0, rows, 8):
        left = []
        right = []
        for row in range(start, start + 8):
            here = high[row : row + 1] == high_ids
            left.append(
                jnp.concatenate(
                    [jnp.where(here, row + 1.0, 0.0), jnp.where(here, lane_ids, 0.0)], axis=0
                ).astype(bf16)
            )
            right.append(jnp.where(low[row : row + 1] == low_ids, 1.0, 0.0).astype(bf16))
        total = total + lax.dot_general(
            jnp.concatenate(left, axis=1),
            jnp.concatenate(right, axis=1),
            (((1,), (1,)), ((), ())),
            preferred_element_type=f32,
        )
    rows_found = total[:high_count].astype(jnp.int32)
    lanes_found = total[high_count:].astype(jnp.int32)
    inverse_ref[...] = (rows_found - 1) * LANES + lanes_found


def unpack(packed_ref, main_ref, last_ref, chunks):
    for chunk in range(chunks):
        for k in range(8):
            main_ref[chunk, k : k + 1, :] = packed_ref[chunk, :, k * LANES : (k + 1) * LANES]
        last_ref[chunk : chunk + 1, :] = packed_ref[chunk, :, 8 * LANES : 9 * LANES]


def pack_group(packed_ref):
    def write(group, vectors, last):
        for k in range(8):
            row = group * 8 + k
            for item in range(8):
                packed_ref[row, :, item * LANES : (item + 1) * LANES] = vectors[k][
                    item : item + 1
                ]
            packed_ref[row, :, 8 * LANES : 9 * LANES] = last[k : k + 1]

    return write


def slots_as_rows(slots_ref, idx_ref, rows):
    for row in range(rows):
        idx_ref[row : row + 1, :] = slots_ref[:, row * LANES : (row + 1) * LANES]


def native_to_group(native, ref, block, k):
    if native.shape[0] == 8:
        ref[pl.ds(64 * block + k, 8, stride=8), :] = native
    else:
        for row in range(native.shape[0]):
            target = 64 * block + 8 * row + k
            ref[target : target + 1, :] = native[row : row + 1]


def dense_load(dense_ref, row, group):
    return dense_ref[pl.ds(pl.multiple_of(row * STRIDE + group * 8, 8), 8), :]


def dense_store(dense_ref, row, group, value):
    dense_ref[pl.ds(pl.multiple_of(row * STRIDE + group * 8, 8), 8), :] = value


def row_blocks():
    return [(block, min(8, PARAMS - 8 * block)) for block in range((PARAMS + 7) // 8)]


def split_splats(splat_ref, parts_ref, chunks):
    for row in range(ROWS):
        for start in range(0, chunks, 16):
            value = splat_ref[row * STRIDE + start : row * STRIDE + start + 16, :]
            target = slice(row * chunks + start, row * chunks + start + 16)
            for term in range(3):
                rounded = value.astype(bf16)
                parts_ref[target, term * LANES : (term + 1) * LANES] = rounded
                value = value - rounded.astype(f32)


def matrix_gather(parts_ref, idx_ref, base, chunks, packed_ref):
    index = idx_ref[pl.ds(pl.multiple_of(base, 8), 8), :]
    high = index >> 7
    low = index & 127
    low_ids = lax.broadcasted_iota(jnp.int32, (LANES, LANES), 0)
    ids = lax.broadcasted_iota(jnp.int32, (8, LANES), 0)
    for pair in range(4):
        rows = (2 * pair, 2 * pair + 1)
        chosen = jnp.concatenate(
            [jnp.where(low[row : row + 1] == low_ids, 1.0, 0.0) for row in rows], axis=1
        ).astype(bf16)
        found = jnp.dot(
            parts_ref[...],
            jnp.concatenate([chosen, chosen, chosen], axis=0),
            preferred_element_type=f32,
        )
        for half, row in enumerate(rows):
            wanted = jnp.broadcast_to(high[row : row + 1], (8, LANES))
            masks = [ids + 8 * block == wanted for block in range(chunks // 8)]
            for item in range(ROWS):
                total = jnp.zeros((8, LANES), f32)
                for block in range(chunks // 8):
                    start = item * chunks + 8 * block
                    piece = found[start : start + 8, half * LANES : (half + 1) * LANES]
                    total = jnp.where(masks[block], piece, total)
                packed_ref[base + row, :, item * LANES : (item + 1) * LANES] = jnp.sum(
                    total, axis=0, keepdims=True
                )


def send_splats(splat_ref, main_ref, parts_ref, idx_ref, packed_ref, chunks, rows):
    for chunk in range(chunks):
        main_ref[chunk] = splat_ref[pl.ds(chunk, 8, stride=STRIDE), :]
    last_ref = splat_ref.at[pl.ds(8 * STRIDE, chunks), :]
    split_splats(splat_ref, parts_ref, chunks)
    write = pack_group(packed_ref)

    def step(group, unused):
        matrix_gather(parts_ref, idx_ref, rows // 2 + 8 * group, chunks, packed_ref)
        permute_group(idx_ref, main_ref, last_ref, chunks, group, write)
        return unused

    lax.fori_loop(0, rows // 16, step, 0)


def first_owner_body(
    half_width,
    half_height,
    camera_hbm,
    params_hbm,
    slots_hbm,
    packed_ref,
    params_ref,
    slots_ref,
    camera_ref,
    even_ref,
    odd_ref,
    splat_ref,
    main_ref,
    parts_ref,
    idx_ref,
    sems,
):
    chunks = params_hbm.shape[1] // LANES
    rows = slots_hbm.shape[1] // LANES
    groups = chunks // 8
    small = [
        pltpu.make_async_copy(camera_hbm, camera_ref, sems.at[groups]),
        pltpu.make_async_copy(slots_hbm, slots_ref, sems.at[groups + 1]),
    ]

    def load(group):
        columns = pl.ds(pl.multiple_of(group * (8 * LANES), 8 * LANES), 8 * LANES)
        return pltpu.make_async_copy(
            params_hbm.at[:, columns], params_ref.at[:, columns], sems.at[group]
        )

    for copy in small:
        copy.start()
    for group in range(groups):
        load(group).start()
    for copy in small:
        copy.wait()
    frame = camera_frame(camera_ref, 0)

    def prepare(group, dense_ref):
        for k in range(8):
            chunk = group * 8 + k
            lanes = pl.ds(pl.multiple_of(chunk * LANES, LANES), LANES)
            for block, size in row_blocks():
                native_to_group(
                    params_ref[8 * block : 8 * block + size, lanes], dense_ref, block, k
                )
        params = [dense_ref[8 * row : 8 * row + 8, :] for row in range(PARAMS)]
        for row, value in enumerate(project(params, frame, half_width, half_height)):
            dense_store(splat_ref, row, group, value)

    def step(pair, unused):
        load(2 * pair).wait()
        load(2 * pair + 1).wait()
        prepare(2 * pair, even_ref)
        prepare(2 * pair + 1, odd_ref)
        return unused

    lax.fori_loop(0, groups // 2, step, 0)
    slots_as_rows(slots_ref, idx_ref, rows)
    send_splats(splat_ref, main_ref, parts_ref, idx_ref, packed_ref, chunks, rows)


def first_owner(camera, params, slots, half_width, half_height):
    chunks = params.shape[1] // LANES
    rows = slots.shape[1] // LANES
    return pl.pallas_call(
        functools.partial(first_owner_body, half_width, half_height),
        out_shape=(pltpu.VMEM((rows, 1, ROWS * LANES), f32), pltpu.VMEM(params.shape, f32)),
        in_specs=[HBM, HBM, HBM],
        out_specs=(VMEM, VMEM),
        scratch_shapes=[
            pltpu.VMEM(slots.shape, jnp.int32),
            pltpu.SMEM(camera.shape, f32),
            pltpu.VMEM((64 * 8, LANES), f32),
            pltpu.VMEM((64 * 8, LANES), f32),
            pltpu.VMEM((ROWS * STRIDE, LANES), f32),
            pltpu.VMEM((chunks, 8, LANES), f32),
            pltpu.VMEM((ROWS * chunks, 3 * LANES), bf16),
            pltpu.VMEM((rows, LANES), jnp.int32),
            pltpu.SemaphoreType.DMA((chunks // 8 + 2,)),
        ],
        compiler_params=pltpu.CompilerParams(vmem_limit_bytes=VMEM_LIMIT),
        name="first_owner",
    )(camera, params, slots)


def second_owner_body(
    half_width,
    half_height,
    camera_ref,
    params_ref,
    first_hbm,
    second_hbm,
    slots_ref,
    next_slots_ref,
    packed_ref,
    out_params_hbm,
    out_first_hbm,
    out_second_hbm,
    out_packed_ref,
    dense_ref,
    grad_ref,
    fresh_ref,
    splat_ref,
    next_splat_ref,
    main_ref,
    parts_ref,
    last_ref,
    idx_ref,
    inverse_ref,
    first_ref,
    second_ref,
    params_out_ref,
    first_out_ref,
    second_out_ref,
    load_sems,
    store_sems,
):
    chunks = params_ref.shape[1] // LANES
    rows = slots_ref.shape[1] // LANES
    groups = chunks // 8

    def columns_of(group):
        return pl.ds(pl.multiple_of(group * (8 * LANES), 8 * LANES), 8 * LANES)

    def loads(group):
        columns = columns_of(group)
        return [
            pltpu.make_async_copy(
                source.at[:, columns], target.at[:, columns], load_sems.at[number, group]
            )
            for number, (source, target) in enumerate(
                [(first_hbm, first_ref), (second_hbm, second_ref)]
            )
        ]

    for group in range(groups):
        for copy in loads(group):
            copy.start()
    slots_as_rows(slots_ref, idx_ref, rows)
    invert(idx_ref, rows, chunks, inverse_ref)
    unpack(packed_ref, main_ref, last_ref, rows)
    frame = camera_frame(camera_ref, 0)
    next_frame = camera_frame(camera_ref, 1)
    rates = rate_values() / bias_first
    row_ids = lax.broadcasted_iota(jnp.int32, (8, LANES), 0)

    def write_columns(group, vectors, last):
        for k in range(8):
            splat_ref[pl.ds(group * 8 + k, 8, stride=STRIDE), :] = vectors[k]
        dense_store(splat_ref, 8, group, last)

    def lanes_of(group, k):
        start = pl.multiple_of(group * (8 * LANES), 8 * LANES) + k * LANES
        return pl.ds(pl.multiple_of(start, LANES), LANES)

    def stores(group):
        columns = columns_of(group)
        return [
            pltpu.make_async_copy(
                source.at[:, columns], target.at[:, columns], store_sems.at[number, group]
            )
            for number, (source, target) in enumerate(
                [
                    (params_out_ref, out_params_hbm),
                    (first_out_ref, out_first_hbm),
                    (second_out_ref, out_second_hbm),
                ]
            )
        ]

    def work(group):
        for copy in loads(group):
            copy.wait()
        for block, size in row_blocks():
            for k in range(8):
                native = params_ref[8 * block : 8 * block + size, lanes_of(group, k)]
                native_to_group(native, dense_ref, block, k)
        params = [dense_ref[8 * row : 8 * row + 8, :] for row in range(PARAMS)]
        splats, pullback = jax.vjp(
            lambda *p: project(list(p), frame, half_width, half_height), *params
        )
        cotangents = [dense_load(splat_ref, row, group) for row in range(ROWS)]
        through_opacity = cotangents[5] * (1.0 - splats[5])
        cotangents[5] = jnp.zeros_like(cotangents[5])
        grads = list(pullback(cotangents))
        grads[10] = through_opacity
        for row, value in enumerate(grads):
            grad_ref[8 * row : 8 * row + 8, :] = value
        for block, size in row_blocks():
            span = slice(8 * block, 8 * block + size)
            block_rates = rates[8 * block : 8 * block + 8]
            step_size = jnp.full((8, LANES), block_rates[0], f32)
            for k in range(1, 8):
                if block_rates[k] != block_rates[0]:
                    step_size = jnp.where(row_ids == k, f32(block_rates[k]), step_size)
            step_size = step_size[:size]
            for k in range(8):
                lanes = lanes_of(group, k)
                gradient = grad_ref[pl.ds(64 * block + k, 8, stride=8), :][:size]
                moment = 0.9 * first_ref[span, lanes] + 0.1 * gradient
                square = 0.999 * second_ref[span, lanes] + 0.001 * gradient * gradient
                scaled = square * (1.0 / bias_second)
                root = scaled * lax.rsqrt(scaled)
                fresh = params_ref[span, lanes] - step_size * moment / (root + adam_epsilon)
                first_out_ref[span, lanes] = moment
                second_out_ref[span, lanes] = square
                params_out_ref[span, lanes] = fresh
                native_to_group(fresh, fresh_ref, block, k)
        for copy in stores(group):
            copy.start()
        params = [fresh_ref[8 * row : 8 * row + 8, :] for row in range(PARAMS)]
        for row, value in enumerate(project(params, next_frame, half_width, half_height)):
            dense_store(next_splat_ref, row, group, value)

    permute_group(inverse_ref, main_ref, last_ref, rows, 0, write_columns)

    def step(group, unused):
        work(group - 1)
        permute_group(inverse_ref, main_ref, last_ref, rows, group, write_columns)
        return unused

    lax.fori_loop(1, groups, step, 0)
    work(groups - 1)
    slots_as_rows(next_slots_ref, idx_ref, rows)
    send_splats(next_splat_ref, main_ref, parts_ref, idx_ref, out_packed_ref, chunks, rows)
    for group in range(groups):
        for copy in stores(group):
            copy.wait()


def second_owner(camera, params, first, second, slots, next_slots, packed, half_width, half_height):
    chunks = params.shape[1] // LANES
    rows = slots.shape[1] // LANES
    shape = jax.ShapeDtypeStruct(params.shape, f32)
    return pl.pallas_call(
        functools.partial(second_owner_body, half_width, half_height),
        out_shape=(shape, shape, shape, pltpu.VMEM((rows, 1, ROWS * LANES), f32)),
        in_specs=[SMEM, VMEM, HBM, HBM, VMEM, VMEM, VMEM],
        out_specs=(ANY, ANY, ANY, VMEM),
        scratch_shapes=[
            pltpu.VMEM((64 * 8, LANES), f32),
            pltpu.VMEM((64 * 8, LANES), f32),
            pltpu.VMEM((64 * 8, LANES), f32),
            pltpu.VMEM((ROWS * STRIDE, LANES), f32),
            pltpu.VMEM((ROWS * STRIDE, LANES), f32),
            pltpu.VMEM((max(chunks, rows), 8, LANES), f32),
            pltpu.VMEM((ROWS * chunks, 3 * LANES), bf16),
            pltpu.VMEM((rows, LANES), f32),
            pltpu.VMEM((rows, LANES), jnp.int32),
            pltpu.VMEM((chunks, LANES), jnp.int32),
            pltpu.VMEM(params.shape, f32),
            pltpu.VMEM(params.shape, f32),
            pltpu.VMEM(params.shape, f32),
            pltpu.VMEM(params.shape, f32),
            pltpu.VMEM(params.shape, f32),
            pltpu.SemaphoreType.DMA((2, chunks // 8)),
            pltpu.SemaphoreType.DMA((3, chunks // 8)),
        ],
        compiler_params=pltpu.CompilerParams(vmem_limit_bytes=VMEM_LIMIT),
        name="second_owner",
    )(camera, params, first, second, slots, next_slots, packed)


def halves(value):
    high = value.astype(bf16)
    return high, (value - high.astype(f32)).astype(bf16)


def triangle_pair(forward):
    rows = lax.broadcasted_iota(jnp.int32, (LIST_LEN, LIST_LEN), 0)
    cols = lax.broadcasted_iota(jnp.int32, (LIST_LEN, LIST_LEN), 1)
    chosen = rows < cols if forward else rows > cols
    one = jnp.where(chosen, 1.0, 0.0).astype(bf16)
    return jnp.concatenate([one, one], axis=0)


def batch_tiles(tile_count):
    return 8


LOG2_E = 1.4426950408889634


def tile_offsets(splat_ref, tile, number):
    left = (number % TILES_X) * tile_edge
    top = (number // TILES_X) * tile_edge
    ids = lax.broadcasted_iota(jnp.int32, (8, LANES), 0)
    u = jnp.broadcast_to(splat_ref[tile, 0:1, :], (8, LANES))
    w = jnp.broadcast_to(splat_ref[tile, 1:2, :], (8, LANES))
    across = [u - ((ids + (left + 8 * h)).astype(f32) + 0.5) for h in range(2)]
    down = [w - ((ids + (top + 8 * h)).astype(f32) + 0.5) for h in range(2)]
    return across, down


def spread_row(ref, item, row):
    return jnp.broadcast_to(ref[item, row : row + 1, :], (8, LANES))


def alpha_phase(splat_ref, tile, number, item, row_ref, alpha_ref, odds_ref, pair_ref):
    a, b, c, o = [jnp.broadcast_to(splat_ref[tile, k : k + 1, :], (8, LANES)) for k in (2, 3, 4, 5)]
    across, down = tile_offsets(splat_ref, tile, number)
    base = item * TILE_PIXELS
    along = [((-0.5 * LOG2_E) * a) * x * x for x in across]
    for h in range(2):
        row_ref[item, 8 * h : 8 * h + 8, :] = ((-0.5 * LOG2_E) * c) * down[h] * down[h]
        row_ref[item, 16 + 8 * h : 24 + 8 * h, :] = ((-LOG2_E) * b) * down[h]
        if odds_ref is not None:
            row_ref[item, 32 + 8 * h : 40 + 8 * h, :] = down[h]
    for row in range(tile_edge):
        fixed = spread_row(row_ref, item, row)
        slope = spread_row(row_ref, item, 16 + row)
        logs = []
        for h in range(2):
            exponent = along[h] + (fixed + slope * across[h])
            alpha = o * jnp.exp2(exponent)
            log_clear = jnp.log(1.0 - alpha) * LOG2_E
            where = slice(base + row * tile_edge + 8 * h, base + row * tile_edge + 8 * h + 8)
            alpha_ref[where, :] = alpha
            if odds_ref is not None:
                odds_ref[where, :] = alpha * jnp.exp2(-log_clear)
            logs.append(log_clear)
        high, low = halves(jnp.concatenate(logs, axis=0))
        where = slice(base + row * tile_edge, base + (row + 1) * tile_edge)
        pair_ref[where, :LIST_LEN] = high
        pair_ref[where, LIST_LEN:] = low


def weight_phase(item, before_ref, alpha_ref, weight_ref, pair_ref):
    for row in range(tile_edge):
        start = item * TILE_PIXELS + row * tile_edge
        where = slice(start, start + tile_edge)
        weight = alpha_ref[where, :] * jnp.exp2(before_ref[where, :])
        if weight_ref is not None:
            weight_ref[where, :] = weight
        high, low = halves(weight)
        pair_ref[where, :LIST_LEN] = high
        pair_ref[where, LIST_LEN:] = low


def split_colours(splat_ref, tile):
    colours = splat_ref[tile, 6:14, :]
    high = colours.astype(bf16).astype(f32)
    return high, colours - high


def colour_sum(high, low, pair):
    upper = jnp.concatenate([high, high], axis=1)
    lower = jnp.concatenate([low, jnp.zeros_like(low)], axis=1)
    result = lax.dot_general(
        jnp.concatenate([upper, lower], axis=0).astype(bf16),
        pair,
        (((1,), (1,)), ((), ())),
        preferred_element_type=f32,
    )
    return result[0:8] + result[8:16]


def write_tiles(splat_ref):
    def write(group, vectors, last):
        for k in range(8):
            tile = group * 8 + k
            splat_ref[tile, 0:8, :] = vectors[k]
            splat_ref[tile, 8:9, :] = last[k : k + 1]
            splat_ref[tile, 9:16, :] = jnp.zeros((7, LANES), f32)

    return write


def staggered(stages, parts):
    for turn in range(len(stages) + parts - 1):
        for part in range(parts):
            if 0 <= turn - part < len(stages):
                stages[turn - part](part)


def train_body(
    numbers_ref,
    lists_ref,
    targets_ref,
    packed_ref,
    out_packed_ref,
    main_ref,
    last_ref,
    splat_ref,
    row_ref,
    alpha_ref,
    odds_ref,
    before_ref,
    weight_ref,
    log_pair_ref,
    pair_ref,
    pull_ref,
    grad_pair_ref,
    grad_ref,
    parts_ref,
    inverse_ref,
):
    tile_count = lists_ref.shape[0]
    chunks = packed_ref.shape[0]
    batch = batch_tiles(tile_count)
    parts = PARTS if batch % PARTS == 0 else 1
    size = batch // parts
    unpack(packed_ref, main_ref, last_ref, chunks)
    write = write_tiles(splat_ref)
    invert(lists_ref, tile_count, chunks, inverse_ref)
    permute_group(lists_ref, main_ref, last_ref, chunks, 0, write)
    forward = triangle_pair(True)
    backward = triangle_pair(False)

    def put(item, tile, value):
        grad_ref[pl.ds(item * STRIDE + tile, 1), :] = value

    def work(step):
        slot = (step % BUFFERS) * batch if isinstance(step, int) else 0
        first = step * batch - slot

        def items(part):
            return range(slot + part * size, slot + (part + 1) * size)

        def span(part):
            start = (slot + part * size) * TILE_PIXELS
            return slice(start, start + size * TILE_PIXELS)

        def alphas(part):
            for item in items(part):
                tile = first + item
                alpha_phase(
                    splat_ref, tile, numbers_ref[tile], item, row_ref, alpha_ref, odds_ref, log_pair_ref
                )

        def befores(part):
            before_ref[span(part), :] = jnp.dot(
                log_pair_ref[span(part), :], forward, preferred_element_type=f32
            )

        def weights(part):
            for item in items(part):
                weight_phase(item, before_ref, alpha_ref, weight_ref, pair_ref)

        def deltas(part):
            members = items(part)
            for start in range(0, len(members), 2):
                pair_items = members[start : start + 2]
                lefts = []
                rights = []
                for place, item in enumerate(pair_items):
                    tile = first + item
                    pixels = slice(item * TILE_PIXELS, (item + 1) * TILE_PIXELS)
                    pair = pair_ref[pixels, :]
                    high, low = split_colours(splat_ref, tile)
                    rendered = colour_sum(high, low, pair)
                    wanted = [targets_ref[channel, pl.ds(tile, 1), :] for channel in range(3)]
                    wanted = jnp.concatenate(wanted + [jnp.zeros((5, TILE_PIXELS), f32)], axis=0)
                    delta = rendered - wanted
                    delta_high = delta.astype(bf16).astype(f32)
                    delta_low = delta - delta_high
                    lefts += [delta_high, delta_high, delta_low, jnp.zeros_like(delta)]
                    right = jnp.concatenate([high, low, high, jnp.zeros_like(high)], axis=0)
                    blank = [jnp.zeros_like(right)] * len(pair_items)
                    blank[place] = right
                    rights.append(jnp.concatenate(blank, axis=1))
                    colour = jnp.dot(
                        jnp.concatenate([delta_high, delta_low], axis=0).astype(bf16),
                        pair,
                        preferred_element_type=f32,
                    )
                    colour = colour[0:8, :LIST_LEN] + (
                        colour[0:8, LIST_LEN:] + colour[8:16, :LIST_LEN]
                    )
                    for channel in range(3):
                        put(6 + channel, tile, colour[channel : channel + 1])
                pulled = lax.dot_general(
                    jnp.concatenate(lefts, axis=0).astype(bf16),
                    jnp.concatenate(rights, axis=0).astype(bf16),
                    (((0,), (0,)), ((), ())),
                    preferred_element_type=f32,
                )
                for place, item in enumerate(pair_items):
                    lanes = slice(place * LIST_LEN, (place + 1) * LIST_LEN)
                    for row in range(tile_edge):
                        begin = item * TILE_PIXELS + row * tile_edge
                        where = slice(begin, begin + tile_edge)
                        factor = pulled[row * tile_edge : (row + 1) * tile_edge, lanes]
                        product = factor * weight_ref[where, :]
                        pull_ref[where, :] = product
                        product_high, product_low = halves(product)
                        grad_pair_ref[where, :LIST_LEN] = product_high
                        grad_pair_ref[where, LIST_LEN:] = product_low

        def afters(part):
            before_ref[span(part), :] = jnp.dot(
                grad_pair_ref[span(part), :], backward, preferred_element_type=f32
            )

        def moments(part):
            for item in items(part):
                tile = first + item
                across, down = tile_offsets(splat_ref, tile, numbers_ref[tile])
                sums = [[jnp.zeros((8, LANES), f32) for j in range(3)] for h in range(2)]
                for row in range(tile_edge):
                    offset = spread_row(row_ref, item, 32 + row)
                    for h in range(2):
                        start = item * TILE_PIXELS + row * tile_edge + 8 * h
                        where = slice(start, start + 8)
                        slope = pull_ref[where, :] - before_ref[where, :] * odds_ref[where, :]
                        once = slope * offset
                        sums[h][0] = sums[h][0] + slope
                        sums[h][1] = sums[h][1] + once
                        sums[h][2] = sums[h][2] + once * offset

                def total(pieces):
                    return jnp.sum(pieces[0] + pieces[1], axis=0, keepdims=True)

                whole = total([sums[h][0] for h in range(2)])
                along = [sums[h][0] * across[h] for h in range(2)]
                moment_x = total(along)
                moment_xx = total([along[h] * across[h] for h in range(2)])
                moment_y = total([sums[h][1] for h in range(2)])
                moment_xy = total([sums[h][1] * across[h] for h in range(2)])
                moment_yy = total([sums[h][2] for h in range(2)])
                a = splat_ref[tile, 2:3, :]
                b = splat_ref[tile, 3:4, :]
                c = splat_ref[tile, 4:5, :]
                put(0, tile, -(a * moment_x + b * moment_y))
                put(1, tile, -(c * moment_y + b * moment_x))
                put(2, tile, -0.5 * moment_xx)
                put(3, tile, -moment_xy)
                put(4, tile, -0.5 * moment_yy)
                put(5, tile, whole)

        staggered([alphas, befores, weights, deltas, afters, moments], parts)

    def batch_step(step, unused):
        work(step - 1)
        permute_group(lists_ref, main_ref, last_ref, chunks, step, write)
        return unused

    lax.fori_loop(1, tile_count // batch, batch_step, 0)
    work(tile_count // batch - 1)
    send_splats(
        grad_ref, main_ref, parts_ref, inverse_ref, out_packed_ref, tile_count, chunks
    )


def train(numbers, lists, targets, packed):
    tile_count = lists.shape[0]
    chunks = packed.shape[0]
    batch = batch_tiles(tile_count)
    pixels = BUFFERS * batch * TILE_PIXELS
    plain = pltpu.VMEM((pixels, LIST_LEN), f32)
    pairs = pltpu.VMEM((pixels, 2 * LIST_LEN), bf16)
    return pl.pallas_call(
        train_body,
        out_shape=pltpu.VMEM(packed.shape, f32),
        in_specs=[SMEM, VMEM, VMEM, VMEM],
        out_specs=VMEM,
        scratch_shapes=[
            pltpu.VMEM((max(chunks, tile_count), 8, LANES), f32),
            pltpu.VMEM((chunks, LANES), f32),
            pltpu.VMEM((tile_count, 16, LANES), f32),
            pltpu.VMEM((BUFFERS * batch, 48, LANES), f32),
            plain,
            plain,
            plain,
            plain,
            pairs,
            pairs,
            plain,
            pairs,
            pltpu.VMEM((ROWS * STRIDE, LANES), f32),
            pltpu.VMEM((ROWS * tile_count, 3 * LANES), bf16),
            pltpu.VMEM((chunks, LANES), jnp.int32),
        ],
        compiler_params=pltpu.CompilerParams(vmem_limit_bytes=VMEM_LIMIT),
        name="train_tiles",
    )(numbers, lists, targets, packed)


def render_body(
    numbers_ref,
    lists_ref,
    packed_ref,
    out_ref,
    main_ref,
    last_ref,
    splat_ref,
    row_ref,
    alpha_ref,
    before_ref,
    log_pair_ref,
    pair_ref,
):
    tile_count = lists_ref.shape[0]
    chunks = packed_ref.shape[0]
    batch = batch_tiles(tile_count)
    parts = PARTS if batch % PARTS == 0 else 1
    size = batch // parts
    unpack(packed_ref, main_ref, last_ref, chunks)
    write = write_tiles(splat_ref)
    permute_group(lists_ref, main_ref, last_ref, chunks, 0, write)
    forward = triangle_pair(True)

    def work(step):
        slot = (step % BUFFERS) * batch if isinstance(step, int) else 0
        first = step * batch - slot

        def items(part):
            return range(slot + part * size, slot + (part + 1) * size)

        def span(part):
            start = (slot + part * size) * TILE_PIXELS
            return slice(start, start + size * TILE_PIXELS)

        def alphas(part):
            for item in items(part):
                tile = first + item
                alpha_phase(
                    splat_ref, tile, numbers_ref[tile], item, row_ref, alpha_ref, None, log_pair_ref
                )

        def befores(part):
            before_ref[span(part), :] = jnp.dot(
                log_pair_ref[span(part), :], forward, preferred_element_type=f32
            )

        def weights(part):
            for item in items(part):
                weight_phase(item, before_ref, alpha_ref, None, pair_ref)

        def colours(part):
            for item in items(part):
                tile = first + item
                high, low = split_colours(splat_ref, tile)
                pair = pair_ref[item * TILE_PIXELS : (item + 1) * TILE_PIXELS, :]
                rendered = colour_sum(high, low, pair)
                for channel in range(3):
                    out_ref[channel, pl.ds(tile, 1), :] = rendered[channel : channel + 1]

        staggered([alphas, befores, weights, colours], parts)

    for step in range(tile_count // batch):
        if step + 1 < tile_count // batch:
            permute_group(lists_ref, main_ref, last_ref, chunks, step + 1, write)
        work(step)


def render(numbers, lists, packed):
    tile_count = lists.shape[0]
    chunks = packed.shape[0]
    batch = batch_tiles(tile_count)
    pixels = BUFFERS * batch * TILE_PIXELS
    plain = pltpu.VMEM((pixels, LIST_LEN), f32)
    pairs = pltpu.VMEM((pixels, 2 * LIST_LEN), bf16)
    return pl.pallas_call(
        render_body,
        out_shape=jax.ShapeDtypeStruct((3, tile_count, TILE_PIXELS), f32),
        in_specs=[SMEM, VMEM, VMEM],
        out_specs=VMEM,
        scratch_shapes=[
            pltpu.VMEM((chunks, 8, LANES), f32),
            pltpu.VMEM((chunks, LANES), f32),
            pltpu.VMEM((tile_count, 16, LANES), f32),
            pltpu.VMEM((BUFFERS * batch, 48, LANES), f32),
            plain,
            plain,
            pairs,
            pairs,
        ],
        compiler_params=pltpu.CompilerParams(vmem_limit_bytes=VMEM_LIMIT),
        name="render_tiles",
    )(numbers, lists, packed)


def exchange(packed, devices):
    rows = packed.shape[0]
    if rows == devices:
        packed = lax.all_to_all(packed, "dev", split_axis=0, concat_axis=0, tiled=True)
        return pltpu.with_memory_space_constraint(packed, pltpu.VMEM)
    cap = rows * LANES // devices
    slots = packed.reshape(rows, ROWS, LANES).transpose(1, 0, 2).reshape(ROWS, devices, cap)
    slots = lax.all_to_all(slots, "dev", split_axis=1, concat_axis=1, tiled=True)
    slots = slots.reshape(ROWS, rows, LANES).transpose(1, 0, 2)
    return slots.reshape(rows, 1, ROWS * LANES)


def shards(
    gauss_params,
    adam_first,
    adam_second,
    camera,
    send_first,
    send_second,
    lists_first,
    lists_second,
    tiles_first,
    tiles_second,
    targets,
):
    devices = lax.axis_size("dev")
    half_width = 0.5 * TILES_X * tile_edge
    half_height = 0.5 * (lists_first.shape[0] * devices // TILES_X * tile_edge)
    keep = functools.partial(pltpu.with_memory_space_constraint, memory_space=pltpu.VMEM)
    leave = functools.partial(pltpu.with_memory_space_constraint, memory_space=pltpu.HBM)
    packed, kept_params = first_owner(
        leave(camera), leave(gauss_params), leave(send_first), half_width, half_height
    )
    packed = exchange(packed, devices)
    packed = train(tiles_first, keep(lists_first), jnp.transpose(targets, (1, 0, 2)), packed)
    packed = exchange(packed, devices)
    new_params, new_first, new_second, packed = second_owner(
        camera,
        keep(kept_params),
        leave(adam_first),
        leave(adam_second),
        keep(send_first),
        keep(send_second),
        packed,
        half_width,
        half_height,
    )
    packed = exchange(packed, devices)
    rendered = render(tiles_second, keep(lists_second), packed)
    return (new_params, new_first, new_second, jnp.transpose(rendered, (1, 0, 2)))


def solution(mesh):
    placed = (
        P(None, "dev"),
        P(None, "dev"),
        P(None, "dev"),
        P(),
        P("dev", None),
        P("dev", None),
        P("dev", None),
        P("dev", None),
        P("dev"),
        P("dev"),
        P("dev", None, None),
    )
    return jax.shard_map(
        shards,
        mesh=mesh,
        in_specs=placed,
        out_specs=(P(None, "dev"), P(None, "dev"), P(None, "dev"), P("dev", None, None)),
        check_vma=False,
    )
```

```python
import functools

import jax
import jax.numpy as jnp
import numpy as np
from jax import lax
from jax.experimental import pallas as pl
from jax.experimental.pallas import tpu as pltpu
from jax.sharding import PartitionSpec as P

PARAMS = 59
LIST_LEN = 128
TILE_PIXELS = 256
TILES_X = 128
LANES = 128
ROWS = 9
STRIDE = 72
PARTS = 4
BUFFERS = 2
VMEM_LIMIT = 36 << 20

tile_edge = 16
focal_length = 1000.0
blur_floor = 0.3
adam_epsilon = 1e-08
bias_first = 1.0 - 0.9**20
bias_second = 1.0 - 0.999**20
sh_first = 0.28209479177387814
sh_second = 0.4886025119029199
sh_third = (
    1.0925484305920792,
    -1.0925484305920792,
    0.31539156525252005,
    -1.0925484305920792,
    0.5462742152960396,
)
sh_fourth = (
    -0.5900435899266435,
    2.890611442640554,
    -0.4570457994644658,
    0.3731763325901154,
    -0.4570457994644658,
    1.445305721320277,
    -0.5900435899266435,
)

f32 = jnp.float32
bf16 = jnp.bfloat16
VMEM = pl.BlockSpec(memory_space=pltpu.VMEM)
SMEM = pl.BlockSpec(memory_space=pltpu.SMEM)
ANY = pl.BlockSpec(memory_space=pl.ANY)
HBM = pl.BlockSpec(memory_space=pltpu.HBM)


def rate_values():
    values = np.full((64,), 0.000125)
    values[0:3] = 0.00016
    values[3:6] = 0.005
    values[6:10] = 0.001
    values[10] = 0.05
    values[11] = 0.0025
    values[27] = 0.0025
    values[43] = 0.0025
    return values


def camera_frame(camera_ref, view):
    shape = (8, LANES)
    angle = [jnp.full(shape, camera_ref[view, k], f32) for k in range(3)]
    shift = [jnp.full(shape, camera_ref[view, 3 + k], f32) for k in range(3)]
    (ca, cb, cc) = [jnp.cos(x) for x in angle]
    (sa, sb, sc) = [jnp.sin(x) for x in angle]
    rot = [
        [cc * cb, cc * sb * sa - sc * ca, cc * sb * ca + sc * sa],
        [sc * cb, sc * sb * sa + cc * ca, sc * sb * ca - cc * sa],
        [-sb, cb * sa, cb * ca],
    ]
    back = [
        rot[0][k] * shift[0] + rot[1][k] * shift[1] + rot[2][k] * shift[2]
        for k in range(3)
    ]
    return rot, shift, back


def sh_terms(x, y, z):
    xx, yy, zz = (x * x, y * y, z * z)
    return [
        -sh_second * y,
        sh_second * z,
        -sh_second * x,
        sh_third[0] * x * y,
        sh_third[1] * y * z,
        sh_third[2] * (2.0 * zz - xx - yy),
        sh_third[3] * x * z,
        sh_third[4] * (xx - yy),
        sh_fourth[0] * y * (3.0 * xx - yy),
        sh_fourth[1] * x * y * z,
        sh_fourth[2] * y * (4.0 * zz - xx - yy),
        sh_fourth[3] * z * (2.0 * zz - 3.0 * xx - 3.0 * yy),
        sh_fourth[4] * x * (4.0 * zz - xx - yy),
        sh_fourth[5] * z * (xx - yy),
        sh_fourth[6] * x * (xx - 3.0 * yy),
    ]


def project(params, frame, half_width, half_height):
    rot, shift, back = frame
    centres = params[0:3]
    viewed = [
        rot[k][0] * centres[0] + rot[k][1] * centres[1] + rot[k][2] * centres[2] + shift[k]
        for k in range(3)
    ]
    inverse = 1.0 / viewed[2]
    scale_z = focal_length * inverse
    u_off = scale_z * viewed[0]
    w_off = scale_z * viewed[1]
    slope_u = u_off * inverse
    slope_w = w_off * inverse
    scales = [jnp.exp(params[3 + k]) for k in range(3)]
    q = params[6:10]
    norm = lax.rsqrt(q[0] * q[0] + q[1] * q[1] + q[2] * q[2] + q[3] * q[3])
    qw, qx, qy, qz = [v * norm for v in q]
    turn = [
        [
            1.0 - 2.0 * (qy * qy + qz * qz),
            2.0 * (qx * qy - qw * qz),
            2.0 * (qx * qz + qw * qy),
        ],
        [
            2.0 * (qx * qy + qw * qz),
            1.0 - 2.0 * (qx * qx + qz * qz),
            2.0 * (qy * qz - qw * qx),
        ],
        [
            2.0 * (qx * qz - qw * qy),
            2.0 * (qy * qz + qw * qx),
            1.0 - 2.0 * (qx * qx + qy * qy),
        ],
    ]
    mapping = [
        [scale_z * rot[0][k] - slope_u * rot[2][k] for k in range(3)],
        [scale_z * rot[1][k] - slope_w * rot[2][k] for k in range(3)],
    ]
    factor = [
        [
            (row[0] * turn[0][k] + row[1] * turn[1][k] + row[2] * turn[2][k]) * scales[k]
            for k in range(3)
        ]
        for row in mapping
    ]
    first, second = factor
    cover_a = first[0] * first[0] + first[1] * first[1] + first[2] * first[2] + blur_floor
    cover_b = first[0] * second[0] + first[1] * second[1] + first[2] * second[2]
    cover_c = second[0] * second[0] + second[1] * second[1] + second[2] * second[2] + blur_floor
    scale_det = 1.0 / (cover_a * cover_c - cover_b * cover_b)
    opacity = 1.0 / (1.0 + jnp.exp(-params[10]))
    towards = [centres[k] + back[k] for k in range(3)]
    length = lax.rsqrt(
        towards[0] * towards[0] + towards[1] * towards[1] + towards[2] * towards[2]
    )
    harmonics = sh_terms(*[v * length for v in towards])
    colours = []
    for channel in range(3):
        running = 0.5 + sh_first * params[11 + 16 * channel]
        for term in range(15):
            running = running + harmonics[term] * params[12 + 16 * channel + term]
        colours.append(jnp.maximum(running, 0.0))
    return [
        u_off + half_width,
        w_off + half_height,
        cover_c * scale_det,
        -cover_b * scale_det,
        cover_a * scale_det,
        opacity,
    ] + colours


def permute_group(idx_ref, main_ref, last_ref, chunks, group, write):
    base = group * 8 if isinstance(group, int) else pl.multiple_of(group * 8, 8)
    index = idx_ref[pl.ds(base, 8), :]
    high = index >> 7
    low = index & 127
    totals = []
    for k in range(8):
        row_high = jnp.broadcast_to(high[k : k + 1], (8, LANES))
        row_low = jnp.broadcast_to(low[k : k + 1], (8, LANES))
        total = jnp.zeros((8, LANES), f32)
        for chunk in range(chunks):
            found = jnp.take_along_axis(
                main_ref[chunk], row_low, axis=1, mode="promise_in_bounds"
            )
            total = jnp.where(row_high == chunk, found, total)
        totals.append(total)
    total = jnp.zeros((8, LANES), f32)
    for chunk in range(chunks):
        source = jnp.broadcast_to(last_ref[chunk : chunk + 1, :], (8, LANES))
        found = jnp.take_along_axis(source, low, axis=1, mode="promise_in_bounds")
        total = jnp.where(high == chunk, found, total)
    write(group, totals, total)


def permute(idx_ref, main_ref, last_ref, chunks, rows, write):
    def group_step(group, unused):
        permute_group(idx_ref, main_ref, last_ref, chunks, group, write)
        return unused

    lax.fori_loop(0, rows // 8, group_step, 0)


def invert(idx_ref, rows, high_count, inverse_ref):
    index = idx_ref[...]
    high = index >> 7
    low = index & 127
    high_ids = lax.broadcasted_iota(jnp.int32, (high_count, LANES), 0)
    low_ids = lax.broadcasted_iota(jnp.int32, (LANES, LANES), 0)
    lane_ids = lax.broadcasted_iota(jnp.int32, (high_count, LANES), 1).astype(f32)
    total = jnp.zeros((2 * high_count, LANES), f32)
    for start in range(0, rows, 8):
        left = []
        right = []
        for row in range(start, start + 8):
            here = high[row : row + 1] == high_ids
            left.append(
                jnp.concatenate(
                    [jnp.where(here, row + 1.0, 0.0), jnp.where(here, lane_ids, 0.0)], axis=0
                ).astype(bf16)
            )
            right.append(jnp.where(low[row : row + 1] == low_ids, 1.0, 0.0).astype(bf16))
        total = total + lax.dot_general(
            jnp.concatenate(left, axis=1),
            jnp.concatenate(right, axis=1),
            (((1,), (1,)), ((), ())),
            preferred_element_type=f32,
        )
    rows_found = total[:high_count].astype(jnp.int32)
    lanes_found = total[high_count:].astype(jnp.int32)
    inverse_ref[...] = (rows_found - 1) * LANES + lanes_found


def unpack(packed_ref, main_ref, last_ref, chunks):
    for chunk in range(chunks):
        for k in range(8):
            main_ref[chunk, k : k + 1, :] = packed_ref[chunk, :, k * LANES : (k + 1) * LANES]
        last_ref[chunk : chunk + 1, :] = packed_ref[chunk, :, 8 * LANES : 9 * LANES]


def pack_group(packed_ref):
    def write(group, vectors, last):
        for k in range(8):
            row = group * 8 + k
            for item in range(8):
                packed_ref[row, :, item * LANES : (item + 1) * LANES] = vectors[k][
                    item : item + 1
                ]
            packed_ref[row, :, 8 * LANES : 9 * LANES] = last[k : k + 1]

    return write


def slots_as_rows(slots_ref, idx_ref, rows):
    for row in range(rows):
        idx_ref[row : row + 1, :] = slots_ref[:, row * LANES : (row + 1) * LANES]


def native_to_group(native, ref, block, k):
    if native.shape[0] == 8:
        ref[pl.ds(64 * block + k, 8, stride=8), :] = native
    else:
        for row in range(native.shape[0]):
            target = 64 * block + 8 * row + k
            ref[target : target + 1, :] = native[row : row + 1]


def dense_load(dense_ref, row, group):
    return dense_ref[pl.ds(pl.multiple_of(row * STRIDE + group * 8, 8), 8), :]


def dense_store(dense_ref, row, group, value):
    dense_ref[pl.ds(pl.multiple_of(row * STRIDE + group * 8, 8), 8), :] = value


def row_blocks():
    return [(block, min(8, PARAMS - 8 * block)) for block in range((PARAMS + 7) // 8)]


def split_splats(splat_ref, parts_ref, chunks):
    for row in range(ROWS):
        for start in range(0, chunks, 16):
            value = splat_ref[row * STRIDE + start : row * STRIDE + start + 16, :]
            target = slice(row * chunks + start, row * chunks + start + 16)
            for term in range(3):
                rounded = value.astype(bf16)
                parts_ref[target, term * LANES : (term + 1) * LANES] = rounded
                value = value - rounded.astype(f32)


def matrix_gather(parts_ref, idx_ref, base, chunks, packed_ref):
    index = idx_ref[pl.ds(pl.multiple_of(base, 8), 8), :]
    high = index >> 7
    low = index & 127
    low_ids = lax.broadcasted_iota(jnp.int32, (LANES, LANES), 0)
    ids = lax.broadcasted_iota(jnp.int32, (8, LANES), 0)
    for pair in range(4):
        rows = (2 * pair, 2 * pair + 1)
        chosen = jnp.concatenate(
            [jnp.where(low[row : row + 1] == low_ids, 1.0, 0.0) for row in rows], axis=1
        ).astype(bf16)
        found = jnp.dot(
            parts_ref[...],
            jnp.concatenate([chosen, chosen, chosen], axis=0),
            preferred_element_type=f32,
        )
        for half, row in enumerate(rows):
            wanted = jnp.broadcast_to(high[row : row + 1], (8, LANES))
            masks = [ids + 8 * block == wanted for block in range(chunks // 8)]
            for item in range(ROWS):
                total = jnp.zeros((8, LANES), f32)
                for block in range(chunks // 8):
                    start = item * chunks + 8 * block
                    piece = found[start : start + 8, half * LANES : (half + 1) * LANES]
                    total = jnp.where(masks[block], piece, total)
                packed_ref[base + row, :, item * LANES : (item + 1) * LANES] = jnp.sum(
                    total, axis=0, keepdims=True
                )


def send_splats(splat_ref, main_ref, parts_ref, idx_ref, packed_ref, chunks, rows):
    for chunk in range(chunks):
        main_ref[chunk] = splat_ref[pl.ds(chunk, 8, stride=STRIDE), :]
    last_ref = splat_ref.at[pl.ds(8 * STRIDE, chunks), :]
    split_splats(splat_ref, parts_ref, chunks)
    write = pack_group(packed_ref)

    def step(group, unused):
        matrix_gather(parts_ref, idx_ref, rows // 2 + 8 * group, chunks, packed_ref)
        permute_group(idx_ref, main_ref, last_ref, chunks, group, write)
        return unused

    lax.fori_loop(0, rows // 16, step, 0)


def first_owner_body(
    half_width,
    half_height,
    camera_hbm,
    params_hbm,
    slots_hbm,
    packed_ref,
    params_ref,
    slots_ref,
    camera_ref,
    even_ref,
    odd_ref,
    splat_ref,
    main_ref,
    parts_ref,
    idx_ref,
    sems,
):
    chunks = params_hbm.shape[1] // LANES
    rows = slots_hbm.shape[1] // LANES
    groups = chunks // 8
    small = [
        pltpu.make_async_copy(camera_hbm, camera_ref, sems.at[groups]),
        pltpu.make_async_copy(slots_hbm, slots_ref, sems.at[groups + 1]),
    ]

    def load(group):
        columns = pl.ds(pl.multiple_of(group * (8 * LANES), 8 * LANES), 8 * LANES)
        return pltpu.make_async_copy(
            params_hbm.at[:, columns], params_ref.at[:, columns], sems.at[group]
        )

    for copy in small:
        copy.start()
    for group in range(groups):
        load(group).start()
    for copy in small:
        copy.wait()
    frame = camera_frame(camera_ref, 0)

    def prepare(group, dense_ref):
        for k in range(8):
            chunk = group * 8 + k
            lanes = pl.ds(pl.multiple_of(chunk * LANES, LANES), LANES)
            for block, size in row_blocks():
                native_to_group(
                    params_ref[8 * block : 8 * block + size, lanes], dense_ref, block, k
                )
        params = [dense_ref[8 * row : 8 * row + 8, :] for row in range(PARAMS)]
        for row, value in enumerate(project(params, frame, half_width, half_height)):
            dense_store(splat_ref, row, group, value)

    def step(pair, unused):
        load(2 * pair).wait()
        load(2 * pair + 1).wait()
        prepare(2 * pair, even_ref)
        prepare(2 * pair + 1, odd_ref)
        return unused

    lax.fori_loop(0, groups // 2, step, 0)
    slots_as_rows(slots_ref, idx_ref, rows)
    send_splats(splat_ref, main_ref, parts_ref, idx_ref, packed_ref, chunks, rows)


def first_owner(camera, params, slots, half_width, half_height):
    chunks = params.shape[1] // LANES
    rows = slots.shape[1] // LANES
    return pl.pallas_call(
        functools.partial(first_owner_body, half_width, half_height),
        out_shape=(pltpu.VMEM((rows, 1, ROWS * LANES), f32), pltpu.VMEM(params.shape, f32)),
        in_specs=[HBM, HBM, HBM],
        out_specs=(VMEM, VMEM),
        scratch_shapes=[
            pltpu.VMEM(slots.shape, jnp.int32),
            pltpu.SMEM(camera.shape, f32),
            pltpu.VMEM((64 * 8, LANES), f32),
            pltpu.VMEM((64 * 8, LANES), f32),
            pltpu.VMEM((ROWS * STRIDE, LANES), f32),
            pltpu.VMEM((chunks, 8, LANES), f32),
            pltpu.VMEM((ROWS * chunks, 3 * LANES), bf16),
            pltpu.VMEM((rows, LANES), jnp.int32),
            pltpu.SemaphoreType.DMA((chunks // 8 + 2,)),
        ],
        compiler_params=pltpu.CompilerParams(vmem_limit_bytes=VMEM_LIMIT),
        name="first_owner",
    )(camera, params, slots)


def second_owner_body(
    half_width,
    half_height,
    camera_ref,
    params_ref,
    first_hbm,
    second_hbm,
    inverse_ref,
    next_slots_ref,
    packed_ref,
    out_params_hbm,
    out_first_hbm,
    out_second_hbm,
    out_packed_ref,
    dense_ref,
    grad_ref,
    fresh_ref,
    splat_ref,
    next_splat_ref,
    main_ref,
    parts_ref,
    last_ref,
    idx_ref,
    first_ref,
    second_ref,
    params_out_ref,
    first_out_ref,
    second_out_ref,
    load_sems,
    store_sems,
):
    chunks = params_ref.shape[1] // LANES
    rows = next_slots_ref.shape[1] // LANES
    groups = chunks // 8

    def columns_of(group):
        return pl.ds(pl.multiple_of(group * (8 * LANES), 8 * LANES), 8 * LANES)

    def loads(group):
        columns = columns_of(group)
        return [
            pltpu.make_async_copy(
                source.at[:, columns], target.at[:, columns], load_sems.at[number, group]
            )
            for number, (source, target) in enumerate(
                [(first_hbm, first_ref), (second_hbm, second_ref)]
            )
        ]

    for group in range(groups):
        for copy in loads(group):
            copy.start()
    unpack(packed_ref, main_ref, last_ref, rows)
    frame = camera_frame(camera_ref, 0)
    next_frame = camera_frame(camera_ref, 1)
    rates = rate_values() / bias_first
    row_ids = lax.broadcasted_iota(jnp.int32, (8, LANES), 0)

    def write_columns(group, vectors, last):
        for k in range(8):
            splat_ref[pl.ds(group * 8 + k, 8, stride=STRIDE), :] = vectors[k]
        dense_store(splat_ref, 8, group, last)

    def lanes_of(group, k):
        start = pl.multiple_of(group * (8 * LANES), 8 * LANES) + k * LANES
        return pl.ds(pl.multiple_of(start, LANES), LANES)

    def stores(group):
        columns = columns_of(group)
        return [
            pltpu.make_async_copy(
                source.at[:, columns], target.at[:, columns], store_sems.at[number, group]
            )
            for number, (source, target) in enumerate(
                [
                    (params_out_ref, out_params_hbm),
                    (first_out_ref, out_first_hbm),
                    (second_out_ref, out_second_hbm),
                ]
            )
        ]

    def work(group):
        for copy in loads(group):
            copy.wait()
        for block, size in row_blocks():
            for k in range(8):
                native = params_ref[8 * block : 8 * block + size, lanes_of(group, k)]
                native_to_group(native, dense_ref, block, k)
        params = [dense_ref[8 * row : 8 * row + 8, :] for row in range(PARAMS)]
        splats, pullback = jax.vjp(
            lambda *p: project(list(p), frame, half_width, half_height), *params
        )
        cotangents = [dense_load(splat_ref, row, group) for row in range(ROWS)]
        through_opacity = cotangents[5] * (1.0 - splats[5])
        cotangents[5] = jnp.zeros_like(cotangents[5])
        grads = list(pullback(cotangents))
        grads[10] = through_opacity
        for row, value in enumerate(grads):
            grad_ref[8 * row : 8 * row + 8, :] = value
        for block, size in row_blocks():
            span = slice(8 * block, 8 * block + size)
            block_rates = rates[8 * block : 8 * block + 8]
            step_size = jnp.full((8, LANES), block_rates[0], f32)
            for k in range(1, 8):
                if block_rates[k] != block_rates[0]:
                    step_size = jnp.where(row_ids == k, f32(block_rates[k]), step_size)
            step_size = step_size[:size]
            for k in range(8):
                lanes = lanes_of(group, k)
                gradient = grad_ref[pl.ds(64 * block + k, 8, stride=8), :][:size]
                moment = 0.9 * first_ref[span, lanes] + 0.1 * gradient
                square = 0.999 * second_ref[span, lanes] + 0.001 * gradient * gradient
                scaled = square * (1.0 / bias_second)
                root = scaled * lax.rsqrt(scaled)
                fresh = params_ref[span, lanes] - step_size * moment / (root + adam_epsilon)
                first_out_ref[span, lanes] = moment
                second_out_ref[span, lanes] = square
                params_out_ref[span, lanes] = fresh
                native_to_group(fresh, fresh_ref, block, k)
        for copy in stores(group):
            copy.start()
        params = [fresh_ref[8 * row : 8 * row + 8, :] for row in range(PARAMS)]
        for row, value in enumerate(project(params, next_frame, half_width, half_height)):
            dense_store(next_splat_ref, row, group, value)

    permute_group(inverse_ref, main_ref, last_ref, rows, 0, write_columns)

    def step(group, unused):
        work(group - 1)
        permute_group(inverse_ref, main_ref, last_ref, rows, group, write_columns)
        return unused

    lax.fori_loop(1, groups, step, 0)
    work(groups - 1)
    slots_as_rows(next_slots_ref, idx_ref, rows)
    send_splats(next_splat_ref, main_ref, parts_ref, idx_ref, out_packed_ref, chunks, rows)
    for group in range(groups):
        for copy in stores(group):
            copy.wait()


def second_owner(camera, params, first, second, inverse, next_slots, packed, half_width, half_height):
    chunks = params.shape[1] // LANES
    rows = next_slots.shape[1] // LANES
    shape = jax.ShapeDtypeStruct(params.shape, f32)
    return pl.pallas_call(
        functools.partial(second_owner_body, half_width, half_height),
        out_shape=(shape, shape, shape, pltpu.VMEM((rows, 1, ROWS * LANES), f32)),
        in_specs=[SMEM, VMEM, HBM, HBM, VMEM, VMEM, VMEM],
        out_specs=(ANY, ANY, ANY, VMEM),
        scratch_shapes=[
            pltpu.VMEM((64 * 8, LANES), f32),
            pltpu.VMEM((64 * 8, LANES), f32),
            pltpu.VMEM((64 * 8, LANES), f32),
            pltpu.VMEM((ROWS * STRIDE, LANES), f32),
            pltpu.VMEM((ROWS * STRIDE, LANES), f32),
            pltpu.VMEM((max(chunks, rows), 8, LANES), f32),
            pltpu.VMEM((ROWS * chunks, 3 * LANES), bf16),
            pltpu.VMEM((rows, LANES), f32),
            pltpu.VMEM((rows, LANES), jnp.int32),
            pltpu.VMEM(params.shape, f32),
            pltpu.VMEM(params.shape, f32),
            pltpu.VMEM(params.shape, f32),
            pltpu.VMEM(params.shape, f32),
            pltpu.VMEM(params.shape, f32),
            pltpu.SemaphoreType.DMA((2, chunks // 8)),
            pltpu.SemaphoreType.DMA((3, chunks // 8)),
        ],
        compiler_params=pltpu.CompilerParams(vmem_limit_bytes=VMEM_LIMIT),
        name="second_owner",
    )(camera, params, first, second, inverse, next_slots, packed)


def prepare_body(lists_ref, slots_ref, unused_ref, lists_inverse_ref, slots_inverse_ref, idx_ref):
    rows = slots_ref.shape[1] // LANES
    invert(lists_ref, lists_ref.shape[0], lists_inverse_ref.shape[0], lists_inverse_ref)
    slots_as_rows(slots_ref, idx_ref, rows)
    invert(idx_ref, rows, slots_inverse_ref.shape[0], slots_inverse_ref)


def prepare(lists, slots, after, columns):
    rows = slots.shape[1] // LANES
    return pl.pallas_call(
        prepare_body,
        out_shape=(
            pltpu.VMEM((rows, LANES), jnp.int32),
            pltpu.VMEM((columns // LANES, LANES), jnp.int32),
        ),
        in_specs=[VMEM, VMEM, ANY],
        out_specs=(VMEM, VMEM),
        scratch_shapes=[pltpu.VMEM((rows, LANES), jnp.int32)],
        compiler_params=pltpu.CompilerParams(vmem_limit_bytes=VMEM_LIMIT),
        name="prepare",
    )(lists, slots, after)


def halves(value):
    high = value.astype(bf16)
    return high, (value - high.astype(f32)).astype(bf16)


def triangle_pair(forward):
    rows = lax.broadcasted_iota(jnp.int32, (LIST_LEN, LIST_LEN), 0)
    cols = lax.broadcasted_iota(jnp.int32, (LIST_LEN, LIST_LEN), 1)
    chosen = rows < cols if forward else rows > cols
    one = jnp.where(chosen, 1.0, 0.0).astype(bf16)
    return jnp.concatenate([one, one], axis=0)


def batch_tiles(tile_count):
    return 8


LOG2_E = 1.4426950408889634


def tile_offsets(splat_ref, tile, number):
    left = (number % TILES_X) * tile_edge
    top = (number // TILES_X) * tile_edge
    ids = lax.broadcasted_iota(jnp.int32, (8, LANES), 0)
    u = jnp.broadcast_to(splat_ref[tile, 0:1, :], (8, LANES))
    w = jnp.broadcast_to(splat_ref[tile, 1:2, :], (8, LANES))
    across = [u - ((ids + (left + 8 * h)).astype(f32) + 0.5) for h in range(2)]
    down = [w - ((ids + (top + 8 * h)).astype(f32) + 0.5) for h in range(2)]
    return across, down


def spread_row(ref, item, row):
    return jnp.broadcast_to(ref[item, row : row + 1, :], (8, LANES))


def alpha_phase(splat_ref, tile, number, item, row_ref, alpha_ref, odds_ref, pair_ref):
    a, b, c, o = [jnp.broadcast_to(splat_ref[tile, k : k + 1, :], (8, LANES)) for k in (2, 3, 4, 5)]
    across, down = tile_offsets(splat_ref, tile, number)
    base = item * TILE_PIXELS
    along = [((-0.5 * LOG2_E) * a) * x * x for x in across]
    for h in range(2):
        row_ref[item, 8 * h : 8 * h + 8, :] = ((-0.5 * LOG2_E) * c) * down[h] * down[h]
        row_ref[item, 16 + 8 * h : 24 + 8 * h, :] = ((-LOG2_E) * b) * down[h]
        if odds_ref is not None:
            row_ref[item, 32 + 8 * h : 40 + 8 * h, :] = down[h]
    for row in range(tile_edge):
        fixed = spread_row(row_ref, item, row)
        slope = spread_row(row_ref, item, 16 + row)
        logs = []
        for h in range(2):
            exponent = along[h] + (fixed + slope * across[h])
            alpha = o * jnp.exp2(exponent)
            log_clear = jnp.log(1.0 - alpha) * LOG2_E
            where = slice(base + row * tile_edge + 8 * h, base + row * tile_edge + 8 * h + 8)
            alpha_ref[where, :] = alpha
            if odds_ref is not None:
                odds_ref[where, :] = alpha * jnp.exp2(-log_clear)
            logs.append(log_clear)
        high, low = halves(jnp.concatenate(logs, axis=0))
        where = slice(base + row * tile_edge, base + (row + 1) * tile_edge)
        pair_ref[where, :LIST_LEN] = high
        pair_ref[where, LIST_LEN:] = low


def weight_phase(item, before_ref, alpha_ref, weight_ref, pair_ref):
    for row in range(tile_edge):
        start = item * TILE_PIXELS + row * tile_edge
        where = slice(start, start + tile_edge)
        weight = alpha_ref[where, :] * jnp.exp2(before_ref[where, :])
        if weight_ref is not None:
            weight_ref[where, :] = weight
        high, low = halves(weight)
        pair_ref[where, :LIST_LEN] = high
        pair_ref[where, LIST_LEN:] = low


def split_colours(splat_ref, tile):
    colours = splat_ref[tile, 6:14, :]
    high = colours.astype(bf16).astype(f32)
    return high, colours - high


def colour_sum(high, low, pair):
    upper = jnp.concatenate([high, high], axis=1)
    lower = jnp.concatenate([low, jnp.zeros_like(low)], axis=1)
    result = lax.dot_general(
        jnp.concatenate([upper, lower], axis=0).astype(bf16),
        pair,
        (((1,), (1,)), ((), ())),
        preferred_element_type=f32,
    )
    return result[0:8] + result[8:16]


def write_tiles(splat_ref):
    def write(group, vectors, last):
        for k in range(8):
            tile = group * 8 + k
            splat_ref[tile, 0:8, :] = vectors[k]
            splat_ref[tile, 8:9, :] = last[k : k + 1]
            splat_ref[tile, 9:16, :] = jnp.zeros((7, LANES), f32)

    return write


def staggered(stages, parts):
    for turn in range(len(stages) + parts - 1):
        for part in range(parts):
            if 0 <= turn - part < len(stages):
                stages[turn - part](part)


def train_body(
    numbers_ref,
    lists_ref,
    targets_ref,
    packed_ref,
    inverse_ref,
    out_packed_ref,
    main_ref,
    last_ref,
    splat_ref,
    row_ref,
    alpha_ref,
    odds_ref,
    before_ref,
    weight_ref,
    log_pair_ref,
    pair_ref,
    pull_ref,
    grad_pair_ref,
    grad_ref,
    parts_ref,
):
    tile_count = lists_ref.shape[0]
    chunks = packed_ref.shape[0]
    batch = batch_tiles(tile_count)
    parts = PARTS if batch % PARTS == 0 else 1
    size = batch // parts
    unpack(packed_ref, main_ref, last_ref, chunks)
    write = write_tiles(splat_ref)
    permute_group(lists_ref, main_ref, last_ref, chunks, 0, write)
    forward = triangle_pair(True)
    backward = triangle_pair(False)

    def put(item, tile, value):
        grad_ref[pl.ds(item * STRIDE + tile, 1), :] = value

    def work(step):
        slot = (step % BUFFERS) * batch if isinstance(step, int) else 0
        first = step * batch - slot

        def items(part):
            return range(slot + part * size, slot + (part + 1) * size)

        def span(part):
            start = (slot + part * size) * TILE_PIXELS
            return slice(start, start + size * TILE_PIXELS)

        def alphas(part):
            for item in items(part):
                tile = first + item
                alpha_phase(
                    splat_ref, tile, numbers_ref[tile], item, row_ref, alpha_ref, odds_ref, log_pair_ref
                )

        def befores(part):
            before_ref[span(part), :] = jnp.dot(
                log_pair_ref[span(part), :], forward, preferred_element_type=f32
            )

        def weights(part):
            for item in items(part):
                weight_phase(item, before_ref, alpha_ref, weight_ref, pair_ref)

        def deltas(part):
            members = items(part)
            for start in range(0, len(members), 2):
                pair_items = members[start : start + 2]
                lefts = []
                rights = []
                for place, item in enumerate(pair_items):
                    tile = first + item
                    pixels = slice(item * TILE_PIXELS, (item + 1) * TILE_PIXELS)
                    pair = pair_ref[pixels, :]
                    high, low = split_colours(splat_ref, tile)
                    rendered = colour_sum(high, low, pair)
                    wanted = [targets_ref[channel, pl.ds(tile, 1), :] for channel in range(3)]
                    wanted = jnp.concatenate(wanted + [jnp.zeros((5, TILE_PIXELS), f32)], axis=0)
                    delta = rendered - wanted
                    delta_high = delta.astype(bf16).astype(f32)
                    delta_low = delta - delta_high
                    lefts += [delta_high, delta_high, delta_low, jnp.zeros_like(delta)]
                    right = jnp.concatenate([high, low, high, jnp.zeros_like(high)], axis=0)
                    blank = [jnp.zeros_like(right)] * len(pair_items)
                    blank[place] = right
                    rights.append(jnp.concatenate(blank, axis=1))
                    colour = jnp.dot(
                        jnp.concatenate([delta_high, delta_low], axis=0).astype(bf16),
                        pair,
                        preferred_element_type=f32,
                    )
                    colour = colour[0:8, :LIST_LEN] + (
                        colour[0:8, LIST_LEN:] + colour[8:16, :LIST_LEN]
                    )
                    for channel in range(3):
                        put(6 + channel, tile, colour[channel : channel + 1])
                pulled = lax.dot_general(
                    jnp.concatenate(lefts, axis=0).astype(bf16),
                    jnp.concatenate(rights, axis=0).astype(bf16),
                    (((0,), (0,)), ((), ())),
                    preferred_element_type=f32,
                )
                for place, item in enumerate(pair_items):
                    lanes = slice(place * LIST_LEN, (place + 1) * LIST_LEN)
                    for row in range(tile_edge):
                        begin = item * TILE_PIXELS + row * tile_edge
                        where = slice(begin, begin + tile_edge)
                        factor = pulled[row * tile_edge : (row + 1) * tile_edge, lanes]
                        product = factor * weight_ref[where, :]
                        pull_ref[where, :] = product
                        product_high, product_low = halves(product)
                        grad_pair_ref[where, :LIST_LEN] = product_high
                        grad_pair_ref[where, LIST_LEN:] = product_low

        def afters(part):
            before_ref[span(part), :] = jnp.dot(
                grad_pair_ref[span(part), :], backward, preferred_element_type=f32
            )

        def moments(part):
            for item in items(part):
                tile = first + item
                across, down = tile_offsets(splat_ref, tile, numbers_ref[tile])
                sums = [[jnp.zeros((8, LANES), f32) for j in range(3)] for h in range(2)]
                for row in range(tile_edge):
                    offset = spread_row(row_ref, item, 32 + row)
                    for h in range(2):
                        start = item * TILE_PIXELS + row * tile_edge + 8 * h
                        where = slice(start, start + 8)
                        slope = pull_ref[where, :] - before_ref[where, :] * odds_ref[where, :]
                        once = slope * offset
                        sums[h][0] = sums[h][0] + slope
                        sums[h][1] = sums[h][1] + once
                        sums[h][2] = sums[h][2] + once * offset

                def total(pieces):
                    return jnp.sum(pieces[0] + pieces[1], axis=0, keepdims=True)

                whole = total([sums[h][0] for h in range(2)])
                along = [sums[h][0] * across[h] for h in range(2)]
                moment_x = total(along)
                moment_xx = total([along[h] * across[h] for h in range(2)])
                moment_y = total([sums[h][1] for h in range(2)])
                moment_xy = total([sums[h][1] * across[h] for h in range(2)])
                moment_yy = total([sums[h][2] for h in range(2)])
                a = splat_ref[tile, 2:3, :]
                b = splat_ref[tile, 3:4, :]
                c = splat_ref[tile, 4:5, :]
                put(0, tile, -(a * moment_x + b * moment_y))
                put(1, tile, -(c * moment_y + b * moment_x))
                put(2, tile, -0.5 * moment_xx)
                put(3, tile, -moment_xy)
                put(4, tile, -0.5 * moment_yy)
                put(5, tile, whole)

        staggered([alphas, befores, weights, deltas, afters, moments], parts)

    for step in range(tile_count // batch):
        if step + 1 < tile_count // batch:
            permute_group(lists_ref, main_ref, last_ref, chunks, step + 1, write)
        work(step)
    send_splats(
        grad_ref, main_ref, parts_ref, inverse_ref, out_packed_ref, tile_count, chunks
    )


def train(numbers, lists, targets, packed, inverse):
    tile_count = lists.shape[0]
    chunks = packed.shape[0]
    batch = batch_tiles(tile_count)
    pixels = BUFFERS * batch * TILE_PIXELS
    plain = pltpu.VMEM((pixels, LIST_LEN), f32)
    pairs = pltpu.VMEM((pixels, 2 * LIST_LEN), bf16)
    return pl.pallas_call(
        train_body,
        out_shape=pltpu.VMEM(packed.shape, f32),
        in_specs=[SMEM, VMEM, VMEM, VMEM, VMEM],
        out_specs=VMEM,
        scratch_shapes=[
            pltpu.VMEM((max(chunks, tile_count), 8, LANES), f32),
            pltpu.VMEM((chunks, LANES), f32),
            pltpu.VMEM((tile_count, 16, LANES), f32),
            pltpu.VMEM((BUFFERS * batch, 48, LANES), f32),
            plain,
            plain,
            plain,
            plain,
            pairs,
            pairs,
            plain,
            pairs,
            pltpu.VMEM((ROWS * STRIDE, LANES), f32),
            pltpu.VMEM((ROWS * tile_count, 3 * LANES), bf16),
        ],
        compiler_params=pltpu.CompilerParams(vmem_limit_bytes=VMEM_LIMIT),
        name="train_tiles",
    )(numbers, lists, targets, packed, inverse)


def render_body(
    numbers_ref,
    lists_ref,
    packed_ref,
    out_ref,
    main_ref,
    last_ref,
    splat_ref,
    row_ref,
    alpha_ref,
    before_ref,
    log_pair_ref,
    pair_ref,
):
    tile_count = lists_ref.shape[0]
    chunks = packed_ref.shape[0]
    batch = batch_tiles(tile_count)
    parts = PARTS if batch % PARTS == 0 else 1
    size = batch // parts
    unpack(packed_ref, main_ref, last_ref, chunks)
    write = write_tiles(splat_ref)
    permute_group(lists_ref, main_ref, last_ref, chunks, 0, write)
    forward = triangle_pair(True)

    def work(step):
        slot = (step % BUFFERS) * batch if isinstance(step, int) else 0
        first = step * batch - slot

        def items(part):
            return range(slot + part * size, slot + (part + 1) * size)

        def span(part):
            start = (slot + part * size) * TILE_PIXELS
            return slice(start, start + size * TILE_PIXELS)

        def alphas(part):
            for item in items(part):
                tile = first + item
                alpha_phase(
                    splat_ref, tile, numbers_ref[tile], item, row_ref, alpha_ref, None, log_pair_ref
                )

        def befores(part):
            before_ref[span(part), :] = jnp.dot(
                log_pair_ref[span(part), :], forward, preferred_element_type=f32
            )

        def weights(part):
            for item in items(part):
                weight_phase(item, before_ref, alpha_ref, None, pair_ref)

        def colours(part):
            for item in items(part):
                tile = first + item
                high, low = split_colours(splat_ref, tile)
                pair = pair_ref[item * TILE_PIXELS : (item + 1) * TILE_PIXELS, :]
                rendered = colour_sum(high, low, pair)
                for channel in range(3):
                    out_ref[channel, pl.ds(tile, 1), :] = rendered[channel : channel + 1]

        staggered([alphas, befores, weights, colours], parts)

    for step in range(tile_count // batch):
        if step + 1 < tile_count // batch:
            permute_group(lists_ref, main_ref, last_ref, chunks, step + 1, write)
        work(step)


def render(numbers, lists, packed):
    tile_count = lists.shape[0]
    chunks = packed.shape[0]
    batch = batch_tiles(tile_count)
    pixels = BUFFERS * batch * TILE_PIXELS
    plain = pltpu.VMEM((pixels, LIST_LEN), f32)
    pairs = pltpu.VMEM((pixels, 2 * LIST_LEN), bf16)
    return pl.pallas_call(
        render_body,
        out_shape=jax.ShapeDtypeStruct((3, tile_count, TILE_PIXELS), f32),
        in_specs=[SMEM, VMEM, VMEM],
        out_specs=VMEM,
        scratch_shapes=[
            pltpu.VMEM((chunks, 8, LANES), f32),
            pltpu.VMEM((chunks, LANES), f32),
            pltpu.VMEM((tile_count, 16, LANES), f32),
            pltpu.VMEM((BUFFERS * batch, 48, LANES), f32),
            plain,
            plain,
            pairs,
            pairs,
        ],
        compiler_params=pltpu.CompilerParams(vmem_limit_bytes=VMEM_LIMIT),
        name="render_tiles",
    )(numbers, lists, packed)


def exchange(packed, devices):
    rows = packed.shape[0]
    if rows == devices:
        packed = lax.all_to_all(packed, "dev", split_axis=0, concat_axis=0, tiled=True)
        return pltpu.with_memory_space_constraint(packed, pltpu.VMEM)
    cap = rows * LANES // devices
    slots = packed.reshape(rows, ROWS, LANES).transpose(1, 0, 2).reshape(ROWS, devices, cap)
    slots = lax.all_to_all(slots, "dev", split_axis=1, concat_axis=1, tiled=True)
    slots = slots.reshape(ROWS, rows, LANES).transpose(1, 0, 2)
    return slots.reshape(rows, 1, ROWS * LANES)


def shards(
    gauss_params,
    adam_first,
    adam_second,
    camera,
    send_first,
    send_second,
    lists_first,
    lists_second,
    tiles_first,
    tiles_second,
    targets,
):
    devices = lax.axis_size("dev")
    half_width = 0.5 * TILES_X * tile_edge
    half_height = 0.5 * (lists_first.shape[0] * devices // TILES_X * tile_edge)
    keep = functools.partial(pltpu.with_memory_space_constraint, memory_space=pltpu.VMEM)
    leave = functools.partial(pltpu.with_memory_space_constraint, memory_space=pltpu.HBM)
    packed, kept_params = first_owner(
        leave(camera), leave(gauss_params), leave(send_first), half_width, half_height
    )
    packed = exchange(packed, devices)
    lists_inverse, slots_inverse = prepare(
        keep(lists_first), keep(send_first), kept_params, gauss_params.shape[1]
    )
    packed = train(
        tiles_first, keep(lists_first), jnp.transpose(targets, (1, 0, 2)), packed, lists_inverse
    )
    packed = exchange(packed, devices)
    new_params, new_first, new_second, packed = second_owner(
        camera,
        keep(kept_params),
        leave(adam_first),
        leave(adam_second),
        keep(slots_inverse),
        keep(send_second),
        packed,
        half_width,
        half_height,
    )
    packed = exchange(packed, devices)
    rendered = render(tiles_second, keep(lists_second), packed)
    return (new_params, new_first, new_second, jnp.transpose(rendered, (1, 0, 2)))


def solution(mesh):
    placed = (
        P(None, "dev"),
        P(None, "dev"),
        P(None, "dev"),
        P(),
        P("dev", None),
        P("dev", None),
        P("dev", None),
        P("dev", None),
        P("dev"),
        P("dev"),
        P("dev", None, None),
    )
    return jax.shard_map(
        shards,
        mesh=mesh,
        in_specs=placed,
        out_specs=(P(None, "dev"), P(None, "dev"), P(None, "dev"), P("dev", None, None)),
        check_vma=False,
    )
```
